16 devices in a mesh: dp: 2 (over y, z), tp: 8 (over x, core).
Axes of the slice: x: 4, y: 2, z: 1, core: 2. Of those that a mesh axis runs over, the one named last changes fastest.
The devices are a block of a 4x4x8 slice.
Arguments:
- x: bfloat16 [512, 3072], P(('dp', 'tp')), parts along dimension 0
- grad_y: bfloat16 [512, 3072], P(('dp', 'tp')), parts along dimension 0
- gain_attn: float32 [2, 3072], replicated
- gain_mlp: float32 [2, 3072], replicated
- w_qkv: bfloat16 [2, 3072, 5120], P(None, None, 'tp')
- w_out: bfloat16 [2, 3072, 3072], P(None, 'tp')
- w_gate: bfloat16 [2, 3072, 8192], P(None, None, 'tp')
- w_up: bfloat16 [2, 3072, 8192], P(None, None, 'tp')
- w_down: bfloat16 [2, 8192, 3072], P(None, 'tp')
Outputs:
- output 1: bfloat16 [512, 3072], P(('dp', 'tp')), parts along dimension 0
- output 2: bfloat16 [512, 3072], P(('dp', 'tp')), parts along dimension 0
- output 3: bfloat16 [4, 3072, 5120], P('dp', None, 'tp'), parts along dimension 0
- output 4: bfloat16 [4, 3072, 3072], P('dp', 'tp'), parts along dimension 0
- output 5: bfloat16 [4, 3072, 8192], P('dp', None, 'tp'), parts along dimension 0
- output 6: bfloat16 [4, 3072, 8192], P('dp', None, 'tp'), parts along dimension 0
- output 7: bfloat16 [4, 8192, 3072], P('dp', 'tp'), parts along dimension 0
- output 8: float32 [4, 3072], P('dp'), parts along dimension 0
- output 9: float32 [4, 3072], P('dp'), parts along dimension 0
There are 2 independent parts. The reference program is written for one: setup_inputs(seed, part) draws one part's arguments, and reference() takes and returns one part's arrays. A program takes and returns all parts, laid end to end along the dimension named above; an argument that names none is the same for every part.
All inputs are finite; a program needn't handle non-finite values.
Results may differ from the reference program's by a relative error of at most 0.017233.
Values are sent between devices in bfloat16 or wider.
A program may use at most 768 MiB of HBM per device.

```python
import jax
import jax.numpy as jnp
from jax import lax

D = 3072
FF = 8192
HEADS = 24
KV_HEADS = 8
HEAD = 128
LAYERS = 2
SEQ_LEN = 256
NORM_EPS = 1e-5
GROUP_SIZE = HEADS // KV_HEADS
QKV_COLS = (HEADS + 2 * KV_HEADS) * HEAD


def setup_inputs(seed: int = 0, part: int = 0) -> dict:
    part_key = jax.random.fold_in(jax.random.key(seed), part)
    act_keys = jax.random.split(part_key, 4)
    weight_keys = jax.random.split(jax.random.key(seed + 1), 7)
    x_mean = jax.random.normal(act_keys[0], (1, D), jnp.float32)
    x = jax.random.normal(act_keys[1], (SEQ_LEN, D), jnp.float32) + x_mean
    grad_mean = jax.random.normal(act_keys[2], (1, D), jnp.float32)
    grad_y = jax.random.normal(act_keys[3], (SEQ_LEN, D), jnp.float32) + grad_mean
    gain_attn = 1.0 + 0.3 * jax.random.normal(weight_keys[0], (LAYERS, D), jnp.float32)
    gain_mlp = 1.0 + 0.3 * jax.random.normal(weight_keys[1], (LAYERS, D), jnp.float32)
    w_qkv = jax.random.normal(weight_keys[2], (LAYERS, D, QKV_COLS), jnp.float32) * D ** -0.5
    w_out = jax.random.normal(weight_keys[3], (LAYERS, HEADS * HEAD, D), jnp.float32) * (HEADS * HEAD) ** -0.5
    w_gate = jax.random.normal(weight_keys[4], (LAYERS, D, FF), jnp.float32) * D ** -0.5
    w_up = jax.random.normal(weight_keys[5], (LAYERS, D, FF), jnp.float32) * D ** -0.5
    w_down = jax.random.normal(weight_keys[6], (LAYERS, FF, D), jnp.float32) * FF ** -0.5
    return {'x': x.astype(jnp.bfloat16), 'grad_y': grad_y.astype(jnp.bfloat16), 'gain_attn': gain_attn, 'gain_mlp': gain_mlp, 'w_qkv': w_qkv.astype(jnp.bfloat16), 'w_out': w_out.astype(jnp.bfloat16), 'w_gate': w_gate.astype(jnp.bfloat16), 'w_up': w_up.astype(jnp.bfloat16), 'w_down': w_down.astype(jnp.bfloat16)}


def rms_norm(hidden_in, gain_vec):
    hidden_f = hidden_in.astype(jnp.float32)
    inv_rms = lax.rsqrt(jnp.mean(hidden_f * hidden_f, axis=-1, keepdims=True) + NORM_EPS)
    return (hidden_f * inv_rms * gain_vec).astype(jnp.bfloat16)


def attention(qkv_out):
    positions = jnp.arange(SEQ_LEN)
    causal = positions[:, None] >= positions[None, :]

    def one_group(group_block):
        queries = group_block[:, :GROUP_SIZE].astype(jnp.float32)
        key_rows = group_block[:, GROUP_SIZE].astype(jnp.float32)
        value_rows = group_block[:, GROUP_SIZE + 1].astype(jnp.float32)
        scores = jnp.einsum('iqh,jh->qij', queries, key_rows) * HEAD ** -0.5
        prob_low = jax.nn.softmax(jnp.where(causal, scores, -1e30), axis=-1).astype(jnp.bfloat16)
        heads_out = jnp.einsum('qij,jh->iqh', prob_low.astype(jnp.float32), value_rows)
        return heads_out.astype(jnp.bfloat16)

    blocks = jnp.moveaxis(qkv_out.reshape(SEQ_LEN, KV_HEADS, GROUP_SIZE + 2, HEAD), 1, 0)
    heads_out = lax.map(jax.checkpoint(one_group), blocks)
    return jnp.moveaxis(heads_out, 0, 1).reshape(SEQ_LEN, HEADS * HEAD)


def decoder_layer(hidden_in, params):
    gain_attn, gain_mlp, w_qkv, w_out, w_gate, w_up, w_down = params
    normed = rms_norm(hidden_in, gain_attn)
    qkv_out = jnp.dot(normed, w_qkv, preferred_element_type=jnp.float32).astype(jnp.bfloat16)
    heads_out = attention(qkv_out)
    hidden_mid = hidden_in + jnp.dot(heads_out, w_out, preferred_element_type=jnp.float32).astype(jnp.bfloat16)
    normed_mid = rms_norm(hidden_mid, gain_mlp)
    gate_act = jnp.dot(normed_mid, w_gate, preferred_element_type=jnp.float32).astype(jnp.bfloat16)
    up_act = jnp.dot(normed_mid, w_up, preferred_element_type=jnp.float32).astype(jnp.bfloat16)
    gated_act = (jax.nn.silu(gate_act.astype(jnp.float32)) * up_act.astype(jnp.float32)).astype(jnp.bfloat16)
    return hidden_mid + jnp.dot(gated_act, w_down, preferred_element_type=jnp.float32).astype(jnp.bfloat16)


def stack_forward(x, params):
    def scan_body(hidden_carry, layer_params):
        return decoder_layer(hidden_carry, layer_params), None
    hidden_out, _ = lax.scan(scan_body, x, params)
    return hidden_out


def reference(x, grad_y, gain_attn, gain_mlp, w_qkv, w_out, w_gate, w_up, w_down):
    params = (gain_attn, gain_mlp, w_qkv, w_out, w_gate, w_up, w_down)
    y, pullback = jax.vjp(stack_forward, x, params)
    grad_x, grad_params = pullback(grad_y)
    return (y, grad_x, grad_params[2], grad_params[3], grad_params[4], grad_params[5], grad_params[6], grad_params[0], grad_params[1])
```

```python
import functools

import jax
import jax.numpy as jnp
from jax import lax
from jax.experimental import pallas as pl
from jax.experimental.pallas import tpu as pltpu
from jax.sharding import PartitionSpec as P

HEAD_DIM = 128
NORM_EPS = 1e-5
CORES = 2
MESH = pl.DeviceIdType.MESH
F32 = jnp.float32
BF16 = jnp.bfloat16
VMEM_LIMIT = 66_000_000
STEPS = 3
ANY = pl.BlockSpec(memory_space=pltpu.HBM)
VMEM_SPEC = pl.BlockSpec(memory_space=pltpu.VMEM)


def dot_nn(a, b):
    return lax.dot_general(a, b, (((1,), (0,)), ((), ())), preferred_element_type=F32)


def dot_nt(a, b):
    return lax.dot_general(a, b, (((1,), (1,)), ((), ())), preferred_element_type=F32)


def dot_tn(a, b):
    return lax.dot_general(a, b, (((0,), (0,)), ((), ())), preferred_element_type=F32)


class Links:
    def __init__(self, chips, send_sem, recv_sem):
        self.me = lax.axis_index('tp')
        self.chips = chips
        self.x = lax.div(self.me, CORES)
        self.c = lax.rem(self.me, CORES)
        self.xr = lax.rem(self.x + 1, chips)
        self.xl = lax.rem(self.x + chips - 1, chips)
        self.xo = lax.rem(self.x + 2, chips)
        self.right = self.xr * CORES + self.c
        self.left = self.xl * CORES + self.c
        self.sib = self.x * CORES + 1 - self.c
        self.send_sem, self.recv_sem, self.used, self.pending = send_sem, recv_sem, 0, []

    def enter(self, peers):
        barrier = pltpu.get_barrier_semaphore()
        for peer in peers:
            pl.semaphore_signal(barrier, inc=1, device_id={'tp': peer}, device_id_type=MESH)
        pl.semaphore_wait(barrier, len(peers))

    def others(self):
        size = self.chips * CORES
        return [lax.rem(self.me + step, size) for step in range(1, size)]

    def copy(self, src, dst, peer):
        copy = pltpu.make_async_remote_copy(
            src_ref=src, dst_ref=dst, send_sem=self.send_sem.at[self.used], recv_sem=self.recv_sem.at[self.used],
            device_id={'tp': peer}, device_id_type=MESH)
        self.used += 1
        copy.start()
        self.pending.append(copy)
        return copy

    def drain(self):
        for copy in self.pending:
            copy.wait_send()
        self.pending = []


class Gather:
    def __init__(self, links, full):
        self.links, self.full = links, full
        self.half = full.shape[3] // 2
        part_a, part_b = pl.ds(0, self.half), pl.ds(self.half, self.half)
        x, c = links.x, links.c
        self.a, self.b = part_a, part_b
        self.right_a = self.send(x, part_a, links.right)
        self.left_b = self.send(x, part_b, links.left)
        self.right_b = self.send(x, part_b, links.right)
        self.left_a = self.send(x, part_a, links.left)
        self.near = [links.copy(full.at[x, c], full.at[x, c], links.sib)]

    def send(self, chip, part, peer):
        ref = self.full.at[chip, self.links.c, :, part]
        return self.links.copy(ref, ref, peer)

    def relay(self):
        links = self.links
        self.right_a.wait_recv()
        relay_a = self.send(links.xl, self.a, links.right)
        self.near.append(self.send(links.xl, self.a, links.sib))
        self.left_b.wait_recv()
        relay_b = self.send(links.xr, self.b, links.left)
        self.near.append(self.send(links.xr, self.b, links.sib))
        self.right_b.wait_recv()
        self.near.append(self.send(links.xl, self.b, links.sib))
        self.left_a.wait_recv()
        self.near.append(self.send(links.xr, self.a, links.sib))
        self.far = (relay_a, relay_b)

    def finish(self):
        links = self.links
        self.far[0].wait_recv()
        self.near.append(self.send(links.xo, self.a, links.sib))
        self.far[1].wait_recv()
        self.near.append(self.send(links.xo, self.b, links.sib))
        for copy in self.near:
            copy.wait_recv()


def reduce_scatter(links, product, part, near, relay, from_left, from_right, fillers=()):
    chips, _, rows, cols = part.shape
    half = cols // 2
    width = half // STEPS
    x, c, xr, xl, xo = links.x, links.c, links.xr, links.xl, links.xo
    fillers = list(fillers)
    swap, first, last = [None] * STEPS, [None] * STEPS, []
    for step in range(STEPS + 2):
        if step < STEPS:
            swap[step] = []
            for base in (step * width, half + step * width):
                span = pl.ds(base, width)
                part[:, :, :, span] = product(base, width).reshape(chips, CORES, rows, width)
                swap[step].append(links.copy(part.at[:, 1 - c, :, span], near.at[:, :, span], links.sib))
        elif fillers:
            fillers.pop(0)()
        if 0 <= step - 1 < STEPS:
            done = step - 1
            span_a, span_b = pl.ds(done * width, width), pl.ds(half + done * width, width)
            for copy, span in zip(swap[done], (span_a, span_b)):
                copy.wait_recv()
                part[:, c, :, span] = part[:, c, :, span] + near[:, :, span]
            first[done] = (
                links.copy(part.at[xo, c, :, span_a], relay.at[0, :, pl.ds(done * width, width)], links.right),
                links.copy(part.at[xo, c, :, span_b], relay.at[1, :, pl.ds(done * width, width)], links.left))
            last.append(links.copy(part.at[xr, c, :, span_b], from_left.at[:, span_b], links.right))
            last.append(links.copy(part.at[xl, c, :, span_a], from_right.at[:, span_a], links.left))
        if 0 <= step - 2 < STEPS:
            done = step - 2
            span_a, span_b = pl.ds(done * width, width), pl.ds(half + done * width, width)
            first[done][0].wait_recv()
            part[xr, c, :, span_a] = part[xr, c, :, span_a] + relay[0, :, pl.ds(done * width, width)]
            last.append(links.copy(part.at[xr, c, :, span_a], from_left.at[:, span_a], links.right))
            first[done][1].wait_recv()
            part[xl, c, :, span_b] = part[xl, c, :, span_b] + relay[1, :, pl.ds(done * width, width)]
            last.append(links.copy(part.at[xl, c, :, span_b], from_right.at[:, span_b], links.left))
    for filler in fillers:
        filler()
    for copy in last:
        copy.wait_recv()
    total = part[x, c] + from_left[...] + from_right[...]
    return total


def rms_norm(hidden, gain):
    hidden_f = hidden.astype(F32)
    inv_rms = lax.rsqrt(jnp.mean(hidden_f * hidden_f, axis=-1, keepdims=True) + NORM_EPS)
    return (hidden_f * inv_rms * gain).astype(BF16)


def rms_norm_pull(hidden, gain, cotangent):
    hidden_f, cot = hidden.astype(F32), cotangent.astype(F32)
    inv_rms = lax.rsqrt(jnp.mean(hidden_f * hidden_f, axis=-1, keepdims=True) + NORM_EPS)
    scaled = cot * gain
    dot = jnp.mean(scaled * hidden_f, axis=-1, keepdims=True)
    d_hidden = scaled * inv_rms - hidden_f * (inv_rms * inv_rms * inv_rms * dot)
    return d_hidden.astype(BF16), jnp.sum(cot * (hidden_f * inv_rms), axis=0, keepdims=True)


def flat(ref):
    chips, cores, rows, cols = ref.shape
    return ref[...].reshape(chips * cores * rows, cols)


def project(full, weight, out, tile):
    def body(index, carry):
        cols = pl.ds(pl.multiple_of(index * tile, tile), tile)
        out[:, cols] = dot_nn(flat(full), weight[:, cols]).astype(BF16)
        return carry
    lax.fori_loop(0, out.shape[1] // tile, body, 0)


def project_t(full, weight, out, tile):
    def body(index, carry):
        span = pl.ds(pl.multiple_of(index * tile, tile), tile)
        out[:, span] = dot_nt(flat(full), weight[span, :]).astype(BF16)
        return carry
    lax.fori_loop(0, out.shape[1] // tile, body, 0)


def head(ref, index):
    return ref[:, index * HEAD_DIM:(index + 1) * HEAD_DIM]


def attention(qkv, heads_out, probs=None):
    group = heads_out.shape[1] // HEAD_DIM
    seq = qkv.shape[0]
    causal = lax.broadcasted_iota(jnp.int32, (seq, seq), 0) >= lax.broadcasted_iota(jnp.int32, (seq, seq), 1)
    for index in range(group):
        scores = dot_nt(head(qkv, index), head(qkv, group)) * HEAD_DIM ** -0.5
        scores = jnp.where(causal, scores, -1e30)
        weight = jnp.exp(scores - jnp.max(scores, axis=-1, keepdims=True))
        prob = weight / jnp.sum(weight, axis=-1, keepdims=True)
        if probs is not None:
            probs[index] = prob
        heads_out[:, index * HEAD_DIM:(index + 1) * HEAD_DIM] = dot_nn(prob.astype(BF16), head(qkv, group + 1)).astype(BF16)


def attention_pull(qkv, probs, d_heads, d_qkv):
    group = d_heads.shape[1] // HEAD_DIM
    d_keys = d_values = None
    for index in range(group):
        d_out, prob = head(d_heads, index), probs[index]
        d_prob = dot_nt(d_out, head(qkv, group + 1))
        d_value = dot_tn(prob.astype(BF16), d_out)
        d_score = (prob * (d_prob - jnp.sum(d_prob * prob, axis=-1, keepdims=True)) * HEAD_DIM ** -0.5).astype(BF16)
        d_qkv[:, index * HEAD_DIM:(index + 1) * HEAD_DIM] = dot_nn(d_score, head(qkv, group)).astype(BF16)
        d_key = dot_tn(d_score, head(qkv, index))
        d_keys = d_key if d_keys is None else d_keys + d_key
        d_values = d_value if d_values is None else d_values + d_value
    d_qkv[:, group * HEAD_DIM:(group + 1) * HEAD_DIM] = d_keys.astype(BF16)
    d_qkv[:, (group + 1) * HEAD_DIM:(group + 2) * HEAD_DIM] = d_values.astype(BF16)


def load(src, dst, sem):
    copy = pltpu.make_async_copy(src, dst, sem)
    copy.start()
    return copy


def forward_kernel(layer, chips, hidden, gain_attn, gain_mlp, w_qkv, w_out, w_gate, w_up, w_down, out,
                   wq, wo, wg, wu, wd, full_in, full_mid, qkv, heads_out, gate, part, near, relay, from_left, from_right,
                   load_sem, send_sem, recv_sem):
    links = Links(chips, send_sem, recv_sem)
    pairs = ((w_qkv, wq), (w_out, wo), (w_gate, wg), (w_up, wu), (w_down, wd))
    loads = [load(src.at[layer], dst, load_sem.at[index]) for index, (src, dst) in enumerate(pairs)]
    row = pl.ds(layer, 1)
    full_in[links.x, links.c] = rms_norm(hidden[...], gain_attn[row, :])
    links.enter((links.right, links.left, links.sib))
    gather = Gather(links, full_in)
    gather.relay()
    gather.finish()
    loads[0].wait()
    project(full_in, wq, qkv, HEAD_DIM)
    attention(qkv, heads_out)
    loads[1].wait()
    total = reduce_scatter(links, lambda col, width: dot_nn(heads_out[...], wo[:, pl.ds(col, width)]),
                           part, near.at[0], relay.at[0], from_left.at[0], from_right.at[0])
    hidden_mid = hidden[...] + total.astype(BF16)
    full_mid[links.x, links.c] = rms_norm(hidden_mid, gain_mlp[row, :])
    out[...] = hidden_mid
    links.drain()
    gather = Gather(links, full_mid)
    gather.relay()
    gather.finish()
    for copy in loads[2:]:
        copy.wait()
    tile = 2 * HEAD_DIM

    def body(index, carry):
        cols = pl.ds(pl.multiple_of(index * tile, tile), tile)
        gate_act = dot_nn(flat(full_mid), wg[:, cols]).astype(BF16).astype(F32)
        up_act = dot_nn(flat(full_mid), wu[:, cols]).astype(BF16).astype(F32)
        gate[:, cols] = (gate_act * jax.nn.sigmoid(gate_act) * up_act).astype(BF16)
        return carry
    lax.fori_loop(0, gate.shape[1] // tile, body, 0)
    total = reduce_scatter(links, lambda col, width: dot_nn(gate[...], wd[:, pl.ds(col, width)]),
                           part, near.at[1], relay.at[1], from_left.at[1], from_right.at[1])
    out[...] = out[...] + total.astype(BF16)
    links.drain()


def backward_kernel(layer, chips, final, hidden, d_out, gain_attn, gain_mlp, w_qkv, w_out, w_gate, w_up, w_down, carried,
                    d_hidden, gains, o_in, o_mid, o_down, o_attn, o_act, o_gate, o_up, o_heads, o_qkv,
                    wq, wo, wg, wu, wd, full_in, full_mid, full_down, full_attn, qkv, heads_out, act, d_gate, d_up, d_heads, d_qkv,
                    probs, part, near, relay, from_left, from_right, gain_mid, gain_last,
                    load_sem, save_sem, send_sem, recv_sem):
    links = Links(chips, send_sem, recv_sem)
    x, c = links.x, links.c
    pairs = ((w_qkv, wq), (w_out, wo), (w_gate, wg), (w_up, wu), (w_down, wd))
    loads = [load(src.at[layer], dst, load_sem.at[index]) for index, (src, dst) in enumerate(pairs)]
    saves = []

    def save(src, dst):
        saves.append(load(src, dst, save_sem.at[len(saves)]))

    row = pl.ds(layer, 1)
    full_in[x, c] = rms_norm(hidden[...], gain_attn[row, :])
    full_down[x, c] = d_out[...]
    links.enter(links.others() if final else (links.right, links.left, links.sib))
    gather = Gather(links, full_in)
    gather_down = Gather(links, full_down)
    gather.relay()
    gather.finish()
    loads[0].wait()
    project(full_in, wq, qkv, HEAD_DIM)
    gather_down.relay()
    attention(qkv, heads_out, probs)
    gather_down.finish()
    save(full_in, o_in)
    save(full_down, o_down)
    save(heads_out, o_heads)
    loads[1].wait()

    def gated():
        loads[4].wait()
        project_t(full_down, wd, act, 2 * HEAD_DIM)

    total = reduce_scatter(links, lambda col, width: dot_nn(heads_out[...], wo[:, pl.ds(col, width)]),
                           part, near.at[0], relay.at[0], from_left.at[0], from_right.at[0], [gated])
    hidden_mid = hidden[...] + total.astype(BF16)
    d_hidden[...] = hidden_mid
    full_mid[x, c] = rms_norm(hidden_mid, gain_mlp[row, :])
    links.drain()
    gather = Gather(links, full_mid)
    gather.relay()
    gather.finish()
    save(full_mid, o_mid)
    loads[2].wait()
    loads[3].wait()
    tile = 2 * HEAD_DIM

    def body(index, carry):
        cols = pl.ds(pl.multiple_of(index * tile, tile), tile)
        gate_act = dot_nn(flat(full_mid), wg[:, cols]).astype(BF16).astype(F32)
        up_act = dot_nn(flat(full_mid), wu[:, cols]).astype(BF16).astype(F32)
        sig = jax.nn.sigmoid(gate_act)
        silu = gate_act * sig
        d_act = act[:, cols].astype(F32)
        d_up[:, cols] = (d_act * silu).astype(BF16)
        d_gate[:, cols] = (d_act * up_act * (sig + silu * (1.0 - sig))).astype(BF16)
        act[:, cols] = (silu * up_act).astype(BF16)
        return carry
    lax.fori_loop(0, act.shape[1] // tile, body, 0)
    save(act, o_act)
    save(d_gate, o_gate)
    save(d_up, o_up)

    def mid_product(col, width):
        return dot_nt(d_gate[...], wg[pl.ds(col, width), :]) + dot_nt(d_up[...], wu[pl.ds(col, width), :])

    total = reduce_scatter(links, mid_product, part, near.at[1], relay.at[1], from_left.at[1], from_right.at[1])
    d_norm, d_gain = rms_norm_pull(d_hidden[...], gain_mlp[row, :], total.astype(BF16))
    d_mid = d_out[...] + d_norm
    full_attn[x, c] = d_mid
    d_hidden[...] = d_mid
    links.drain()
    gather = Gather(links, full_attn)
    lanes = gain_mid.shape[2]
    done = carried.shape[0] if final else 0

    def put(ref, index, value):
        for line in range(lanes):
            ref[index, line:line + 1, :] = value[:, line * HEAD_DIM:(line + 1) * HEAD_DIM]

    mine = gain_mid.at[links.me]
    if final:
        mine[0:done] = carried[...]
    put(mine, done, d_gain)
    gather.relay()
    gather.finish()
    save(full_attn, o_attn)
    shares = []
    if final:
        shares = [links.copy(mine, mine, peer) for peer in links.others()]
    project_t(full_attn, wo, d_heads, HEAD_DIM)
    attention_pull(qkv, probs, d_heads, d_qkv)
    save(d_qkv, o_qkv)
    total = reduce_scatter(links, lambda col, width: dot_nt(d_qkv[...], wq[pl.ds(col, width), :]),
                           part, near.at[2], relay.at[2], from_left.at[2], from_right.at[2])
    d_norm, d_gain = rms_norm_pull(hidden[...], gain_attn[row, :], total.astype(BF16))
    mine_last = gain_last.at[links.me]
    put(mine_last, 0, d_gain)
    if final:
        shares += [links.copy(mine_last, mine_last, peer) for peer in links.others()]
    d_hidden[...] = d_hidden[...] + d_norm
    if final:
        for copy in shares:
            copy.wait_recv()
        size = chips * CORES
        gains[0:done + 1] = sum([gain_mid[peer] for peer in range(1, size)], gain_mid[0])
        gains[done + 1:done + 2] = sum([gain_last[peer] for peer in range(1, size)], gain_last[0])
    else:
        gains[0:1] = mine[...]
        gains[1:2] = mine_last[...]
    for copy in saves:
        copy.wait()
    links.drain()


def grads_kernel(layer, fresh, *refs):
    ins, rest = refs[:9], refs[9:]
    if not fresh:
        rest = rest[5:]
    outs, rest = rest[:5], rest[5:]
    full_in, full_mid, full_down, full_attn, act, d_gate, d_up, heads_out, d_qkv = rest[:9]
    stage, load_sem, save_sem = rest[9:]
    loads = [load(src, dst, load_sem.at[index]) for index, (src, dst) in enumerate(zip(ins, rest[:9]))]
    tile = stage.shape[1]
    wide = 1024
    jobs = ((act, full_down, outs[4], (4, 2)), (full_mid, d_gate, outs[2], (1, 5)), (full_mid, d_up, outs[3], (6,)),
            (heads_out, full_attn, outs[1], (7, 3)), (full_in, d_qkv, outs[0], (0, 8)))
    for left, right, out, needs in jobs:
        for index in needs:
            loads[index].wait()
        rows, cols = out.shape[1], out.shape[2]
        size = min(tile, rows)
        if rows % size:
            size = size // 2
        count = rows // size

        def slot_copy(slot, start, size=size, cols=cols, out=out):
            return pltpu.make_async_copy(stage.at[slot, pl.ds(0, size), pl.ds(0, cols)],
                                         out.at[layer, pl.ds(start, size), :], save_sem.at[slot])

        def body(index, carry, left=left, right=right, size=size, cols=cols, slot_copy=slot_copy):
            slot = lax.rem(index, 2)
            start = pl.multiple_of(index * size, size)

            @pl.when(index >= 2)
            def _():
                slot_copy(slot, start).wait()
            span = pl.ds(start, size)
            if len(left.shape) == 4:
                chips, cores, some, _ = left.shape
                turned = left[:, :, :, span].reshape(chips * cores * some, size)
            else:
                turned = left[:, span]
            turned = turned.T
            for col in range(0, cols, wide):
                width = min(wide, cols - col)
                if len(right.shape) == 4:
                    chips, cores, some, _ = right.shape
                    piece = right[:, :, :, col:col + width].reshape(chips * cores * some, width)
                else:
                    piece = right[:, col:col + width]
                stage[slot, 0:size, col:col + width] = dot_nn(turned, piece).astype(BF16)
            slot_copy(slot, start).start()
            return carry
        lax.fori_loop(0, count, body, 0)
        for slot in range(min(2, count)):
            slot_copy(slot, 0).wait()


def vmem(*shape, dtype=BF16):
    return pltpu.VMEM(shape, dtype)


def solution(mesh):
    chips = mesh.shape['tp'] // CORES
    row_spec = P(('dp', 'tp'), None)
    col_spec = P(None, None, 'tp')
    mid_spec = P(None, 'tp', None)
    in_specs = (row_spec, row_spec, P(None, None), P(None, None), col_spec, mid_spec, col_spec, col_spec, mid_spec)
    out_specs = (row_spec, row_spec, P('dp', None, 'tp'), P('dp', 'tp', None), P('dp', None, 'tp'), P('dp', None, 'tp'), P('dp', 'tp', None), P('dp', None), P('dp', None))

    def device_step(x, grad_y, gain_attn, gain_mlp, w_qkv, w_out, w_gate, w_up, w_down):
        layers, width, qkv_cols = w_qkv.shape
        head_cols, units, rows = w_out.shape[1], w_gate.shape[2], x.shape[0]
        group = head_cols // HEAD_DIM
        seq = chips * CORES * rows
        lanes = width // HEAD_DIM
        full = (chips, CORES, rows, width)
        weights = (w_qkv, w_out, w_gate, w_up, w_down)
        weight_bufs = [vmem(*weight.shape[1:]) for weight in weights]

        def ring_bufs(uses):
            return [vmem(*full, dtype=F32), vmem(uses, chips, rows, width, dtype=F32), vmem(uses, 2, rows, width // 2, dtype=F32),
                    vmem(uses, rows, width, dtype=F32), vmem(uses, rows, width, dtype=F32)]

        def dma(count):
            return pltpu.SemaphoreType.DMA((count,))

        def params(ident):
            return pltpu.CompilerParams(collective_id=ident, has_side_effects=True, vmem_limit_bytes=VMEM_LIMIT)

        def forward(layer, hidden):
            copies = 2 * 13 + 2 * 8 * STEPS
            return pl.pallas_call(
                functools.partial(forward_kernel, layer, chips),
                out_shape=jax.ShapeDtypeStruct(hidden.shape, BF16),
                in_specs=[VMEM_SPEC] * 3 + [ANY] * 5,
                out_specs=VMEM_SPEC,
                scratch_shapes=weight_bufs + [vmem(*full), vmem(*full), vmem(seq, qkv_cols), vmem(seq, head_cols), vmem(seq, units)]
                + ring_bufs(2) + [dma(5), dma(copies), dma(copies)],
                compiler_params=params(layer), name=f'forward_{layer}',
            )(hidden, gain_attn, gain_mlp, *weights)

        def backward(layer, hidden, d_out, carried):
            final = layer == 0
            peers = chips * CORES - 1
            copies = 4 * 13 + 3 * 8 * STEPS + 2 * peers
            done = carried.shape[0] if final else 0
            factor = lambda *shape: jax.ShapeDtypeStruct(shape, BF16)
            return pl.pallas_call(
                functools.partial(backward_kernel, layer, chips, final),
                out_shape=[factor(*hidden.shape), jax.ShapeDtypeStruct((done + 2, lanes, HEAD_DIM), F32)] + [factor(*full)] * 4
                + [factor(seq, units)] * 3 + [factor(seq, head_cols), factor(seq, qkv_cols)],
                in_specs=[VMEM_SPEC] * 4 + [ANY] * 5 + [VMEM_SPEC],
                out_specs=[VMEM_SPEC] * 2 + [ANY] * 9,
                scratch_shapes=weight_bufs + [vmem(*full)] * 4
                + [vmem(seq, qkv_cols), vmem(seq, head_cols), vmem(seq, units), vmem(seq, units), vmem(seq, units),
                   vmem(seq, head_cols), vmem(seq, qkv_cols), vmem(group, seq, seq, dtype=F32)] + ring_bufs(3)
                + [vmem(chips * CORES, done + 1, lanes, HEAD_DIM, dtype=F32), vmem(chips * CORES, 1, lanes, HEAD_DIM, dtype=F32),
                   dma(5), dma(9), dma(copies), dma(copies)],
                compiler_params=params(layers + layer), name=f'backward_{layer}',
            )(hidden, d_out, gain_attn, gain_mlp, *weights, carried)

        grad_shapes = [jax.ShapeDtypeStruct(weight.shape, BF16) for weight in weights]

        def grads(layer, factors, into):
            given = [] if into is None else list(into)
            return pl.pallas_call(
                functools.partial(grads_kernel, layer, into is None),
                out_shape=grad_shapes,
                in_specs=[ANY] * (len(factors) + len(given)),
                out_specs=[ANY] * 5,
                scratch_shapes=[vmem(*factor.shape) for factor in factors] + [vmem(2, 256, width), dma(len(factors)), dma(2)],
                input_output_aliases={len(factors) + index: index for index in range(len(given))},
                compiler_params=pltpu.CompilerParams(vmem_limit_bytes=VMEM_LIMIT), name=f'grads_{layer}',
            )(*factors, *given)

        kept = [x]
        for layer in range(layers):
            kept.append(forward(layer, kept[-1]))
        d_hidden, out_grads, partial_gains = grad_y, None, []
        for layer in reversed(range(layers)):
            carried = jnp.concatenate(partial_gains) if partial_gains else jnp.zeros((1, lanes, HEAD_DIM), F32)
            d_hidden, gains, *factors = backward(layer, kept[layer], d_hidden, carried)
            partial_gains.append(gains)
            out_grads = grads(layer, factors, out_grads)
            d_hidden, *out_grads = lax.optimization_barrier((d_hidden, *out_grads))
        order = gains.reshape(layers, 2, width)[::-1]
        return (kept[-1], d_hidden, *out_grads, order[:, 1], order[:, 0])

    return jax.shard_map(device_step, mesh=mesh, in_specs=in_specs, out_specs=out_specs, check_vma=False)
```

```python
import functools

import jax
import jax.numpy as jnp
from jax import lax
from jax.experimental import pallas as pl
from jax.experimental.pallas import tpu as pltpu
from jax.sharding import PartitionSpec as P

HEAD_DIM = 128
NORM_EPS = 1e-5
CORES = 2
MESH = pl.DeviceIdType.MESH
F32 = jnp.float32
BF16 = jnp.bfloat16
VMEM_LIMIT = 66_000_000
SPLIT = (2, 5, 5)
STEPS = len(SPLIT)
ANY = pl.BlockSpec(memory_space=pltpu.HBM)
VMEM_SPEC = pl.BlockSpec(memory_space=pltpu.VMEM)


def dot_nn(a, b):
    return lax.dot_general(a, b, (((1,), (0,)), ((), ())), preferred_element_type=F32)


def dot_nt(a, b):
    return lax.dot_general(a, b, (((1,), (1,)), ((), ())), preferred_element_type=F32)


def dot_tn(a, b):
    return lax.dot_general(a, b, (((0,), (0,)), ((), ())), preferred_element_type=F32)


class Links:
    def __init__(self, chips, send_sem, recv_sem):
        self.me = lax.axis_index('tp')
        self.chips = chips
        self.x = lax.div(self.me, CORES)
        self.c = lax.rem(self.me, CORES)
        self.xr = lax.rem(self.x + 1, chips)
        self.xl = lax.rem(self.x + chips - 1, chips)
        self.xo = lax.rem(self.x + 2, chips)
        self.right = self.xr * CORES + self.c
        self.left = self.xl * CORES + self.c
        self.sib = self.x * CORES + 1 - self.c
        self.send_sem, self.recv_sem, self.used, self.pending = send_sem, recv_sem, 0, []

    def enter(self, peers):
        barrier = pltpu.get_barrier_semaphore()
        for peer in peers:
            pl.semaphore_signal(barrier, inc=1, device_id={'tp': peer}, device_id_type=MESH)
        pl.semaphore_wait(barrier, len(peers))

    def others(self):
        size = self.chips * CORES
        return [lax.rem(self.me + step, size) for step in range(1, size)]

    def copy(self, src, dst, peer):
        copy = pltpu.make_async_remote_copy(
            src_ref=src, dst_ref=dst, send_sem=self.send_sem.at[self.used], recv_sem=self.recv_sem.at[self.used],
            device_id={'tp': peer}, device_id_type=MESH)
        self.used += 1
        copy.start()
        self.pending.append(copy)
        return copy

    def drain(self):
        for copy in self.pending:
            copy.wait_send()
        self.pending = []


class Gather:
    def __init__(self, links, full):
        self.links, self.full = links, full
        self.half = full.shape[3] // 2
        part_a, part_b = pl.ds(0, self.half), pl.ds(self.half, self.half)
        x, c = links.x, links.c
        self.a, self.b = part_a, part_b
        self.right_a = self.send(x, part_a, links.right)
        self.left_b = self.send(x, part_b, links.left)
        self.right_b = self.send(x, part_b, links.right)
        self.left_a = self.send(x, part_a, links.left)
        self.near = [links.copy(full.at[x, c], full.at[x, c], links.sib)]

    def send(self, chip, part, peer):
        ref = self.full.at[chip, self.links.c, :, part]
        return self.links.copy(ref, ref, peer)

    @jax.named_scope('gather')
    def relay(self):
        links = self.links
        self.right_a.wait_recv()
        relay_a = self.send(links.xl, self.a, links.right)
        self.near.append(self.send(links.xl, self.a, links.sib))
        self.left_b.wait_recv()
        relay_b = self.send(links.xr, self.b, links.left)
        self.near.append(self.send(links.xr, self.b, links.sib))
        self.right_b.wait_recv()
        self.near.append(self.send(links.xl, self.b, links.sib))
        self.left_a.wait_recv()
        self.near.append(self.send(links.xr, self.a, links.sib))
        self.far = (relay_a, relay_b)

    @jax.named_scope('finish')
    def finish(self):
        links = self.links
        self.far[0].wait_recv()
        self.near.append(self.send(links.xo, self.a, links.sib))
        self.far[1].wait_recv()
        self.near.append(self.send(links.xo, self.b, links.sib))
        for copy in self.near:
            copy.wait_recv()


def reduce_scatter(links, product, part, near, relay, from_left, from_right, fillers=()):
    chips, _, rows, cols = part.shape
    half = cols // 2
    unit = half // sum(SPLIT)
    starts = [unit * sum(SPLIT[:step]) for step in range(STEPS)]
    x, c, xr, xl, xo = links.x, links.c, links.xr, links.xl, links.xo
    fillers = list(fillers)
    swap, first, last = [None] * STEPS, [None] * STEPS, []

    def spans(step):
        width = unit * SPLIT[step]
        return pl.ds(starts[step], width), pl.ds(half + starts[step], width)

    for step in range(STEPS + 2):
        if step < STEPS:
            swap[step] = []
            for span in spans(step):
                with jax.named_scope(f'product{step}'):
                    part[:, :, :, span] = product(span.start, span.size).reshape(chips, CORES, rows, span.size)
                swap[step].append(links.copy(part.at[:, 1 - c, :, span], near.at[:, :, span], links.sib))
        elif fillers:
            with jax.named_scope(f'filler{step}'):
                fillers.pop(0)()
        if 0 <= step - 1 < STEPS:
            done = step - 1
            span_a, span_b = spans(done)
            with jax.named_scope(f'swap{done}'):
                for copy, span in zip(swap[done], (span_a, span_b)):
                    copy.wait_recv()
                    part[:, c, :, span] = part[:, c, :, span] + near[:, :, span]
            first[done] = (
                links.copy(part.at[xo, c, :, span_a], relay.at[0, :, span_a], links.right),
                links.copy(part.at[xo, c, :, span_b], relay.at[1, :, span_a], links.left))
            last.append(links.copy(part.at[xr, c, :, span_b], from_left.at[:, span_b], links.right))
            last.append(links.copy(part.at[xl, c, :, span_a], from_right.at[:, span_a], links.left))
        if 0 <= step - 2 < STEPS:
            done = step - 2
            span_a, span_b = spans(done)
            with jax.named_scope(f'relay{done}'):
                first[done][0].wait_recv()
                part[xr, c, :, span_a] = part[xr, c, :, span_a] + relay[0, :, span_a]
                last.append(links.copy(part.at[xr, c, :, span_a], from_left.at[:, span_a], links.right))
                first[done][1].wait_recv()
                part[xl, c, :, span_b] = part[xl, c, :, span_b] + relay[1, :, span_a]
                last.append(links.copy(part.at[xl, c, :, span_b], from_right.at[:, span_b], links.left))
    for filler in fillers:
        filler()
    with jax.named_scope('last'):
        for copy in last:
            copy.wait_recv()
    return part[x, c] + from_left[...] + from_right[...]


def rms_norm(hidden, gain):
    hidden_f = hidden.astype(F32)
    inv_rms = lax.rsqrt(jnp.mean(hidden_f * hidden_f, axis=-1, keepdims=True) + NORM_EPS)
    return (hidden_f * inv_rms * gain).astype(BF16)


def rms_norm_pull(hidden, gain, cotangent):
    hidden_f, cot = hidden.astype(F32), cotangent.astype(F32)
    inv_rms = lax.rsqrt(jnp.mean(hidden_f * hidden_f, axis=-1, keepdims=True) + NORM_EPS)
    scaled = cot * gain
    dot = jnp.mean(scaled * hidden_f, axis=-1, keepdims=True)
    d_hidden = scaled * inv_rms - hidden_f * (inv_rms * inv_rms * inv_rms * dot)
    return d_hidden.astype(BF16), jnp.sum(cot * (hidden_f * inv_rms), axis=0, keepdims=True)


def flat(ref):
    chips, cores, rows, cols = ref.shape
    return ref[...].reshape(chips * cores * rows, cols)


def project(full, weight, out, tile):
    def body(index, carry):
        cols = pl.ds(pl.multiple_of(index * tile, tile), tile)
        out[:, cols] = dot_nn(flat(full), weight[:, cols]).astype(BF16)
        return carry
    lax.fori_loop(0, out.shape[1] // tile, body, 0)


def project_t(full, weight, out, tile):
    def body(index, carry):
        span = pl.ds(pl.multiple_of(index * tile, tile), tile)
        out[:, span] = dot_nt(flat(full), weight[span, :]).astype(BF16)
        return carry
    lax.fori_loop(0, out.shape[1] // tile, body, 0)


def head(ref, index):
    return ref[:, index * HEAD_DIM:(index + 1) * HEAD_DIM]


def attention(qkv, heads_out, probs=None):
    group = heads_out.shape[1] // HEAD_DIM
    seq = qkv.shape[0]
    causal = lax.broadcasted_iota(jnp.int32, (seq, seq), 0) >= lax.broadcasted_iota(jnp.int32, (seq, seq), 1)
    for index in range(group):
        scores = dot_nt(head(qkv, index), head(qkv, group)) * HEAD_DIM ** -0.5
        scores = jnp.where(causal, scores, -1e30)
        weight = jnp.exp(scores - jnp.max(scores, axis=-1, keepdims=True))
        prob = weight / jnp.sum(weight, axis=-1, keepdims=True)
        if probs is not None:
            probs[index] = prob
        heads_out[:, index * HEAD_DIM:(index + 1) * HEAD_DIM] = dot_nn(prob.astype(BF16), head(qkv, group + 1)).astype(BF16)


def attention_pull(qkv, probs, d_heads, d_qkv):
    group = d_heads.shape[1] // HEAD_DIM
    d_keys = d_values = None
    for index in range(group):
        d_out, prob = head(d_heads, index), probs[index]
        d_prob = dot_nt(d_out, head(qkv, group + 1))
        d_value = dot_tn(prob.astype(BF16), d_out)
        d_score = (prob * (d_prob - jnp.sum(d_prob * prob, axis=-1, keepdims=True)) * HEAD_DIM ** -0.5).astype(BF16)
        d_qkv[:, index * HEAD_DIM:(index + 1) * HEAD_DIM] = dot_nn(d_score, head(qkv, group)).astype(BF16)
        d_key = dot_tn(d_score, head(qkv, index))
        d_keys = d_key if d_keys is None else d_keys + d_key
        d_values = d_value if d_values is None else d_values + d_value
    d_qkv[:, group * HEAD_DIM:(group + 1) * HEAD_DIM] = d_keys.astype(BF16)
    d_qkv[:, (group + 1) * HEAD_DIM:(group + 2) * HEAD_DIM] = d_values.astype(BF16)


def load(src, dst, sem):
    copy = pltpu.make_async_copy(src, dst, sem)
    copy.start()
    return copy


def forward_kernel(layers, chips, hidden, gain_attn, gain_mlp, w_qkv, w_out, w_gate, w_up, w_down, outs,
                   wq, wo, wg, wu, wd, full_in, full_mid, qkv, heads_out, act, part, near, relay, from_left, from_right,
                   state, load_sem, send_sem, recv_sem):
    links = Links(chips, send_sem, recv_sem)
    state[...] = hidden[...]
    links.enter((links.right, links.left, links.sib))
    pairs = ((w_qkv, wq), (w_out, wo), (w_gate, wg), (w_up, wu), (w_down, wd))

    def one_layer(layer, carry):
        links.used = 0
        row = pl.ds(layer, 1)
        loads = [load(src.at[layer], dst, load_sem.at[index]) for index, (src, dst) in enumerate(pairs)]
        with jax.named_scope('norm_in'):
            full_in[links.x, links.c] = rms_norm(state[...], gain_attn[row, :])
        gather = Gather(links, full_in)
        gather.relay()
        gather.finish()
        loads[0].wait()
        with jax.named_scope('qkv'):
            project(full_in, wq, qkv, HEAD_DIM)
        with jax.named_scope('attention'):
            attention(qkv, heads_out)
        loads[1].wait()
        total = reduce_scatter(links, lambda col, width: dot_nn(heads_out[...], wo[:, pl.ds(col, width)]),
                               part, near.at[0], relay.at[0], from_left.at[0], from_right.at[0])
        with jax.named_scope('norm_mid'):
            hidden_mid = state[...] + total.astype(BF16)
            full_mid[links.x, links.c] = rms_norm(hidden_mid, gain_mlp[row, :])
            state[...] = hidden_mid
        links.drain()
        gather = Gather(links, full_mid)
        gather.relay()
        gather.finish()
        for copy in loads[2:]:
            copy.wait()
        tile = 2 * HEAD_DIM

        def body(index, carry):
            cols = pl.ds(pl.multiple_of(index * tile, tile), tile)
            gate_act = dot_nn(flat(full_mid), wg[:, cols]).astype(BF16).astype(F32)
            up_act = dot_nn(flat(full_mid), wu[:, cols]).astype(BF16).astype(F32)
            act[:, cols] = (gate_act * jax.nn.sigmoid(gate_act) * up_act).astype(BF16)
            return carry
        with jax.named_scope('gate_up'):
            lax.fori_loop(0, act.shape[1] // tile, body, 0)
        total = reduce_scatter(links, lambda col, width: dot_nn(act[...], wd[:, pl.ds(col, width)]),
                               part, near.at[1], relay.at[1], from_left.at[1], from_right.at[1])
        state[...] = state[...] + total.astype(BF16)
        outs[layer] = state[...]
        links.drain()
        return carry
    lax.fori_loop(0, layers, one_layer, 0)


def turn(src, dst):
    seq = dst.shape[1]
    tile = HEAD_DIM if dst.shape[0] % (2 * HEAD_DIM) else 2 * HEAD_DIM

    def body(index, carry):
        span = pl.ds(pl.multiple_of(index * tile, tile), tile)
        block = src[:, :, :, span].reshape(seq, tile) if len(src.shape) == 4 else src[:, span]
        dst[span, :] = block.T
        return carry
    lax.fori_loop(0, dst.shape[0] // tile, body, 0)


def backward_kernel(layer, chips, final, hidden, d_out, gain_attn, gain_mlp, w_qkv, w_out, w_gate, w_up, w_down, carried,
                    d_hidden, gains, o_in, o_mid, o_down, o_attn, o_act, o_gate, o_up, o_heads, o_qkv,
                    wq, wo, wg, wu, wd, full_in, full_mid, full_down, full_attn, qkv, heads_out, act, d_gate, d_up, d_heads, d_qkv,
                    probs, t_in, t_mid, t_act, t_heads, part, near, relay, from_left, from_right, gain_mid, gain_last,
                    load_sem, save_sem, send_sem, recv_sem):
    links = Links(chips, send_sem, recv_sem)
    x, c = links.x, links.c
    pairs = ((w_qkv, wq), (w_out, wo), (w_gate, wg), (w_up, wu), (w_down, wd))
    loads = [load(src.at[layer], dst, load_sem.at[index]) for index, (src, dst) in enumerate(pairs)]
    saves = []

    def save(src, dst):
        saves.append(load(src, dst, save_sem.at[len(saves)]))

    row = pl.ds(layer, 1)
    full_in[x, c] = rms_norm(hidden[...], gain_attn[row, :])
    full_down[x, c] = d_out[...]
    links.enter(links.others() if final else (links.right, links.left, links.sib))
    gather = Gather(links, full_in)
    gather_down = Gather(links, full_down)
    gather.relay()
    gather.finish()
    loads[0].wait()
    with jax.named_scope('qkv'):
        project(full_in, wq, qkv, HEAD_DIM)
    gather_down.relay()
    with jax.named_scope('attention'):
        attention(qkv, heads_out, probs)
    gather_down.finish()
    save(full_down, o_down)
    loads[1].wait()

    def gated():
        loads[4].wait()
        project_t(full_down, wd, act, 2 * HEAD_DIM)

    def turn_in():
        turn(full_in, t_in)
        turn(heads_out, t_heads)
        save(t_in, o_in)
        save(t_heads, o_heads)

    def turn_mid():
        turn(full_mid, t_mid)
        turn(act, t_act)
        save(t_mid, o_mid)
        save(t_act, o_act)

    total = reduce_scatter(links, lambda col, width: dot_nn(heads_out[...], wo[:, pl.ds(col, width)]),
                           part, near.at[0], relay.at[0], from_left.at[0], from_right.at[0], [gated, turn_in])
    hidden_mid = hidden[...] + total.astype(BF16)
    d_hidden[...] = hidden_mid
    full_mid[x, c] = rms_norm(hidden_mid, gain_mlp[row, :])
    links.drain()
    gather = Gather(links, full_mid)
    gather.relay()
    gather.finish()
    loads[2].wait()
    loads[3].wait()
    tile = 2 * HEAD_DIM

    def body(index, carry):
        cols = pl.ds(pl.multiple_of(index * tile, tile), tile)
        gate_act = dot_nn(flat(full_mid), wg[:, cols]).astype(BF16).astype(F32)
        up_act = dot_nn(flat(full_mid), wu[:, cols]).astype(BF16).astype(F32)
        sig = jax.nn.sigmoid(gate_act)
        silu = gate_act * sig
        d_act = act[:, cols].astype(F32)
        d_up[:, cols] = (d_act * silu).astype(BF16)
        d_gate[:, cols] = (d_act * up_act * (sig + silu * (1.0 - sig))).astype(BF16)
        act[:, cols] = (silu * up_act).astype(BF16)
        return carry
    with jax.named_scope('gate_up'):
        lax.fori_loop(0, act.shape[1] // tile, body, 0)
    save(d_gate, o_gate)
    save(d_up, o_up)

    def mid_product(col, width):
        return dot_nt(d_gate[...], wg[pl.ds(col, width), :]) + dot_nt(d_up[...], wu[pl.ds(col, width), :])

    total = reduce_scatter(links, mid_product, part, near.at[1], relay.at[1], from_left.at[1], from_right.at[1],
                           [turn_mid])
    d_norm, d_gain = rms_norm_pull(d_hidden[...], gain_mlp[row, :], total.astype(BF16))
    d_mid = d_out[...] + d_norm
    full_attn[x, c] = d_mid
    d_hidden[...] = d_mid
    links.drain()
    gather = Gather(links, full_attn)
    lanes = gain_mid.shape[2]
    done = carried.shape[0] if final else 0

    def put(ref, index, value):
        for line in range(lanes):
            ref[index, line:line + 1, :] = value[:, line * HEAD_DIM:(line + 1) * HEAD_DIM]

    mine = gain_mid.at[links.me]
    if final:
        mine[1:done + 1] = carried[...]
    put(mine, 0, d_gain)
    gather.relay()
    gather.finish()
    save(full_attn, o_attn)
    shares = []
    if final:
        shares = [links.copy(mine, mine, peer) for peer in links.others()]
    with jax.named_scope('d_heads'):
        project_t(full_attn, wo, d_heads, HEAD_DIM)
    with jax.named_scope('attention_pull'):
        attention_pull(qkv, probs, d_heads, d_qkv)
    save(d_qkv, o_qkv)
    total = reduce_scatter(links, lambda col, width: dot_nt(d_qkv[...], wq[pl.ds(col, width), :]),
                           part, near.at[2], relay.at[2], from_left.at[2], from_right.at[2])
    d_norm, d_gain = rms_norm_pull(hidden[...], gain_attn[row, :], total.astype(BF16))
    mine_last = gain_last.at[links.me]
    put(mine_last, 0, d_gain)
    if final:
        shares += [links.copy(mine_last, mine_last, peer) for peer in links.others()]
    d_hidden[...] = d_hidden[...] + d_norm
    if final:
        for copy in shares:
            copy.wait_recv()
        size = chips * CORES
        gains[1:done + 2] = sum([gain_mid[peer] for peer in range(1, size)], gain_mid[0])
        gains[0:1] = sum([gain_last[peer] for peer in range(1, size)], gain_last[0])
    else:
        gains[0:1] = mine_last[...]
        gains[1:2] = mine[...]
    for copy in saves:
        copy.wait()
    links.drain()


def grads_kernel(layer, fresh, *refs):
    ins, rest = refs[:9], refs[9:]
    if not fresh:
        rest = rest[5:]
    outs, rest = rest[:5], rest[5:]
    t_in, t_mid, full_down, full_attn, t_act, d_gate, d_up, t_heads, d_qkv = rest[:9]
    deep, tall, load_sem, save_sem = rest[9:]
    order = (4, 2, 1, 5, 6, 7, 3, 0, 8)
    loads = {index: load(ins[index], rest[index], load_sem.at[index]) for index in order}
    jobs = ((t_act, full_down, outs[4], 256, (4, 2)), (t_mid, d_gate, outs[2], 512, (1, 5)), (t_mid, d_up, outs[3], 512, (6,)),
            (t_heads, full_attn, outs[1], 192, (7, 3)), (t_in, d_qkv, outs[0], 1024, (0, 8)))
    busy = [[], []]
    for place, (left, right, out, size, needs) in enumerate(jobs):
        for index in needs:
            loads[index].wait()
        for copy in busy[place % 2]:
            copy.wait()
        rows, cols = out.shape[1], out.shape[2]
        count = rows // size
        base = 2 * (place % 2)
        stage = deep if cols > tall.shape[2] else tall

        def slot_copy(slot, start, size=size, cols=cols, out=out, stage=stage):
            return pltpu.make_async_copy(stage.at[slot, pl.ds(0, size), pl.ds(0, cols)],
                                         out.at[layer, pl.ds(start, size), :], save_sem.at[slot])

        def body(index, carry, left=left, right=right, size=size, cols=cols, slot_copy=slot_copy, base=base, stage=stage):
            slot = base + lax.rem(index, 2)
            start = pl.multiple_of(index * size, size)

            @pl.when(index >= 2)
            def _():
                slot_copy(slot, start).wait()
            turned = left[pl.ds(start, size), :]
            for col in range(0, cols, 256):
                width = min(256, cols - col)
                if len(right.shape) == 4:
                    chips, cores, some, _ = right.shape
                    piece = right[:, :, :, col:col + width].reshape(chips * cores * some, width)
                else:
                    piece = right[:, col:col + width]
                stage[slot, 0:size, col:col + width] = dot_nn(turned, piece).astype(BF16)
            slot_copy(slot, start).start()
            return carry
        lax.fori_loop(0, count, body, 0)
        busy[place % 2] = [slot_copy(base + slot, 0) for slot in range(min(2, count))]
    for copies in busy:
        for copy in copies:
            copy.wait()


def vmem(*shape, dtype=BF16):
    return pltpu.VMEM(shape, dtype)


def solution(mesh):
    chips = mesh.shape['tp'] // CORES
    row_spec = P(('dp', 'tp'), None)
    col_spec = P(None, None, 'tp')
    mid_spec = P(None, 'tp', None)
    in_specs = (row_spec, row_spec, P(None, None), P(None, None), col_spec, mid_spec, col_spec, col_spec, mid_spec)
    out_specs = (row_spec, row_spec, P('dp', None, 'tp'), P('dp', 'tp', None), P('dp', None, 'tp'), P('dp', None, 'tp'), P('dp', 'tp', None), P('dp', None), P('dp', None))

    def device_step(x, grad_y, gain_attn, gain_mlp, w_qkv, w_out, w_gate, w_up, w_down):
        layers, width, qkv_cols = w_qkv.shape
        head_cols, units, rows = w_out.shape[1], w_gate.shape[2], x.shape[0]
        group = head_cols // HEAD_DIM
        seq = chips * CORES * rows
        lanes = width // HEAD_DIM
        full = (chips, CORES, rows, width)
        weights = (w_qkv, w_out, w_gate, w_up, w_down)
        weight_bufs = [vmem(*weight.shape[1:]) for weight in weights]

        def ring_bufs(uses):
            return [vmem(*full, dtype=F32), vmem(uses, chips, rows, width, dtype=F32), vmem(uses, 2, rows, width // 2, dtype=F32),
                    vmem(uses, rows, width, dtype=F32), vmem(uses, rows, width, dtype=F32)]

        def dma(count):
            return pltpu.SemaphoreType.DMA((count,))

        def params(ident):
            return pltpu.CompilerParams(collective_id=ident, has_side_effects=True, vmem_limit_bytes=VMEM_LIMIT)

        def forward(hidden):
            copies = 2 * 13 + 2 * 8 * STEPS
            return pl.pallas_call(
                functools.partial(forward_kernel, layers, chips),
                out_shape=jax.ShapeDtypeStruct((layers, *hidden.shape), BF16),
                in_specs=[VMEM_SPEC] * 3 + [ANY] * 5,
                out_specs=VMEM_SPEC,
                scratch_shapes=weight_bufs + [vmem(*full), vmem(*full), vmem(seq, qkv_cols), vmem(seq, head_cols), vmem(seq, units)]
                + ring_bufs(2) + [vmem(*hidden.shape), dma(5), dma(copies), dma(copies)],
                compiler_params=params(layers), name='forward',
            )(hidden, gain_attn, gain_mlp, *weights)

        def backward(layer, hidden, d_out, carried):
            final = layer == 0
            peers = chips * CORES - 1
            copies = 4 * 13 + 3 * 8 * STEPS + 2 * peers
            done = carried.shape[0] if final else 0
            factor = lambda *shape: jax.ShapeDtypeStruct(shape, BF16)
            return pl.pallas_call(
                functools.partial(backward_kernel, layer, chips, final),
                out_shape=[factor(*hidden.shape), jax.ShapeDtypeStruct((done + 2, lanes, HEAD_DIM), F32)]
                + [factor(width, seq)] * 2 + [factor(*full)] * 2
                + [factor(units, seq), factor(seq, units), factor(seq, units), factor(head_cols, seq), factor(seq, qkv_cols)],
                in_specs=[VMEM_SPEC] * 4 + [ANY] * 5 + [VMEM_SPEC],
                out_specs=[VMEM_SPEC] * 2 + [ANY] * 9,
                scratch_shapes=weight_bufs + [vmem(*full)] * 4
                + [vmem(seq, qkv_cols), vmem(seq, head_cols), vmem(seq, units), vmem(seq, units), vmem(seq, units),
                   vmem(seq, head_cols), vmem(seq, qkv_cols), vmem(group, seq, seq, dtype=F32),
                   vmem(width, seq), vmem(width, seq), vmem(units, seq), vmem(head_cols, seq)] + ring_bufs(3)
                + [vmem(chips * CORES, done + 1, lanes, HEAD_DIM, dtype=F32), vmem(chips * CORES, 1, lanes, HEAD_DIM, dtype=F32),
                   dma(5), dma(9), dma(copies), dma(copies)],
                compiler_params=params(layer), name=f'backward_{layer}',
            )(hidden, d_out, gain_attn, gain_mlp, *weights, carried)

        grad_shapes = [jax.ShapeDtypeStruct(weight.shape, BF16) for weight in weights]

        def grads(layer, factors, into):
            given = [] if into is None else list(into)
            return pl.pallas_call(
                functools.partial(grads_kernel, layer, into is None),
                out_shape=grad_shapes,
                in_specs=[ANY] * (len(factors) + len(given)),
                out_specs=[ANY] * 5,
                scratch_shapes=[vmem(*factor.shape) for factor in factors] + [vmem(4, 256, width), vmem(4, 1024, units), dma(len(factors)), dma(4)],
                input_output_aliases={len(factors) + index: index for index in range(len(given))},
                compiler_params=pltpu.CompilerParams(vmem_limit_bytes=VMEM_LIMIT), name=f'grads_{layer}',
            )(*factors, *given)

        layer_outs = forward(x)
        kept = [x] + [layer_outs[layer] for layer in range(layers)]
        d_hidden, out_grads, partial_gains = grad_y, None, []
        for layer in reversed(range(layers)):
            carried = jnp.concatenate(partial_gains[::-1]) if partial_gains else jnp.zeros((1, lanes, HEAD_DIM), F32)
            d_hidden, gains, *factors = backward(layer, kept[layer], d_hidden, carried)
            partial_gains.append(gains)
            out_grads = grads(layer, factors, out_grads)
            d_hidden, *out_grads = lax.optimization_barrier((d_hidden, *out_grads))
        pairs = gains.reshape(layers, 2, width)
        return (kept[-1], d_hidden, *out_grads, pairs[:, 0], pairs[:, 1])

    return jax.shard_map(device_step, mesh=mesh, in_specs=in_specs, out_specs=out_specs, check_vma=False)
```

```python
import functools

import jax
import jax.numpy as jnp
from jax import lax
from jax.experimental import pallas as pl
from jax.experimental.pallas import tpu as pltpu
from jax.sharding import PartitionSpec as P

HEAD_DIM = 128
NORM_EPS = 1e-5
CORES = 2
MESH = pl.DeviceIdType.MESH
F32 = jnp.float32
BF16 = jnp.bfloat16
VMEM_LIMIT = 66_000_000
SPLIT = (1, 3, 4, 4)
STEPS = len(SPLIT)
ANY = pl.BlockSpec(memory_space=pltpu.HBM)
VMEM_SPEC = pl.BlockSpec(memory_space=pltpu.VMEM)


def dot_nn(a, b):
    return lax.dot_general(a, b, (((1,), (0,)), ((), ())), preferred_element_type=F32)


def dot_nt(a, b):
    return lax.dot_general(a, b, (((1,), (1,)), ((), ())), preferred_element_type=F32)


def dot_tn(a, b):
    return lax.dot_general(a, b, (((0,), (0,)), ((), ())), preferred_element_type=F32)


class Links:
    def __init__(self, chips, send_sem, recv_sem):
        self.me = lax.axis_index('tp')
        self.chips = chips
        self.x = lax.div(self.me, CORES)
        self.c = lax.rem(self.me, CORES)
        self.xr = lax.rem(self.x + 1, chips)
        self.xl = lax.rem(self.x + chips - 1, chips)
        self.xo = lax.rem(self.x + 2, chips)
        self.right = self.xr * CORES + self.c
        self.left = self.xl * CORES + self.c
        self.sib = self.x * CORES + 1 - self.c
        self.send_sem, self.recv_sem, self.used, self.pending = send_sem, recv_sem, 0, []

    def enter(self, peers):
        barrier = pltpu.get_barrier_semaphore()
        for peer in peers:
            pl.semaphore_signal(barrier, inc=1, device_id={'tp': peer}, device_id_type=MESH)
        pl.semaphore_wait(barrier, len(peers))

    def others(self):
        size = self.chips * CORES
        return [lax.rem(self.me + step, size) for step in range(1, size)]

    def copy(self, src, dst, peer):
        copy = pltpu.make_async_remote_copy(
            src_ref=src, dst_ref=dst, send_sem=self.send_sem.at[self.used], recv_sem=self.recv_sem.at[self.used],
            device_id={'tp': peer}, device_id_type=MESH)
        self.used += 1
        copy.start()
        self.pending.append(copy)
        return copy

    def drain(self):
        for copy in self.pending:
            copy.wait_send()
        self.pending = []


class Gather:
    def __init__(self, links, full):
        self.links, self.full = links, full
        self.half = full.shape[3] // 2
        part_a, part_b = pl.ds(0, self.half), pl.ds(self.half, self.half)
        x, c = links.x, links.c
        self.a, self.b = part_a, part_b
        self.right_a = self.send(x, part_a, links.right)
        self.left_b = self.send(x, part_b, links.left)
        self.right_b = self.send(x, part_b, links.right)
        self.left_a = self.send(x, part_a, links.left)
        self.near = [links.copy(full.at[x, c], full.at[x, c], links.sib)]

    def send(self, chip, part, peer):
        ref = self.full.at[chip, self.links.c, :, part]
        return self.links.copy(ref, ref, peer)

    @jax.named_scope('gather')
    def relay(self):
        links = self.links
        self.right_a.wait_recv()
        relay_a = self.send(links.xl, self.a, links.right)
        self.near.append(self.send(links.xl, self.a, links.sib))
        self.left_b.wait_recv()
        relay_b = self.send(links.xr, self.b, links.left)
        self.near.append(self.send(links.xr, self.b, links.sib))
        self.far = (relay_a, relay_b)

    @jax.named_scope('finish')
    def finish(self):
        links = self.links
        self.right_b.wait_recv()
        self.near.append(self.send(links.xl, self.b, links.sib))
        self.left_a.wait_recv()
        self.near.append(self.send(links.xr, self.a, links.sib))
        self.far[0].wait_recv()
        self.near.append(self.send(links.xo, self.a, links.sib))
        self.far[1].wait_recv()
        self.near.append(self.send(links.xo, self.b, links.sib))
        for copy in self.near:
            copy.wait_recv()


def reduce_scatter(links, product, part, near, relay, from_left, from_right, fillers=()):
    chips, _, rows, cols = part.shape
    half = cols // 2
    unit = half // sum(SPLIT)
    starts = [unit * sum(SPLIT[:step]) for step in range(STEPS)]
    x, c, xr, xl, xo = links.x, links.c, links.xr, links.xl, links.xo
    fillers = list(fillers)
    swap, first, last = [None] * STEPS, [None] * STEPS, []

    def spans(step):
        width = unit * SPLIT[step]
        return pl.ds(starts[step], width), pl.ds(half + starts[step], width)

    for step in range(STEPS + 2):
        if step < STEPS:
            swap[step] = []
            for span in spans(step):
                with jax.named_scope(f'product{step}'):
                    part[:, :, :, span] = product(span.start, span.size).reshape(chips, CORES, rows, span.size)
                swap[step].append(links.copy(part.at[:, 1 - c, :, span], near.at[:, :, span], links.sib))
        elif fillers:
            with jax.named_scope(f'filler{step}'):
                fillers.pop(0)()
        if 0 <= step - 1 < STEPS:
            done = step - 1
            span_a, span_b = spans(done)
            with jax.named_scope(f'swap{done}'):
                for copy, span in zip(swap[done], (span_a, span_b)):
                    copy.wait_recv()
                    part[:, c, :, span] = part[:, c, :, span] + near[:, :, span]
            first[done] = (
                links.copy(part.at[xo, c, :, span_a], relay.at[0, :, span_a], links.right),
                links.copy(part.at[xo, c, :, span_b], relay.at[1, :, span_a], links.left))
            last.append(links.copy(part.at[xr, c, :, span_b], from_left.at[:, span_b], links.right))
            last.append(links.copy(part.at[xl, c, :, span_a], from_right.at[:, span_a], links.left))
        if 0 <= step - 2 < STEPS:
            done = step - 2
            span_a, span_b = spans(done)
            with jax.named_scope(f'relay{done}'):
                first[done][0].wait_recv()
                part[xr, c, :, span_a] = part[xr, c, :, span_a] + relay[0, :, span_a]
                last.append(links.copy(part.at[xr, c, :, span_a], from_left.at[:, span_a], links.right))
                first[done][1].wait_recv()
                part[xl, c, :, span_b] = part[xl, c, :, span_b] + relay[1, :, span_a]
                last.append(links.copy(part.at[xl, c, :, span_b], from_right.at[:, span_b], links.left))
    for filler in fillers:
        filler()
    with jax.named_scope('last'):
        for copy in last:
            copy.wait_recv()
    return part[x, c] + from_left[...] + from_right[...]


def rms_norm(hidden, gain):
    hidden_f = hidden.astype(F32)
    inv_rms = lax.rsqrt(jnp.mean(hidden_f * hidden_f, axis=-1, keepdims=True) + NORM_EPS)
    return (hidden_f * inv_rms * gain).astype(BF16)


def rms_norm_pull(hidden, gain, cotangent):
    hidden_f, cot = hidden.astype(F32), cotangent.astype(F32)
    inv_rms = lax.rsqrt(jnp.mean(hidden_f * hidden_f, axis=-1, keepdims=True) + NORM_EPS)
    scaled = cot * gain
    dot = jnp.mean(scaled * hidden_f, axis=-1, keepdims=True)
    d_hidden = scaled * inv_rms - hidden_f * (inv_rms * inv_rms * inv_rms * dot)
    return d_hidden.astype(BF16), jnp.sum(cot * (hidden_f * inv_rms), axis=0, keepdims=True)


def flat(ref):
    chips, cores, rows, cols = ref.shape
    return ref[...].reshape(chips * cores * rows, cols)


def project(full, weight, out, tile):
    def body(index, carry):
        cols = pl.ds(pl.multiple_of(index * tile, tile), tile)
        out[:, cols] = dot_nn(flat(full), weight[:, cols]).astype(BF16)
        return carry
    lax.fori_loop(0, out.shape[1] // tile, body, 0)


def project_t(full, weight, out, tile):
    def body(index, carry):
        span = pl.ds(pl.multiple_of(index * tile, tile), tile)
        out[:, span] = dot_nt(flat(full), weight[span, :]).astype(BF16)
        return carry
    lax.fori_loop(0, out.shape[1] // tile, body, 0)


def head(ref, index):
    return ref[:, index * HEAD_DIM:(index + 1) * HEAD_DIM]


def attention(qkv, heads_out, probs=None):
    group = heads_out.shape[1] // HEAD_DIM
    seq = qkv.shape[0]
    causal = lax.broadcasted_iota(jnp.int32, (seq, seq), 0) >= lax.broadcasted_iota(jnp.int32, (seq, seq), 1)
    for index in range(group):
        scores = dot_nt(head(qkv, index), head(qkv, group)) * HEAD_DIM ** -0.5
        scores = jnp.where(causal, scores, -1e30)
        weight = jnp.exp(scores - jnp.max(scores, axis=-1, keepdims=True))
        prob = weight / jnp.sum(weight, axis=-1, keepdims=True)
        if probs is not None:
            probs[index] = prob
        heads_out[:, index * HEAD_DIM:(index + 1) * HEAD_DIM] = dot_nn(prob.astype(BF16), head(qkv, group + 1)).astype(BF16)


def attention_pull(qkv, probs, d_heads, d_qkv):
    group = d_heads.shape[1] // HEAD_DIM
    d_keys = d_values = None
    for index in range(group):
        d_out, prob = head(d_heads, index), probs[index]
        d_prob = dot_nt(d_out, head(qkv, group + 1))
        d_value = dot_tn(prob.astype(BF16), d_out)
        d_score = (prob * (d_prob - jnp.sum(d_prob * prob, axis=-1, keepdims=True)) * HEAD_DIM ** -0.5).astype(BF16)
        d_qkv[:, index * HEAD_DIM:(index + 1) * HEAD_DIM] = dot_nn(d_score, head(qkv, group)).astype(BF16)
        d_key = dot_tn(d_score, head(qkv, index))
        d_keys = d_key if d_keys is None else d_keys + d_key
        d_values = d_value if d_values is None else d_values + d_value
    d_qkv[:, group * HEAD_DIM:(group + 1) * HEAD_DIM] = d_keys.astype(BF16)
    d_qkv[:, (group + 1) * HEAD_DIM:(group + 2) * HEAD_DIM] = d_values.astype(BF16)


def load(src, dst, sem):
    copy = pltpu.make_async_copy(src, dst, sem)
    copy.start()
    return copy


def forward_kernel(layers, chips, hidden, gain_attn, gain_mlp, w_qkv, w_out, w_gate, w_up, w_down, *refs):
    outs, refs = refs[:layers], refs[layers:]
    (wq, wo, wg, wu, wd, full_in, full_mid, qkv, heads_out, act, part, near, relay, from_left, from_right,
     state, load_sem, send_sem, recv_sem) = refs
    links = Links(chips, send_sem, recv_sem)
    state[...] = hidden[...]
    links.enter((links.right, links.left, links.sib))
    pairs = ((w_qkv, wq), (w_out, wo), (w_gate, wg), (w_up, wu), (w_down, wd))

    def one_layer(layer, carry):
        links.used = 0
        row = pl.ds(layer, 1)
        loads = [load(src.at[layer], dst, load_sem.at[index]) for index, (src, dst) in enumerate(pairs)]
        with jax.named_scope('norm_in'):
            full_in[links.x, links.c] = rms_norm(state[...], gain_attn[row, :])
        gather = Gather(links, full_in)
        gather.relay()
        gather.finish()
        loads[0].wait()
        with jax.named_scope('qkv'):
            project(full_in, wq, qkv, qkv.shape[1])
        with jax.named_scope('attention'):
            attention(qkv, heads_out)
        loads[1].wait()
        total = reduce_scatter(links, lambda col, width: dot_nn(heads_out[...], wo[:, pl.ds(col, width)]),
                               part, near.at[0], relay.at[0], from_left.at[0], from_right.at[0])
        with jax.named_scope('norm_mid'):
            hidden_mid = state[...] + total.astype(BF16)
            full_mid[links.x, links.c] = rms_norm(hidden_mid, gain_mlp[row, :])
            state[...] = hidden_mid
        links.drain()
        gather = Gather(links, full_mid)
        gather.relay()
        gather.finish()
        for copy in loads[2:]:
            copy.wait()
        tile = 2 * HEAD_DIM

        def body(index, carry):
            cols = pl.ds(pl.multiple_of(index * tile, tile), tile)
            gate_act = dot_nn(flat(full_mid), wg[:, cols]).astype(BF16).astype(F32)
            up_act = dot_nn(flat(full_mid), wu[:, cols]).astype(BF16).astype(F32)
            act[:, cols] = (gate_act * jax.nn.sigmoid(gate_act) * up_act).astype(BF16)
            return carry
        with jax.named_scope('gate_up'):
            lax.fori_loop(0, act.shape[1] // tile, body, 0)
        total = reduce_scatter(links, lambda col, width: dot_nn(act[...], wd[:, pl.ds(col, width)]),
                               part, near.at[1], relay.at[1], from_left.at[1], from_right.at[1])
        state[...] = state[...] + total.astype(BF16)
        for index, out in enumerate(outs):
            @pl.when(layer == index)
            def _(out=out):
                out[...] = state[...]
        links.drain()
        return carry
    lax.fori_loop(0, layers, one_layer, 0)


def turn(src, dst):
    seq = dst.shape[1]
    tile = HEAD_DIM if dst.shape[0] % (2 * HEAD_DIM) else 2 * HEAD_DIM

    def body(index, carry):
        span = pl.ds(pl.multiple_of(index * tile, tile), tile)
        block = src[:, :, :, span].reshape(seq, tile) if len(src.shape) == 4 else src[:, span]
        dst[span, :] = block.T
        return carry
    lax.fori_loop(0, dst.shape[0] // tile, body, 0)


def backward_kernel(layer, chips, final, hidden, d_out, gain_attn, gain_mlp, w_qkv, w_out, w_gate, w_up, w_down, *refs):
    carried, refs = (refs[0], refs[1:]) if final else (None, refs)
    (d_hidden, gains, o_in, o_mid, o_down, o_attn, o_act, o_gate, o_up, o_heads, o_qkv,
     wq, wo, wg, wu, wd, full_in, full_mid, full_down, full_attn, qkv, heads_out, act, d_gate, d_up, d_heads, d_qkv,
     probs, t_in, t_mid, t_act, t_heads, part, near, relay, from_left, from_right, gain_mid, gain_last,
     load_sem, save_sem, send_sem, recv_sem) = refs
    links = Links(chips, send_sem, recv_sem)
    x, c = links.x, links.c
    pairs = ((w_qkv, wq), (w_out, wo), (w_gate, wg), (w_up, wu), (w_down, wd))
    loads = [load(src.at[layer], dst, load_sem.at[index]) for index, (src, dst) in enumerate(pairs)]
    saves = []

    def save(src, dst):
        saves.append(load(src, dst, save_sem.at[len(saves)]))

    row = pl.ds(layer, 1)
    full_in[x, c] = rms_norm(hidden[...], gain_attn[row, :])
    full_down[x, c] = d_out[...]
    links.enter(links.others() if final else (links.right, links.left, links.sib))
    gather = Gather(links, full_in)
    gather.relay()
    gather_down = Gather(links, full_down)
    gather.finish()
    loads[0].wait()
    with jax.named_scope('qkv'):
        project(full_in, wq, qkv, qkv.shape[1])
    gather_down.relay()
    with jax.named_scope('attention'):
        attention(qkv, heads_out, probs)
    loads[1].wait()

    def gated():
        gather_down.finish()
        save(full_down, o_down)
        loads[4].wait()
        project_t(full_down, wd, act, 2 * HEAD_DIM)

    def turn_in():
        turn(full_in, t_in)
        turn(heads_out, t_heads)
        save(t_in, o_in)
        save(t_heads, o_heads)

    def turn_mid():
        turn(full_mid, t_mid)
        turn(act, t_act)
        save(t_mid, o_mid)
        save(t_act, o_act)

    total = reduce_scatter(links, lambda col, width: dot_nn(heads_out[...], wo[:, pl.ds(col, width)]),
                           part, near.at[0], relay.at[0], from_left.at[0], from_right.at[0], [gated, turn_in])
    hidden_mid = hidden[...] + total.astype(BF16)
    d_hidden[...] = hidden_mid
    full_mid[x, c] = rms_norm(hidden_mid, gain_mlp[row, :])
    links.drain()
    gather = Gather(links, full_mid)
    gather.relay()
    gather.finish()
    loads[2].wait()
    loads[3].wait()
    tile = 2 * HEAD_DIM

    def body(index, carry):
        cols = pl.ds(pl.multiple_of(index * tile, tile), tile)
        gate_act = dot_nn(flat(full_mid), wg[:, cols]).astype(BF16).astype(F32)
        up_act = dot_nn(flat(full_mid), wu[:, cols]).astype(BF16).astype(F32)
        sig = jax.nn.sigmoid(gate_act)
        silu = gate_act * sig
        d_act = act[:, cols].astype(F32)
        d_up[:, cols] = (d_act * silu).astype(BF16)
        d_gate[:, cols] = (d_act * up_act * (sig + silu * (1.0 - sig))).astype(BF16)
        act[:, cols] = (silu * up_act).astype(BF16)
        return carry
    with jax.named_scope('gate_up'):
        lax.fori_loop(0, act.shape[1] // tile, body, 0)
    save(d_gate, o_gate)
    save(d_up, o_up)

    def mid_product(col, width):
        return dot_nt(d_gate[...], wg[pl.ds(col, width), :]) + dot_nt(d_up[...], wu[pl.ds(col, width), :])

    total = reduce_scatter(links, mid_product, part, near.at[1], relay.at[1], from_left.at[1], from_right.at[1],
                           [turn_mid])
    d_norm, d_gain = rms_norm_pull(d_hidden[...], gain_mlp[row, :], total.astype(BF16))
    d_mid = d_out[...] + d_norm
    full_attn[x, c] = d_mid
    d_hidden[...] = d_mid
    links.drain()
    gather = Gather(links, full_attn)
    lanes = gain_mid.shape[2]
    done = carried.shape[0] if final else 0

    def put(ref, index, value):
        for line in range(lanes):
            ref[index, line:line + 1, :] = value[:, line * HEAD_DIM:(line + 1) * HEAD_DIM]

    mine = gain_mid.at[links.me]
    if final:
        mine[1:done + 1] = carried[...]
    put(mine, 0, d_gain)
    gather.relay()
    gather.finish()
    save(full_attn, o_attn)
    shares = []
    if final:
        shares = [links.copy(mine, mine, peer) for peer in links.others()]
    with jax.named_scope('d_heads'):
        project_t(full_attn, wo, d_heads, d_heads.shape[1])
    with jax.named_scope('attention_pull'):
        attention_pull(qkv, probs, d_heads, d_qkv)
    save(d_qkv, o_qkv)
    total = reduce_scatter(links, lambda col, width: dot_nt(d_qkv[...], wq[pl.ds(col, width), :]),
                           part, near.at[2], relay.at[2], from_left.at[2], from_right.at[2])
    d_norm, d_gain = rms_norm_pull(hidden[...], gain_attn[row, :], total.astype(BF16))
    mine_last = gain_last.at[links.me]
    put(mine_last, 0, d_gain)
    if final:
        shares += [links.copy(mine_last, mine_last, peer) for peer in links.others()]
    d_hidden[...] = d_hidden[...] + d_norm
    if final:
        for copy in shares:
            copy.wait_recv()
        size = chips * CORES
        gains[1:done + 2] = sum([gain_mid[peer] for peer in range(1, size)], gain_mid[0])
        gains[0:1] = sum([gain_last[peer] for peer in range(1, size)], gain_last[0])
    else:
        gains[0:1] = mine_last[...]
        gains[1:2] = mine[...]
    for copy in saves:
        copy.wait()
    links.drain()


def grads_kernel(layer, fresh, *refs):
    ins, rest = refs[:9], refs[9:]
    if not fresh:
        rest = rest[5:]
    outs, rest = rest[:5], rest[5:]
    t_in, t_mid, full_down, full_attn, t_act, d_gate, d_up, t_heads, d_qkv = rest[:9]
    deep, tall, load_sem, save_sem = rest[9:]
    order = (4, 2, 1, 5, 6, 7, 3, 0, 8)
    loads = {index: load(ins[index], rest[index], load_sem.at[index]) for index in order}
    jobs = ((t_act, full_down, outs[4], 256, (4, 2)), (t_mid, d_gate, outs[2], 512, (1, 5)), (t_mid, d_up, outs[3], 512, (6,)),
            (t_heads, full_attn, outs[1], 192, (7, 3)), (t_in, d_qkv, outs[0], 1024, (0, 8)))
    busy = [[], []]
    for place, (left, right, out, size, needs) in enumerate(jobs):
        for index in needs:
            loads[index].wait()
        for copy in busy[place % 2]:
            copy.wait()
        rows, cols = out.shape[1], out.shape[2]
        count = rows // size
        base = 2 * (place % 2)
        stage = deep if cols > tall.shape[2] else tall

        def slot_copy(slot, start, size=size, cols=cols, out=out, stage=stage):
            return pltpu.make_async_copy(stage.at[slot, pl.ds(0, size), pl.ds(0, cols)],
                                         out.at[layer, pl.ds(start, size), :], save_sem.at[slot])

        def body(index, carry, left=left, right=right, size=size, cols=cols, slot_copy=slot_copy, base=base, stage=stage):
            slot = base + lax.rem(index, 2)
            start = pl.multiple_of(index * size, size)

            @pl.when(index >= 2)
            def _():
                slot_copy(slot, start).wait()
            turned = left[pl.ds(start, size), :]
            for col in range(0, cols, 256):
                width = min(256, cols - col)
                if len(right.shape) == 4:
                    chips, cores, some, _ = right.shape
                    piece = right[:, :, :, col:col + width].reshape(chips * cores * some, width)
                else:
                    piece = right[:, col:col + width]
                stage[slot, 0:size, col:col + width] = dot_nn(turned, piece).astype(BF16)
            slot_copy(slot, start).start()
            return carry
        lax.fori_loop(0, count, body, 0)
        busy[place % 2] = [slot_copy(base + slot, 0) for slot in range(min(2, count))]
    for copies in busy:
        for copy in copies:
            copy.wait()


def vmem(*shape, dtype=BF16):
    return pltpu.VMEM(shape, dtype)


def solution(mesh):
    chips = mesh.shape['tp'] // CORES
    row_spec = P(('dp', 'tp'), None)
    col_spec = P(None, None, 'tp')
    mid_spec = P(None, 'tp', None)
    in_specs = (row_spec, row_spec, P(None, None), P(None, None), col_spec, mid_spec, col_spec, col_spec, mid_spec)
    out_specs = (row_spec, row_spec, P('dp', None, 'tp'), P('dp', 'tp', None), P('dp', None, 'tp'), P('dp', None, 'tp'), P('dp', 'tp', None), P('dp', None), P('dp', None))

    def device_step(x, grad_y, gain_attn, gain_mlp, w_qkv, w_out, w_gate, w_up, w_down):
        layers, width, qkv_cols = w_qkv.shape
        head_cols, units, rows = w_out.shape[1], w_gate.shape[2], x.shape[0]
        group = head_cols // HEAD_DIM
        seq = chips * CORES * rows
        lanes = width // HEAD_DIM
        full = (chips, CORES, rows, width)
        weights = (w_qkv, w_out, w_gate, w_up, w_down)
        weight_bufs = [vmem(*weight.shape[1:]) for weight in weights]

        def ring_bufs(uses):
            return [vmem(*full, dtype=F32), vmem(uses, chips, rows, width, dtype=F32), vmem(uses, 2, rows, width // 2, dtype=F32),
                    vmem(uses, rows, width, dtype=F32), vmem(uses, rows, width, dtype=F32)]

        def dma(count):
            return pltpu.SemaphoreType.DMA((count,))

        def params(ident):
            return pltpu.CompilerParams(collective_id=ident, has_side_effects=True, vmem_limit_bytes=VMEM_LIMIT)

        def forward(hidden):
            copies = 2 * 13 + 2 * 8 * STEPS
            return pl.pallas_call(
                functools.partial(forward_kernel, layers, chips),
                out_shape=[jax.ShapeDtypeStruct(hidden.shape, BF16)] * layers,
                in_specs=[VMEM_SPEC] * 3 + [ANY] * 5,
                out_specs=[VMEM_SPEC] * layers,
                scratch_shapes=weight_bufs + [vmem(*full), vmem(*full), vmem(seq, qkv_cols), vmem(seq, head_cols), vmem(seq, units)]
                + ring_bufs(2) + [vmem(*hidden.shape), dma(5), dma(copies), dma(copies)],
                compiler_params=params(layers), name='forward',
            )(hidden, gain_attn, gain_mlp, *weights)

        def backward(layer, hidden, d_out, carried):
            final = layer == 0
            peers = chips * CORES - 1
            copies = 4 * 13 + 3 * 8 * STEPS + 2 * peers
            done = carried[0].shape[0] if final else 0
            factor = lambda *shape: jax.ShapeDtypeStruct(shape, BF16)
            return pl.pallas_call(
                functools.partial(backward_kernel, layer, chips, final),
                out_shape=[factor(*hidden.shape), jax.ShapeDtypeStruct((done + 2, lanes, HEAD_DIM), F32)]
                + [factor(width, seq)] * 2 + [factor(*full)] * 2
                + [factor(units, seq), factor(seq, units), factor(seq, units), factor(head_cols, seq), factor(seq, qkv_cols)],
                in_specs=[VMEM_SPEC] * 4 + [ANY] * 5 + [VMEM_SPEC] * len(carried),
                out_specs=[VMEM_SPEC] * 2 + [ANY] * 9,
                scratch_shapes=weight_bufs + [vmem(*full)] * 4
                + [vmem(seq, qkv_cols), vmem(seq, head_cols), vmem(seq, units), vmem(seq, units), vmem(seq, units),
                   vmem(seq, head_cols), vmem(seq, qkv_cols), vmem(group, seq, seq, dtype=F32),
                   vmem(width, seq), vmem(width, seq), vmem(units, seq), vmem(head_cols, seq)] + ring_bufs(3)
                + [vmem(chips * CORES, done + 1, lanes, HEAD_DIM, dtype=F32), vmem(chips * CORES, 1, lanes, HEAD_DIM, dtype=F32),
                   dma(5), dma(9), dma(copies), dma(copies)],
                compiler_params=params(layer), name=f'backward_{layer}',
            )(hidden, d_out, gain_attn, gain_mlp, *weights, *carried)

        grad_shapes = [jax.ShapeDtypeStruct(weight.shape, BF16) for weight in weights]

        def grads(layer, factors, into):
            given = [] if into is None else list(into)
            return pl.pallas_call(
                functools.partial(grads_kernel, layer, into is None),
                out_shape=grad_shapes,
                in_specs=[ANY] * (len(factors) + len(given)),
                out_specs=[ANY] * 5,
                scratch_shapes=[vmem(*factor.shape) for factor in factors] + [vmem(4, 256, width), vmem(4, 1024, units), dma(len(factors)), dma(4)],
                input_output_aliases={len(factors) + index: index for index in range(len(given))},
                compiler_params=pltpu.CompilerParams(vmem_limit_bytes=VMEM_LIMIT), name=f'grads_{layer}',
            )(*factors, *given)

        kept = [x, *forward(x)]
        d_hidden, out_grads, partial_gains = grad_y, None, []
        for layer in reversed(range(layers)):
            carried = [jnp.concatenate(partial_gains[::-1])] if layer == 0 else []
            d_hidden, gains, *factors = backward(layer, kept[layer], d_hidden, carried)
            partial_gains.append(gains)
            out_grads = grads(layer, factors, out_grads)
            d_hidden, *out_grads = lax.optimization_barrier((d_hidden, *out_grads))
        pairs = gains.reshape(layers, 2, width)
        return (kept[-1], d_hidden, *out_grads, pairs[:, 0], pairs[:, 1])

    return jax.shard_map(device_step, mesh=mesh, in_specs=in_specs, out_specs=out_specs, check_vma=False)
```

```python
import functools

import jax
import jax.numpy as jnp
from jax import lax
from jax.experimental import pallas as pl
from jax.experimental.pallas import tpu as pltpu
from jax.sharding import PartitionSpec as P

HEAD_DIM = 128
NORM_EPS = 1e-5
CORES = 2
MESH = pl.DeviceIdType.MESH
F32 = jnp.float32
BF16 = jnp.bfloat16
VMEM_LIMIT = 66_000_000
SPLIT = (1, 3, 4, 4)
STEPS = len(SPLIT)
ANY = pl.BlockSpec(memory_space=pltpu.HBM)
VMEM_SPEC = pl.BlockSpec(memory_space=pltpu.VMEM)


def dot_nn(a, b):
    return lax.dot_general(a, b, (((1,), (0,)), ((), ())), preferred_element_type=F32)


def dot_nt(a, b):
    return lax.dot_general(a, b, (((1,), (1,)), ((), ())), preferred_element_type=F32)


def dot_tn(a, b):
    return lax.dot_general(a, b, (((0,), (0,)), ((), ())), preferred_element_type=F32)


class Links:
    def __init__(self, chips, send_sem, recv_sem):
        self.me = lax.axis_index('tp')
        self.chips = chips
        self.x = lax.div(self.me, CORES)
        self.c = lax.rem(self.me, CORES)
        self.xr = lax.rem(self.x + 1, chips)
        self.xl = lax.rem(self.x + chips - 1, chips)
        self.xo = lax.rem(self.x + 2, chips)
        self.right = self.xr * CORES + self.c
        self.left = self.xl * CORES + self.c
        self.sib = self.x * CORES + 1 - self.c
        self.send_sem, self.recv_sem, self.used, self.pending = send_sem, recv_sem, 0, []

    def enter(self, peers):
        barrier = pltpu.get_barrier_semaphore()
        for peer in peers:
            pl.semaphore_signal(barrier, inc=1, device_id={'tp': peer}, device_id_type=MESH)
        pl.semaphore_wait(barrier, len(peers))

    def others(self):
        size = self.chips * CORES
        return [lax.rem(self.me + step, size) for step in range(1, size)]

    def copy(self, src, dst, peer):
        copy = pltpu.make_async_remote_copy(
            src_ref=src, dst_ref=dst, send_sem=self.send_sem.at[self.used], recv_sem=self.recv_sem.at[self.used],
            device_id={'tp': peer}, device_id_type=MESH)
        self.used += 1
        copy.start()
        self.pending.append(copy)
        return copy

    def drain(self):
        for copy in self.pending:
            copy.wait_send()
        self.pending = []


class Gather:
    def __init__(self, links, full):
        self.links, self.full = links, full
        self.half = full.shape[3] // 2
        part_a, part_b = pl.ds(0, self.half), pl.ds(self.half, self.half)
        x, c = links.x, links.c
        self.a, self.b = part_a, part_b
        self.right_a = self.send(x, part_a, links.right)
        self.left_b = self.send(x, part_b, links.left)
        self.right_b = self.send(x, part_b, links.right)
        self.left_a = self.send(x, part_a, links.left)
        self.near = [links.copy(full.at[x, c], full.at[x, c], links.sib)]

    def send(self, chip, part, peer):
        ref = self.full.at[chip, self.links.c, :, part]
        return self.links.copy(ref, ref, peer)

    @jax.named_scope('gather')
    def relay(self):
        links = self.links
        self.right_a.wait_recv()
        relay_a = self.send(links.xl, self.a, links.right)
        self.near.append(self.send(links.xl, self.a, links.sib))
        self.left_b.wait_recv()
        relay_b = self.send(links.xr, self.b, links.left)
        self.near.append(self.send(links.xr, self.b, links.sib))
        self.far = (relay_a, relay_b)

    @jax.named_scope('finish')
    def finish(self):
        links = self.links
        self.right_b.wait_recv()
        self.near.append(self.send(links.xl, self.b, links.sib))
        self.left_a.wait_recv()
        self.near.append(self.send(links.xr, self.a, links.sib))
        self.far[0].wait_recv()
        self.near.append(self.send(links.xo, self.a, links.sib))
        self.far[1].wait_recv()
        self.near.append(self.send(links.xo, self.b, links.sib))
        for copy in self.near:
            copy.wait_recv()


def reduce_scatter(links, product, part, near, relay, from_left, from_right, fillers=()):
    chips, _, rows, cols = part.shape
    half = cols // 2
    unit = half // sum(SPLIT)
    starts = [unit * sum(SPLIT[:step]) for step in range(STEPS)]
    x, c, xr, xl, xo = links.x, links.c, links.xr, links.xl, links.xo
    swap, first, last = [None] * STEPS, [None] * STEPS, []

    def spans(step):
        width = unit * SPLIT[step]
        return pl.ds(starts[step], width), pl.ds(half + starts[step], width)

    def make(step):
        swap[step] = []
        for span in spans(step):
            part[:, :, :, span] = product(span.start, span.size).reshape(chips, CORES, rows, span.size)
            swap[step].append(links.copy(part.at[:, 1 - c, :, span], near.at[:, :, span], links.sib))

    def send(step):
        span_a, span_b = spans(step)
        for copy, span in zip(swap[step], (span_a, span_b)):
            copy.wait_recv()
            part[:, c, :, span] = part[:, c, :, span] + near[:, :, span]
        first[step] = (
            links.copy(part.at[xo, c, :, span_a], relay.at[0, :, span_a], links.right),
            links.copy(part.at[xo, c, :, span_b], relay.at[1, :, span_a], links.left))
        last.append(links.copy(part.at[xr, c, :, span_b], from_left.at[:, span_b], links.right))
        last.append(links.copy(part.at[xl, c, :, span_a], from_right.at[:, span_a], links.left))

    def pass_on(step):
        span_a, span_b = spans(step)
        first[step][0].wait_recv()
        part[xr, c, :, span_a] = part[xr, c, :, span_a] + relay[0, :, span_a]
        last.append(links.copy(part.at[xr, c, :, span_a], from_left.at[:, span_a], links.right))
        first[step][1].wait_recv()
        part[xl, c, :, span_b] = part[xl, c, :, span_b] + relay[1, :, span_a]
        last.append(links.copy(part.at[xl, c, :, span_b], from_right.at[:, span_b], links.left))

    for step in range(STEPS):
        with jax.named_scope(f'make{step}'):
            make(step)
        if step:
            with jax.named_scope(f'send{step - 1}'):
                send(step - 1)
    with jax.named_scope(f'send{STEPS - 1}'):
        send(STEPS - 1)
    with jax.named_scope('fillers'):
        for filler in fillers:
            filler()
    for step in range(STEPS):
        with jax.named_scope(f'pass_on{step}'):
            pass_on(step)
    with jax.named_scope('last'):
        for copy in last:
            copy.wait_recv()
    return part[x, c] + from_left[...] + from_right[...]


def rms_norm(hidden, gain):
    hidden_f = hidden.astype(F32)
    inv_rms = lax.rsqrt(jnp.mean(hidden_f * hidden_f, axis=-1, keepdims=True) + NORM_EPS)
    return (hidden_f * inv_rms * gain).astype(BF16)


def rms_norm_pull(hidden, gain, cotangent):
    hidden_f, cot = hidden.astype(F32), cotangent.astype(F32)
    inv_rms = lax.rsqrt(jnp.mean(hidden_f * hidden_f, axis=-1, keepdims=True) + NORM_EPS)
    scaled = cot * gain
    dot = jnp.mean(scaled * hidden_f, axis=-1, keepdims=True)
    d_hidden = scaled * inv_rms - hidden_f * (inv_rms * inv_rms * inv_rms * dot)
    return d_hidden.astype(BF16), jnp.sum(cot * (hidden_f * inv_rms), axis=0, keepdims=True)


def flat(ref):
    chips, cores, rows, cols = ref.shape
    return ref[...].reshape(chips * cores * rows, cols)


def project(full, weight, out, tile):
    def body(index, carry):
        cols = pl.ds(pl.multiple_of(index * tile, tile), tile)
        out[:, cols] = dot_nn(flat(full), weight[:, cols]).astype(BF16)
        return carry
    lax.fori_loop(0, out.shape[1] // tile, body, 0)


def project_t(full, weight, out, tile):
    def body(index, carry):
        span = pl.ds(pl.multiple_of(index * tile, tile), tile)
        out[:, span] = dot_nt(flat(full), weight[span, :]).astype(BF16)
        return carry
    lax.fori_loop(0, out.shape[1] // tile, body, 0)


def head(ref, index):
    return ref[:, index * HEAD_DIM:(index + 1) * HEAD_DIM]


def attention(qkv, heads_out, probs=None):
    group = heads_out.shape[1] // HEAD_DIM
    seq = qkv.shape[0]
    causal = lax.broadcasted_iota(jnp.int32, (seq, seq), 0) >= lax.broadcasted_iota(jnp.int32, (seq, seq), 1)
    for index in range(group):
        scores = dot_nt(head(qkv, index), head(qkv, group)) * HEAD_DIM ** -0.5
        scores = jnp.where(causal, scores, -1e30)
        weight = jnp.exp(scores - jnp.max(scores, axis=-1, keepdims=True))
        prob = weight / jnp.sum(weight, axis=-1, keepdims=True)
        if probs is not None:
            probs[index] = prob
        heads_out[:, index * HEAD_DIM:(index + 1) * HEAD_DIM] = dot_nn(prob.astype(BF16), head(qkv, group + 1)).astype(BF16)


def attention_pull(qkv, probs, d_heads, d_qkv):
    group = d_heads.shape[1] // HEAD_DIM
    d_keys = d_values = None
    for index in range(group):
        d_out, prob = head(d_heads, index), probs[index]
        d_prob = dot_nt(d_out, head(qkv, group + 1))
        d_value = dot_tn(prob.astype(BF16), d_out)
        d_score = (prob * (d_prob - jnp.sum(d_prob * prob, axis=-1, keepdims=True)) * HEAD_DIM ** -0.5).astype(BF16)
        d_qkv[:, index * HEAD_DIM:(index + 1) * HEAD_DIM] = dot_nn(d_score, head(qkv, group)).astype(BF16)
        d_key = dot_tn(d_score, head(qkv, index))
        d_keys = d_key if d_keys is None else d_keys + d_key
        d_values = d_value if d_values is None else d_values + d_value
    d_qkv[:, group * HEAD_DIM:(group + 1) * HEAD_DIM] = d_keys.astype(BF16)
    d_qkv[:, (group + 1) * HEAD_DIM:(group + 2) * HEAD_DIM] = d_values.astype(BF16)


def load(src, dst, sem):
    copy = pltpu.make_async_copy(src, dst, sem)
    copy.start()
    return copy


def forward_kernel(layers, chips, hidden, gain_attn, gain_mlp, w_qkv, w_out, w_gate, w_up, w_down, *refs):
    outs, refs = refs[:layers], refs[layers:]
    (wq, wo, wg, wu, wd, full_in, full_mid, qkv, heads_out, act, part, near, relay, from_left, from_right,
     state, load_sem, send_sem, recv_sem) = refs
    links = Links(chips, send_sem, recv_sem)
    state[...] = hidden[...]
    links.enter((links.right, links.left, links.sib))
    pairs = ((w_qkv, wq), (w_out, wo), (w_gate, wg), (w_up, wu), (w_down, wd))

    def one_layer(layer, carry):
        links.used = 0
        row = pl.ds(layer, 1)
        loads = [load(src.at[layer], dst, load_sem.at[index]) for index, (src, dst) in enumerate(pairs)]
        with jax.named_scope('norm_in'):
            full_in[links.x, links.c] = rms_norm(state[...], gain_attn[row, :])
        gather = Gather(links, full_in)
        gather.relay()
        gather.finish()
        loads[0].wait()
        with jax.named_scope('qkv'):
            project(full_in, wq, qkv, qkv.shape[1])
        with jax.named_scope('attention'):
            attention(qkv, heads_out)
        loads[1].wait()
        total = reduce_scatter(links, lambda col, width: dot_nn(heads_out[...], wo[:, pl.ds(col, width)]),
                               part, near.at[0], relay.at[0], from_left.at[0], from_right.at[0])
        with jax.named_scope('norm_mid'):
            hidden_mid = state[...] + total.astype(BF16)
            full_mid[links.x, links.c] = rms_norm(hidden_mid, gain_mlp[row, :])
            state[...] = hidden_mid
        links.drain()
        gather = Gather(links, full_mid)
        gather.relay()
        gather.finish()
        for copy in loads[2:]:
            copy.wait()
        tile = 2 * HEAD_DIM

        def body(index, carry):
            cols = pl.ds(pl.multiple_of(index * tile, tile), tile)
            gate_act = dot_nn(flat(full_mid), wg[:, cols]).astype(BF16).astype(F32)
            up_act = dot_nn(flat(full_mid), wu[:, cols]).astype(BF16).astype(F32)
            act[:, cols] = (gate_act * jax.nn.sigmoid(gate_act) * up_act).astype(BF16)
            return carry
        with jax.named_scope('gate_up'):
            lax.fori_loop(0, act.shape[1] // tile, body, 0)
        total = reduce_scatter(links, lambda col, width: dot_nn(act[...], wd[:, pl.ds(col, width)]),
                               part, near.at[1], relay.at[1], from_left.at[1], from_right.at[1])
        state[...] = state[...] + total.astype(BF16)
        for index, out in enumerate(outs):
            @pl.when(layer == index)
            def _(out=out):
                out[...] = state[...]
        links.drain()
        return carry
    lax.fori_loop(0, layers, one_layer, 0)


def turn(src, dst):
    seq = dst.shape[1]
    tile = HEAD_DIM if dst.shape[0] % (2 * HEAD_DIM) else 2 * HEAD_DIM

    def body(index, carry):
        span = pl.ds(pl.multiple_of(index * tile, tile), tile)
        block = src[:, :, :, span].reshape(seq, tile) if len(src.shape) == 4 else src[:, span]
        dst[span, :] = block.T
        return carry
    lax.fori_loop(0, dst.shape[0] // tile, body, 0)


def backward_kernel(layer, chips, final, hidden, d_out, gain_attn, gain_mlp, w_qkv, w_out, w_gate, w_up, w_down, *refs):
    carried, refs = (refs[0], refs[1:]) if final else (None, refs)
    (d_hidden, gains, o_in, o_mid, o_down, o_attn, o_act, o_gate, o_up, o_heads, o_qkv,
     wq, wo, wgu, wd, full_in, full_mid, full_down, full_attn, qkv, heads_out, act, d_gu, d_heads, d_qkv,
     probs, t_in, t_mid, t_act, t_heads, part, near, relay, from_left, from_right, gain_mid, gain_last,
     load_sem, save_sem, send_sem, recv_sem) = refs
    links = Links(chips, send_sem, recv_sem)
    x, c = links.x, links.c
    units = act.shape[1]
    left, right = pl.ds(0, units), pl.ds(units, units)
    wg, wu, d_gate, d_up = wgu.at[:, left], wgu.at[:, right], d_gu.at[:, left], d_gu.at[:, right]
    pairs = ((w_qkv, wq), (w_out, wo), (w_gate, wg), (w_up, wu), (w_down, wd))
    loads = [load(src.at[layer], dst, load_sem.at[index]) for index, (src, dst) in enumerate(pairs)]
    saves = []

    def save(src, dst):
        saves.append(load(src, dst, save_sem.at[len(saves)]))

    row = pl.ds(layer, 1)
    full_in[x, c] = rms_norm(hidden[...], gain_attn[row, :])
    full_down[x, c] = d_out[...]
    links.enter(links.others() if final else (links.right, links.left, links.sib))
    gather = Gather(links, full_in)
    gather.relay()
    gather_down = Gather(links, full_down)
    gather.finish()
    loads[0].wait()
    with jax.named_scope('qkv'):
        project(full_in, wq, qkv, qkv.shape[1])
    gather_down.relay()
    with jax.named_scope('attention'):
        attention(qkv, heads_out, probs)
    loads[1].wait()

    def gated():
        gather_down.finish()
        save(full_down, o_down)
        loads[4].wait()
        project_t(full_down, wd, act, 2 * HEAD_DIM)

    def turn_in():
        turn(full_in, t_in)
        turn(heads_out, t_heads)
        save(t_in, o_in)
        save(t_heads, o_heads)

    def turn_mid():
        turn(full_mid, t_mid)
        turn(act, t_act)
        save(t_mid, o_mid)
        save(t_act, o_act)

    total = reduce_scatter(links, lambda col, width: dot_nn(heads_out[...], wo[:, pl.ds(col, width)]),
                           part, near.at[0], relay.at[0], from_left.at[0], from_right.at[0], [gated, turn_in])
    hidden_mid = hidden[...] + total.astype(BF16)
    d_hidden[...] = hidden_mid
    full_mid[x, c] = rms_norm(hidden_mid, gain_mlp[row, :])
    links.drain()
    gather = Gather(links, full_mid)
    gather.relay()
    gather.finish()
    loads[2].wait()
    loads[3].wait()
    tile = 2 * HEAD_DIM

    def body(index, carry):
        cols = pl.ds(pl.multiple_of(index * tile, tile), tile)
        gate_act = dot_nn(flat(full_mid), wg[:, cols]).astype(BF16).astype(F32)
        up_act = dot_nn(flat(full_mid), wu[:, cols]).astype(BF16).astype(F32)
        sig = jax.nn.sigmoid(gate_act)
        silu = gate_act * sig
        d_act = act[:, cols].astype(F32)
        d_up[:, cols] = (d_act * silu).astype(BF16)
        d_gate[:, cols] = (d_act * up_act * (sig + silu * (1.0 - sig))).astype(BF16)
        act[:, cols] = (silu * up_act).astype(BF16)
        return carry
    with jax.named_scope('gate_up'):
        lax.fori_loop(0, act.shape[1] // tile, body, 0)
    save(d_gate, o_gate)
    save(d_up, o_up)

    def mid_product(col, width):
        return dot_nt(d_gu[...], wgu[pl.ds(col, width), :])

    total = reduce_scatter(links, mid_product, part, near.at[1], relay.at[1], from_left.at[1], from_right.at[1],
                           [turn_mid])
    d_norm, d_gain = rms_norm_pull(d_hidden[...], gain_mlp[row, :], total.astype(BF16))
    d_mid = d_out[...] + d_norm
    full_attn[x, c] = d_mid
    d_hidden[...] = d_mid
    links.drain()
    gather = Gather(links, full_attn)
    lanes = gain_mid.shape[2]
    done = carried.shape[0] if final else 0

    def put(ref, index, value):
        for line in range(lanes):
            ref[index, line:line + 1, :] = value[:, line * HEAD_DIM:(line + 1) * HEAD_DIM]

    mine = gain_mid.at[links.me]
    if final:
        mine[1:done + 1] = carried[...]
    put(mine, 0, d_gain)
    gather.relay()
    gather.finish()
    save(full_attn, o_attn)
    shares = []
    if final:
        shares = [links.copy(mine, mine, peer) for peer in links.others()]
    with jax.named_scope('d_heads'):
        project_t(full_attn, wo, d_heads, d_heads.shape[1])
    with jax.named_scope('attention_pull'):
        attention_pull(qkv, probs, d_heads, d_qkv)
    save(d_qkv, o_qkv)
    total = reduce_scatter(links, lambda col, width: dot_nt(d_qkv[...], wq[pl.ds(col, width), :]),
                           part, near.at[2], relay.at[2], from_left.at[2], from_right.at[2])
    d_norm, d_gain = rms_norm_pull(hidden[...], gain_attn[row, :], total.astype(BF16))
    mine_last = gain_last.at[links.me]
    put(mine_last, 0, d_gain)
    if final:
        shares += [links.copy(mine_last, mine_last, peer) for peer in links.others()]
    d_hidden[...] = d_hidden[...] + d_norm
    if final:
        for copy in shares:
            copy.wait_recv()
        size = chips * CORES
        gains[1:done + 2] = sum([gain_mid[peer] for peer in range(1, size)], gain_mid[0])
        gains[0:1] = sum([gain_last[peer] for peer in range(1, size)], gain_last[0])
    else:
        gains[0:1] = mine_last[...]
        gains[1:2] = mine[...]
    for copy in saves:
        copy.wait()
    links.drain()


def grads_kernel(layer, fresh, final, *refs):
    ins, refs = refs[:9], refs[9:]
    small, refs = (refs[:3], refs[3:]) if final else (None, refs)
    if not fresh:
        refs = refs[5:]
    outs, refs = refs[:5], refs[5:]
    small_outs, refs = (refs[:4], refs[4:]) if final else (None, refs)
    bufs, (deep, tall, load_sem, save_sem) = refs[:9], refs[9:]
    t_in, t_mid, full_down, full_attn, t_act, d_gate, d_up, t_heads, d_qkv = bufs
    loads = {}

    def fetch(*names):
        for name in names:
            loads[name] = load(ins[name], bufs[name], load_sem.at[name])

    fetch(2, 4)
    later = [(1, 5), (6,), (7, 3), (0, 8), ()]
    jobs = ((t_act, full_down, outs[4], 256, (4, 2)), (t_mid, d_gate, outs[2], 512, (1, 5)), (t_mid, d_up, outs[3], 512, (6,)),
            (t_heads, full_attn, outs[1], 192, (7, 3)), (t_in, d_qkv, outs[0], 1024, (0, 8)))
    busy = [[], []]
    for place, (left, right, out, size, needs) in enumerate(jobs):
        for index in needs:
            loads[index].wait()
        fetch(*later[place])
        for copy in busy[place % 2]:
            copy.wait()
        rows, cols = out.shape[1], out.shape[2]
        count = rows // size
        base = 2 * (place % 2)
        stage = deep if cols > tall.shape[2] else tall

        def slot_copy(slot, start, size=size, cols=cols, out=out, stage=stage):
            return pltpu.make_async_copy(stage.at[slot, pl.ds(0, size), pl.ds(0, cols)],
                                         out.at[layer, pl.ds(start, size), :], save_sem.at[slot])

        def body(index, carry, left=left, right=right, size=size, cols=cols, slot_copy=slot_copy, base=base, stage=stage):
            slot = base + lax.rem(index, 2)
            start = pl.multiple_of(index * size, size)

            @pl.when(index >= 2)
            def _():
                slot_copy(slot, start).wait()
            turned = left[pl.ds(start, size), :]
            for col in range(0, cols, 256):
                width = min(256, cols - col)
                if len(right.shape) == 4:
                    chips, cores, some, _ = right.shape
                    piece = right[:, :, :, col:col + width].reshape(chips * cores * some, width)
                else:
                    piece = right[:, col:col + width]
                stage[slot, 0:size, col:col + width] = dot_nn(turned, piece).astype(BF16)
            slot_copy(slot, start).start()
            return carry
        lax.fori_loop(0, count, body, 0)
        busy[place % 2] = [slot_copy(base + slot, 0) for slot in range(min(2, count))]
    if final:
        small_outs[0][...] = small[0][...]
        small_outs[1][...] = small[1][...]
        for index in range(small[2].shape[0]):
            target = small_outs[2 + index % 2]
            for line in range(small[2].shape[1]):
                target[index // 2:index // 2 + 1, line * HEAD_DIM:(line + 1) * HEAD_DIM] = small[2][index, line:line + 1, :]
    for copies in busy:
        for copy in copies:
            copy.wait()


def vmem(*shape, dtype=BF16):
    return pltpu.VMEM(shape, dtype)


def solution(mesh):
    chips = mesh.shape['tp'] // CORES
    row_spec = P(('dp', 'tp'), None)
    col_spec = P(None, None, 'tp')
    mid_spec = P(None, 'tp', None)
    in_specs = (row_spec, row_spec, P(None, None), P(None, None), col_spec, mid_spec, col_spec, col_spec, mid_spec)
    out_specs = (row_spec, row_spec, P('dp', None, 'tp'), P('dp', 'tp', None), P('dp', None, 'tp'), P('dp', None, 'tp'), P('dp', 'tp', None), P('dp', None), P('dp', None))

    def device_step(x, grad_y, gain_attn, gain_mlp, w_qkv, w_out, w_gate, w_up, w_down):
        layers, width, qkv_cols = w_qkv.shape
        head_cols, units, rows = w_out.shape[1], w_gate.shape[2], x.shape[0]
        group = head_cols // HEAD_DIM
        seq = chips * CORES * rows
        lanes = width // HEAD_DIM
        full = (chips, CORES, rows, width)
        weights = (w_qkv, w_out, w_gate, w_up, w_down)
        weight_bufs = [vmem(*weight.shape[1:]) for weight in weights]

        def ring_bufs(uses):
            return [vmem(*full, dtype=F32), vmem(uses, chips, rows, width, dtype=F32), vmem(uses, 2, rows, width // 2, dtype=F32),
                    vmem(uses, rows, width, dtype=F32), vmem(uses, rows, width, dtype=F32)]

        def dma(count):
            return pltpu.SemaphoreType.DMA((count,))

        def params(ident):
            return pltpu.CompilerParams(collective_id=ident, has_side_effects=True, vmem_limit_bytes=VMEM_LIMIT)

        def forward(hidden):
            copies = 2 * 13 + 2 * 8 * STEPS
            return pl.pallas_call(
                functools.partial(forward_kernel, layers, chips),
                out_shape=[jax.ShapeDtypeStruct(hidden.shape, BF16)] * layers,
                in_specs=[VMEM_SPEC] * 3 + [ANY] * 5,
                out_specs=[VMEM_SPEC] * layers,
                scratch_shapes=weight_bufs + [vmem(*full), vmem(*full), vmem(seq, qkv_cols), vmem(seq, head_cols), vmem(seq, units)]
                + ring_bufs(2) + [vmem(*hidden.shape), dma(5), dma(copies), dma(copies)],
                compiler_params=params(layers), name='forward',
            )(hidden, gain_attn, gain_mlp, *weights)

        def backward(layer, hidden, d_out, carried):
            final = layer == 0
            peers = chips * CORES - 1
            copies = 4 * 13 + 3 * 8 * STEPS + 2 * peers
            done = carried[0].shape[0] if final else 0
            factor = lambda *shape: jax.ShapeDtypeStruct(shape, BF16)
            return pl.pallas_call(
                functools.partial(backward_kernel, layer, chips, final),
                out_shape=[factor(*hidden.shape), jax.ShapeDtypeStruct((done + 2, lanes, HEAD_DIM), F32)]
                + [factor(width, seq)] * 2 + [factor(*full)] * 2
                + [factor(units, seq), factor(seq, units), factor(seq, units), factor(head_cols, seq), factor(seq, qkv_cols)],
                in_specs=[VMEM_SPEC] * 4 + [ANY] * 5 + [VMEM_SPEC] * len(carried),
                out_specs=[VMEM_SPEC] * 2 + [ANY] * 9,
                scratch_shapes=weight_bufs[:2] + [vmem(width, 2 * units), weight_bufs[4]] + [vmem(*full)] * 4
                + [vmem(seq, qkv_cols), vmem(seq, head_cols), vmem(seq, units), vmem(seq, 2 * units),
                   vmem(seq, head_cols), vmem(seq, qkv_cols), vmem(group, seq, seq, dtype=F32),
                   vmem(width, seq), vmem(width, seq), vmem(units, seq), vmem(head_cols, seq)] + ring_bufs(3)
                + [vmem(chips * CORES, done + 1, lanes, HEAD_DIM, dtype=F32), vmem(chips * CORES, 1, lanes, HEAD_DIM, dtype=F32),
                   dma(5), dma(9), dma(copies), dma(copies)],
                compiler_params=params(layer), name=f'backward_{layer}',
            )(hidden, d_out, gain_attn, gain_mlp, *weights, *carried)

        grad_shapes = [jax.ShapeDtypeStruct(weight.shape, BF16) for weight in weights]

        def grads(layer, factors, small, into):
            fresh, final = not into, layer == 0
            shapes = [jax.ShapeDtypeStruct(value.shape, value.dtype) for value in (x, x, gain_attn, gain_mlp)]
            return pl.pallas_call(
                functools.partial(grads_kernel, layer, fresh, final),
                out_shape=grad_shapes + (shapes if final else []),
                in_specs=[ANY] * len(factors) + [VMEM_SPEC] * len(small) + [ANY] * len(into),
                out_specs=[ANY] * 5 + [VMEM_SPEC] * (4 if final else 0),
                scratch_shapes=[vmem(*factor.shape) for factor in factors] + [vmem(4, 256, width), vmem(4, 1024, units), dma(len(factors)), dma(4)],
                input_output_aliases={len(factors) + len(small) + index: index for index in range(len(into))},
                compiler_params=pltpu.CompilerParams(vmem_limit_bytes=VMEM_LIMIT), name=f'grads_{layer}',
            )(*factors, *small, *into)

        kept = [x, *forward(x)]
        d_hidden, out_grads, partial_gains = grad_y, [], []
        for layer in reversed(range(layers)):
            carried = [jnp.concatenate(partial_gains[::-1])] if layer == 0 else []
            d_hidden, gains, *factors = backward(layer, kept[layer], d_hidden, carried)
            partial_gains.append(gains)
            if layer:
                out_grads = grads(layer, factors, [], out_grads)
                d_hidden, *out_grads = lax.optimization_barrier((d_hidden, *out_grads))
        *out_grads, y, grad_x, grad_attn, grad_mlp = grads(0, factors, [kept[-1], d_hidden, gains], out_grads)
        return (y, grad_x, *out_grads, grad_attn, grad_mlp)

    return jax.shard_map(device_step, mesh=mesh, in_specs=in_specs, out_specs=out_specs, check_vma=False)
```

```python
import functools

import jax
import jax.numpy as jnp
from jax import lax
from jax.experimental import pallas as pl
from jax.experimental.pallas import tpu as pltpu
from jax.sharding import PartitionSpec as P

HEAD_DIM = 128
NORM_EPS = 1e-5
CORES = 2
MESH = pl.DeviceIdType.MESH
F32 = jnp.float32
BF16 = jnp.bfloat16
VMEM_LIMIT = 66_000_000
SPLIT = (1, 3, 4, 4)
STEPS = len(SPLIT)
ANY = pl.BlockSpec(memory_space=pltpu.HBM)
VMEM_SPEC = pl.BlockSpec(memory_space=pltpu.VMEM)


def dot_nn(a, b):
    return lax.dot_general(a, b, (((1,), (0,)), ((), ())), preferred_element_type=F32)


def dot_nt(a, b):
    return lax.dot_general(a, b, (((1,), (1,)), ((), ())), preferred_element_type=F32)


def dot_tn(a, b):
    return lax.dot_general(a, b, (((0,), (0,)), ((), ())), preferred_element_type=F32)


class Links:
    def __init__(self, chips, send_sem, recv_sem):
        self.me = lax.axis_index('tp')
        self.chips = chips
        self.x = lax.div(self.me, CORES)
        self.c = lax.rem(self.me, CORES)
        self.xr = lax.rem(self.x + 1, chips)
        self.xl = lax.rem(self.x + chips - 1, chips)
        self.xo = lax.rem(self.x + 2, chips)
        self.right = self.xr * CORES + self.c
        self.left = self.xl * CORES + self.c
        self.sib = self.x * CORES + 1 - self.c
        self.send_sem, self.recv_sem, self.used, self.pending = send_sem, recv_sem, 0, []

    def enter(self, peers):
        barrier = pltpu.get_barrier_semaphore()
        for peer in peers:
            pl.semaphore_signal(barrier, inc=1, device_id={'tp': peer}, device_id_type=MESH)
        pl.semaphore_wait(barrier, len(peers))

    def others(self):
        size = self.chips * CORES
        return [lax.rem(self.me + step, size) for step in range(1, size)]

    def copy(self, src, dst, peer):
        copy = pltpu.make_async_remote_copy(
            src_ref=src, dst_ref=dst, send_sem=self.send_sem.at[self.used], recv_sem=self.recv_sem.at[self.used],
            device_id={'tp': peer}, device_id_type=MESH)
        self.used += 1
        copy.start()
        self.pending.append(copy)
        return copy

    def drain(self):
        for copy in self.pending:
            copy.wait_send()
        self.pending = []


class Gather:
    def __init__(self, links, full):
        self.links, self.full = links, full
        self.half = full.shape[3] // 2
        part_a, part_b = pl.ds(0, self.half), pl.ds(self.half, self.half)
        x, c = links.x, links.c
        self.a, self.b = part_a, part_b
        self.right_a = self.send(x, part_a, links.right)
        self.left_b = self.send(x, part_b, links.left)
        self.right_b = self.send(x, part_b, links.right)
        self.left_a = self.send(x, part_a, links.left)
        self.near = [links.copy(full.at[x, c], full.at[x, c], links.sib)]

    def send(self, chip, part, peer):
        ref = self.full.at[chip, self.links.c, :, part]
        return self.links.copy(ref, ref, peer)

    @jax.named_scope('gather')
    def relay(self):
        links = self.links
        self.right_a.wait_recv()
        relay_a = self.send(links.xl, self.a, links.right)
        self.near.append(self.send(links.xl, self.a, links.sib))
        self.left_b.wait_recv()
        relay_b = self.send(links.xr, self.b, links.left)
        self.near.append(self.send(links.xr, self.b, links.sib))
        self.far = (relay_a, relay_b)

    @jax.named_scope('finish')
    def finish(self):
        links = self.links
        self.right_b.wait_recv()
        self.near.append(self.send(links.xl, self.b, links.sib))
        self.left_a.wait_recv()
        self.near.append(self.send(links.xr, self.a, links.sib))
        self.far[0].wait_recv()
        self.near.append(self.send(links.xo, self.a, links.sib))
        self.far[1].wait_recv()
        self.near.append(self.send(links.xo, self.b, links.sib))
        for copy in self.near:
            copy.wait_recv()


def reduce_scatter(links, product, part, near, relay, from_left, from_right, fillers=()):
    chips, _, rows, cols = part.shape
    half = cols // 2
    unit = half // sum(SPLIT)
    starts = [unit * sum(SPLIT[:step]) for step in range(STEPS)]
    x, c, xr, xl, xo = links.x, links.c, links.xr, links.xl, links.xo
    swap, first, last = [None] * STEPS, [None] * STEPS, []

    def spans(step):
        width = unit * SPLIT[step]
        return pl.ds(starts[step], width), pl.ds(half + starts[step], width)

    def make(step):
        swap[step] = []
        for span in spans(step):
            part[:, :, :, span] = product(span.start, span.size).reshape(chips, CORES, rows, span.size)
            swap[step].append(links.copy(part.at[:, 1 - c, :, span], near.at[:, :, span], links.sib))

    def send(step):
        span_a, span_b = spans(step)
        for copy, span in zip(swap[step], (span_a, span_b)):
            copy.wait_recv()
            part[:, c, :, span] = part[:, c, :, span] + near[:, :, span]
        first[step] = (
            links.copy(part.at[xo, c, :, span_a], relay.at[0, :, span_a], links.right),
            links.copy(part.at[xo, c, :, span_b], relay.at[1, :, span_a], links.left))
        last.append(links.copy(part.at[xr, c, :, span_b], from_left.at[:, span_b], links.right))
        last.append(links.copy(part.at[xl, c, :, span_a], from_right.at[:, span_a], links.left))

    def pass_on(step):
        span_a, span_b = spans(step)
        first[step][0].wait_recv()
        part[xr, c, :, span_a] = part[xr, c, :, span_a] + relay[0, :, span_a]
        last.append(links.copy(part.at[xr, c, :, span_a], from_left.at[:, span_a], links.right))
        first[step][1].wait_recv()
        part[xl, c, :, span_b] = part[xl, c, :, span_b] + relay[1, :, span_a]
        last.append(links.copy(part.at[xl, c, :, span_b], from_right.at[:, span_b], links.left))

    for step in range(STEPS):
        with jax.named_scope(f'make{step}'):
            make(step)
        if step:
            with jax.named_scope(f'send{step - 1}'):
                send(step - 1)
    with jax.named_scope(f'send{STEPS - 1}'):
        send(STEPS - 1)
    with jax.named_scope('fillers'):
        for filler in fillers:
            filler()
    for step in range(STEPS):
        with jax.named_scope(f'pass_on{step}'):
            pass_on(step)
    with jax.named_scope('last'):
        for copy in last:
            copy.wait_recv()
    return part[x, c] + from_left[...] + from_right[...]


def rms_norm(hidden, gain):
    hidden_f = hidden.astype(F32)
    inv_rms = lax.rsqrt(jnp.mean(hidden_f * hidden_f, axis=-1, keepdims=True) + NORM_EPS)
    return (hidden_f * inv_rms * gain).astype(BF16)


def rms_norm_pull(hidden, gain, cotangent):
    hidden_f, cot = hidden.astype(F32), cotangent.astype(F32)
    inv_rms = lax.rsqrt(jnp.mean(hidden_f * hidden_f, axis=-1, keepdims=True) + NORM_EPS)
    scaled = cot * gain
    dot = jnp.mean(scaled * hidden_f, axis=-1, keepdims=True)
    d_hidden = scaled * inv_rms - hidden_f * (inv_rms * inv_rms * inv_rms * dot)
    return d_hidden.astype(BF16), jnp.sum(cot * (hidden_f * inv_rms), axis=0, keepdims=True)


def flat(ref):
    chips, cores, rows, cols = ref.shape
    return ref[...].reshape(chips * cores * rows, cols)


def project(full, weight, out, tile):
    def body(index, carry):
        cols = pl.ds(pl.multiple_of(index * tile, tile), tile)
        out[:, cols] = dot_nn(flat(full), weight[:, cols]).astype(BF16)
        return carry
    lax.fori_loop(0, out.shape[1] // tile, body, 0)


def project_t(full, weight, out, tile):
    def body(index, carry):
        span = pl.ds(pl.multiple_of(index * tile, tile), tile)
        out[:, span] = dot_nt(flat(full), weight[span, :]).astype(BF16)
        return carry
    lax.fori_loop(0, out.shape[1] // tile, body, 0)


def head(ref, index):
    return ref[:, index * HEAD_DIM:(index + 1) * HEAD_DIM]


def attention(qkv, heads_out, probs=None):
    group = heads_out.shape[1] // HEAD_DIM
    seq = qkv.shape[0]
    causal = lax.broadcasted_iota(jnp.int32, (seq, seq), 0) >= lax.broadcasted_iota(jnp.int32, (seq, seq), 1)
    for index in range(group):
        scores = dot_nt(head(qkv, index), head(qkv, group)) * HEAD_DIM ** -0.5
        scores = jnp.where(causal, scores, -1e30)
        weight = jnp.exp(scores - jnp.max(scores, axis=-1, keepdims=True))
        prob = weight / jnp.sum(weight, axis=-1, keepdims=True)
        if probs is not None:
            probs[index] = prob
        heads_out[:, index * HEAD_DIM:(index + 1) * HEAD_DIM] = dot_nn(prob.astype(BF16), head(qkv, group + 1)).astype(BF16)


def attention_pull(qkv, probs, d_heads, d_qkv):
    group = d_heads.shape[1] // HEAD_DIM
    d_keys = d_values = None
    for index in range(group):
        d_out, prob = head(d_heads, index), probs[index]
        d_prob = dot_nt(d_out, head(qkv, group + 1))
        d_value = dot_tn(prob.astype(BF16), d_out)
        d_score = (prob * (d_prob - jnp.sum(d_prob * prob, axis=-1, keepdims=True)) * HEAD_DIM ** -0.5).astype(BF16)
        d_qkv[:, index * HEAD_DIM:(index + 1) * HEAD_DIM] = dot_nn(d_score, head(qkv, group)).astype(BF16)
        d_key = dot_tn(d_score, head(qkv, index))
        d_keys = d_key if d_keys is None else d_keys + d_key
        d_values = d_value if d_values is None else d_values + d_value
    d_qkv[:, group * HEAD_DIM:(group + 1) * HEAD_DIM] = d_keys.astype(BF16)
    d_qkv[:, (group + 1) * HEAD_DIM:(group + 2) * HEAD_DIM] = d_values.astype(BF16)


def load(src, dst, sem):
    copy = pltpu.make_async_copy(src, dst, sem)
    copy.start()
    return copy


def forward_kernel(layers, chips, hidden, gain_attn, gain_mlp, w_qkv, w_out, w_gate, w_up, w_down, *refs):
    outs, refs = refs[:layers], refs[layers:]
    (wq, wo, wg, wu, wd, full_in, full_mid, qkv, heads_out, act, part, near, relay, from_left, from_right,
     state, load_sem, send_sem, recv_sem) = refs
    links = Links(chips, send_sem, recv_sem)
    state[...] = hidden[...]
    links.enter((links.right, links.left, links.sib))
    pairs = ((w_qkv, wq), (w_out, wo), (w_gate, wg), (w_up, wu), (w_down, wd))

    def one_layer(layer, carry):
        links.used = 0
        row = pl.ds(layer, 1)
        loads = [load(src.at[layer], dst, load_sem.at[index]) for index, (src, dst) in enumerate(pairs)]
        with jax.named_scope('norm_in'):
            full_in[links.x, links.c] = rms_norm(state[...], gain_attn[row, :])
        gather = Gather(links, full_in)
        gather.relay()
        gather.finish()
        loads[0].wait()
        with jax.named_scope('qkv'):
            project(full_in, wq, qkv, qkv.shape[1])
        with jax.named_scope('attention'):
            attention(qkv, heads_out)
        loads[1].wait()
        total = reduce_scatter(links, lambda col, width: dot_nn(heads_out[...], wo[:, pl.ds(col, width)]),
                               part, near.at[0], relay.at[0], from_left.at[0], from_right.at[0])
        with jax.named_scope('norm_mid'):
            hidden_mid = state[...] + total.astype(BF16)
            full_mid[links.x, links.c] = rms_norm(hidden_mid, gain_mlp[row, :])
            state[...] = hidden_mid
        links.drain()
        gather = Gather(links, full_mid)
        gather.relay()
        gather.finish()
        for copy in loads[2:]:
            copy.wait()
        tile = 2 * HEAD_DIM

        def body(index, carry):
            cols = pl.ds(pl.multiple_of(index * tile, tile), tile)
            gate_act = dot_nn(flat(full_mid), wg[:, cols]).astype(BF16).astype(F32)
            up_act = dot_nn(flat(full_mid), wu[:, cols]).astype(BF16).astype(F32)
            act[:, cols] = (gate_act * jax.nn.sigmoid(gate_act) * up_act).astype(BF16)
            return carry
        with jax.named_scope('gate_up'):
            lax.fori_loop(0, act.shape[1] // tile, body, 0)
        total = reduce_scatter(links, lambda col, width: dot_nn(act[...], wd[:, pl.ds(col, width)]),
                               part, near.at[1], relay.at[1], from_left.at[1], from_right.at[1])
        state[...] = state[...] + total.astype(BF16)
        for index, out in enumerate(outs):
            @pl.when(layer == index)
            def _(out=out):
                out[...] = state[...]
        links.drain()
        return carry
    lax.fori_loop(0, layers, one_layer, 0)


def turn(src, dst):
    seq = dst.shape[1]
    tile = HEAD_DIM if dst.shape[0] % (2 * HEAD_DIM) else 2 * HEAD_DIM

    def body(index, carry):
        span = pl.ds(pl.multiple_of(index * tile, tile), tile)
        block = src[:, :, :, span].reshape(seq, tile) if len(src.shape) == 4 else src[:, span]
        dst[span, :] = block.T
        return carry
    lax.fori_loop(0, dst.shape[0] // tile, body, 0)


def backward_kernel(layer, chips, final, hidden, d_out, gain_attn, gain_mlp, w_qkv, w_out, w_gate, w_up, w_down, *refs):
    carried, refs = (refs[0], refs[1:]) if final else (None, refs)
    (d_hidden, gains, o_in, o_mid, o_down, o_attn, o_act, o_gate, o_up, o_heads, o_qkv,
     wq, wo, wgu, wd, full_in, full_mid, full_down, full_attn, qkv, heads_out, act, d_gu, d_heads, d_qkv,
     probs, t_in, t_mid, t_act, t_heads, part, near, relay, from_left, from_right, gain_mid, gain_last,
     load_sem, save_sem, send_sem, recv_sem) = refs
    links = Links(chips, send_sem, recv_sem)
    x, c = links.x, links.c
    units = act.shape[1]
    left, right = pl.ds(0, units), pl.ds(units, units)
    wg, wu, d_gate, d_up = wgu.at[:, left], wgu.at[:, right], d_gu.at[:, left], d_gu.at[:, right]
    pairs = ((w_qkv, wq), (w_out, wo), (w_gate, wg), (w_up, wu), (w_down, wd))
    loads = [load(src.at[layer], dst, load_sem.at[index]) for index, (src, dst) in enumerate(pairs)]
    saves = []

    def save(src, dst):
        saves.append(load(src, dst, save_sem.at[len(saves)]))

    row = pl.ds(layer, 1)
    full_in[x, c] = rms_norm(hidden[...], gain_attn[row, :])
    full_down[x, c] = d_out[...]
    links.enter(links.others() if final else (links.right, links.left, links.sib))
    gather = Gather(links, full_in)
    gather.relay()
    gather_down = Gather(links, full_down)
    gather.finish()
    loads[0].wait()
    with jax.named_scope('qkv'):
        project(full_in, wq, qkv, qkv.shape[1])
    gather_down.relay()
    with jax.named_scope('attention'):
        attention(qkv, heads_out, probs)
    loads[1].wait()

    def gated():
        gather_down.finish()
        save(full_down, o_down)
        loads[4].wait()
        project_t(full_down, wd, act, 2 * HEAD_DIM)

    def turn_in():
        turn(full_in, t_in)
        turn(heads_out, t_heads)
        save(t_in, o_in)
        save(t_heads, o_heads)

    def turn_mid():
        turn(full_mid, t_mid)
        turn(act, t_act)
        save(t_mid, o_mid)
        save(t_act, o_act)

    total = reduce_scatter(links, lambda col, width: dot_nn(heads_out[...], wo[:, pl.ds(col, width)]),
                           part, near.at[0], relay.at[0], from_left.at[0], from_right.at[0], [gated, turn_in])
    hidden_mid = hidden[...] + total.astype(BF16)
    d_hidden[...] = hidden_mid
    full_mid[x, c] = rms_norm(hidden_mid, gain_mlp[row, :])
    links.drain()
    gather = Gather(links, full_mid)
    gather.relay()
    gather.finish()
    loads[2].wait()
    loads[3].wait()
    tile = 2 * HEAD_DIM

    def body(index, carry):
        cols = pl.ds(pl.multiple_of(index * tile, tile), tile)
        gate_act = dot_nn(flat(full_mid), wg[:, cols]).astype(BF16).astype(F32)
        up_act = dot_nn(flat(full_mid), wu[:, cols]).astype(BF16).astype(F32)
        sig = jax.nn.sigmoid(gate_act)
        silu = gate_act * sig
        d_act = act[:, cols].astype(F32)
        d_up[:, cols] = (d_act * silu).astype(BF16)
        d_gate[:, cols] = (d_act * up_act * (sig + silu * (1.0 - sig))).astype(BF16)
        act[:, cols] = (silu * up_act).astype(BF16)
        return carry
    with jax.named_scope('gate_up'):
        lax.fori_loop(0, act.shape[1] // tile, body, 0)
    save(d_gate, o_gate)
    save(d_up, o_up)

    def mid_product(col, width):
        return dot_nt(d_gu[...], wgu[pl.ds(col, width), :])

    total = reduce_scatter(links, mid_product, part, near.at[1], relay.at[1], from_left.at[1], from_right.at[1],
                           [turn_mid])
    with jax.named_scope('pull_mid'):
        d_norm, d_gain = rms_norm_pull(d_hidden[...], gain_mlp[row, :], total.astype(BF16))
    d_mid = d_out[...] + d_norm
    full_attn[x, c] = d_mid
    d_hidden[...] = d_mid
    links.drain()
    gather = Gather(links, full_attn)
    lanes = gain_mid.shape[2]
    done = carried.shape[0] if final else 0

    def put(ref, index, value):
        for line in range(lanes):
            ref[index, line:line + 1, :] = value[:, line * HEAD_DIM:(line + 1) * HEAD_DIM]

    mine = gain_mid.at[links.me]
    if final:
        mine[1:done + 1] = carried[...]
    put(mine, 0, d_gain)
    gather.relay()
    gather.finish()
    save(full_attn, o_attn)
    shares = []
    if final:
        shares = [links.copy(mine, mine, peer) for peer in links.others()]
    with jax.named_scope('d_heads'):
        project_t(full_attn, wo, d_heads, d_heads.shape[1])
    with jax.named_scope('attention_pull'):
        attention_pull(qkv, probs, d_heads, d_qkv)
    save(d_qkv, o_qkv)
    total = reduce_scatter(links, lambda col, width: dot_nt(d_qkv[...], wq[pl.ds(col, width), :]),
                           part, near.at[2], relay.at[2], from_left.at[2], from_right.at[2])
    with jax.named_scope('pull_in'):
        d_norm, d_gain = rms_norm_pull(hidden[...], gain_attn[row, :], total.astype(BF16))
    mine_last = gain_last.at[links.me]
    put(mine_last, 0, d_gain)
    if final:
        shares += [links.copy(mine_last, mine_last, peer) for peer in links.others()]
    d_hidden[...] = d_hidden[...] + d_norm
    if final:
        with jax.named_scope('shares'):
            for copy in shares:
                copy.wait_recv()
        size = chips * CORES
        gains[1:done + 2] = sum([gain_mid[peer] for peer in range(1, size)], gain_mid[0])
        gains[0:1] = sum([gain_last[peer] for peer in range(1, size)], gain_last[0])
    else:
        gains[0:1] = mine_last[...]
        gains[1:2] = mine[...]
    with jax.named_scope('saves'):
        for copy in saves:
            copy.wait()
        links.drain()


def grads_kernel(layer, fresh, final, *refs):
    ins, refs = refs[:9], refs[9:]
    small, refs = (refs[:3], refs[3:]) if final else (None, refs)
    if not fresh:
        refs = refs[5:]
    outs, refs = refs[:5], refs[5:]
    small_outs, refs = (refs[:4], refs[4:]) if final else (None, refs)
    bufs, stages, (load_sem, save_sem) = refs[:9], refs[9:14], refs[14:]
    t_in, t_mid, full_down, full_attn, t_act, d_gate, d_up, t_heads, d_qkv = bufs
    loads = {}

    def fetch(*names):
        for name in names:
            loads[name] = load(ins[name], bufs[name], load_sem.at[name])

    fetch(8, 0)
    jobs = ((t_in, d_qkv, 0, 1024, (8, 0)), (t_heads, full_attn, 1, 192, (7, 3)), (t_mid, d_gate, 2, 512, (1, 5)),
            (t_mid, d_up, 3, 512, (6,)), (t_act, full_down, 4, 256, (4, 2)))
    stores = []
    for left, right, place, size, needs in jobs:
        for index in needs:
            loads[index].wait()
        if not place:
            fetch(7, 3, 1, 5, 6, 4, 2)
        out, stage = outs[place], stages[place]
        rows, cols = out.shape[1], out.shape[2]

        def body(index, carry, left=left, right=right, size=size, cols=cols, out=out, stage=stage, place=place):
            span = pl.ds(pl.multiple_of(index * size, size), size)
            turned = left[span, :]
            for col in range(0, cols, 256):
                width = min(256, cols - col)
                if len(right.shape) == 4:
                    chips, cores, some, _ = right.shape
                    piece = right[:, :, :, col:col + width].reshape(chips * cores * some, width)
                else:
                    piece = right[:, col:col + width]
                stage[span, col:col + width] = dot_nn(turned, piece).astype(BF16)
            load(stage.at[span, :], out.at[layer, span, :], save_sem.at[place])
            return carry
        with jax.named_scope(f'job{place}'):
            lax.fori_loop(0, rows // size, body, 0)
        stores.append(pltpu.make_async_copy(stage, out.at[layer], save_sem.at[place]))
    if final:
        small_outs[0][...] = small[0][...]
        small_outs[1][...] = small[1][...]
        for index in range(small[2].shape[0]):
            target = small_outs[2 + index % 2]
            for line in range(small[2].shape[1]):
                target[index // 2:index // 2 + 1, line * HEAD_DIM:(line + 1) * HEAD_DIM] = small[2][index, line:line + 1, :]
    with jax.named_scope('stores'):
        for copy in stores:
            copy.wait()


def vmem(*shape, dtype=BF16):
    return pltpu.VMEM(shape, dtype)


def solution(mesh):
    chips = mesh.shape['tp'] // CORES
    row_spec = P(('dp', 'tp'), None)
    col_spec = P(None, None, 'tp')
    mid_spec = P(None, 'tp', None)
    in_specs = (row_spec, row_spec, P(None, None), P(None, None), col_spec, mid_spec, col_spec, col_spec, mid_spec)
    out_specs = (row_spec, row_spec, P('dp', None, 'tp'), P('dp', 'tp', None), P('dp', None, 'tp'), P('dp', None, 'tp'), P('dp', 'tp', None), P('dp', None), P('dp', None))

    def device_step(x, grad_y, gain_attn, gain_mlp, w_qkv, w_out, w_gate, w_up, w_down):
        layers, width, qkv_cols = w_qkv.shape
        head_cols, units, rows = w_out.shape[1], w_gate.shape[2], x.shape[0]
        group = head_cols // HEAD_DIM
        seq = chips * CORES * rows
        lanes = width // HEAD_DIM
        full = (chips, CORES, rows, width)
        weights = (w_qkv, w_out, w_gate, w_up, w_down)
        weight_bufs = [vmem(*weight.shape[1:]) for weight in weights]

        def ring_bufs(uses):
            return [vmem(*full, dtype=F32), vmem(uses, chips, rows, width, dtype=F32), vmem(uses, 2, rows, width // 2, dtype=F32),
                    vmem(uses, rows, width, dtype=F32), vmem(uses, rows, width, dtype=F32)]

        def dma(count):
            return pltpu.SemaphoreType.DMA((count,))

        def params(ident):
            return pltpu.CompilerParams(collective_id=ident, has_side_effects=True, vmem_limit_bytes=VMEM_LIMIT)

        def forward(hidden):
            copies = 2 * 13 + 2 * 8 * STEPS
            return pl.pallas_call(
                functools.partial(forward_kernel, layers, chips),
                out_shape=[jax.ShapeDtypeStruct(hidden.shape, BF16)] * layers,
                in_specs=[VMEM_SPEC] * 3 + [ANY] * 5,
                out_specs=[VMEM_SPEC] * layers,
                scratch_shapes=weight_bufs + [vmem(*full), vmem(*full), vmem(seq, qkv_cols), vmem(seq, head_cols), vmem(seq, units)]
                + ring_bufs(2) + [vmem(*hidden.shape), dma(5), dma(copies), dma(copies)],
                compiler_params=params(layers), name='forward',
            )(hidden, gain_attn, gain_mlp, *weights)

        def backward(layer, hidden, d_out, carried):
            final = layer == 0
            peers = chips * CORES - 1
            copies = 4 * 13 + 3 * 8 * STEPS + 2 * peers
            done = carried[0].shape[0] if final else 0
            factor = lambda *shape: jax.ShapeDtypeStruct(shape, BF16)
            return pl.pallas_call(
                functools.partial(backward_kernel, layer, chips, final),
                out_shape=[factor(*hidden.shape), jax.ShapeDtypeStruct((done + 2, lanes, HEAD_DIM), F32)]
                + [factor(width, seq)] * 2 + [factor(*full)] * 2
                + [factor(units, seq), factor(seq, units), factor(seq, units), factor(head_cols, seq), factor(seq, qkv_cols)],
                in_specs=[VMEM_SPEC] * 4 + [ANY] * 5 + [VMEM_SPEC] * len(carried),
                out_specs=[VMEM_SPEC] * 2 + [ANY] * 9,
                scratch_shapes=weight_bufs[:2] + [vmem(width, 2 * units), weight_bufs[4]] + [vmem(*full)] * 4
                + [vmem(seq, qkv_cols), vmem(seq, head_cols), vmem(seq, units), vmem(seq, 2 * units),
                   vmem(seq, head_cols), vmem(seq, qkv_cols), vmem(group, seq, seq, dtype=F32),
                   vmem(width, seq), vmem(width, seq), vmem(units, seq), vmem(head_cols, seq)] + ring_bufs(3)
                + [vmem(chips * CORES, done + 1, lanes, HEAD_DIM, dtype=F32), vmem(chips * CORES, 1, lanes, HEAD_DIM, dtype=F32),
                   dma(5), dma(9), dma(copies), dma(copies)],
                compiler_params=params(layer), name=f'backward_{layer}',
            )(hidden, d_out, gain_attn, gain_mlp, *weights, *carried)

        grad_shapes = [jax.ShapeDtypeStruct(weight.shape, BF16) for weight in weights]

        def grads(layer, factors, small, into):
            fresh, final = not into, layer == 0
            shapes = [jax.ShapeDtypeStruct(value.shape, value.dtype) for value in (x, x, gain_attn, gain_mlp)]
            return pl.pallas_call(
                functools.partial(grads_kernel, layer, fresh, final),
                out_shape=grad_shapes + (shapes if final else []),
                in_specs=[ANY] * len(factors) + [VMEM_SPEC] * len(small) + [ANY] * len(into),
                out_specs=[ANY] * 5 + [VMEM_SPEC] * (4 if final else 0),
                scratch_shapes=[vmem(*factor.shape) for factor in factors] + [vmem(*weight.shape[1:]) for weight in weights]
                + [dma(len(factors)), dma(5)],
                input_output_aliases={len(factors) + len(small) + index: index for index in range(len(into))},
                compiler_params=pltpu.CompilerParams(vmem_limit_bytes=VMEM_LIMIT), name=f'grads_{layer}',
            )(*factors, *small, *into)

        kept = [x, *forward(x)]
        d_hidden, out_grads, partial_gains = grad_y, [], []
        for layer in reversed(range(layers)):
            carried = [jnp.concatenate(partial_gains[::-1])] if layer == 0 else []
            d_hidden, gains, *factors = backward(layer, kept[layer], d_hidden, carried)
            partial_gains.append(gains)
            if layer:
                out_grads = grads(layer, factors, [], out_grads)
                d_hidden, *out_grads = lax.optimization_barrier((d_hidden, *out_grads))
        *out_grads, y, grad_x, grad_attn, grad_mlp = grads(0, factors, [kept[-1], d_hidden, gains], out_grads)
        return (y, grad_x, *out_grads, grad_attn, grad_mlp)

    return jax.shard_map(device_step, mesh=mesh, in_specs=in_specs, out_specs=out_specs, check_vma=False)
```

```python
import functools
import itertools

import jax
import jax.numpy as jnp
from jax import lax
from jax.experimental import pallas as pl
from jax.experimental.pallas import tpu as pltpu
from jax.sharding import PartitionSpec as P

HEAD_DIM = 128
NORM_EPS = 1e-5
CORES = 2
MESH = pl.DeviceIdType.MESH
F32 = jnp.float32
BF16 = jnp.bfloat16
VMEM_LIMIT = 66_000_000
SPLIT = (2, 2, 4, 4)
STEPS = len(SPLIT)
GATHER, GATHER_DOWN, SCATTER = 0, 13, 26
SHARE = SCATTER + 8 * STEPS + 2
ANY = pl.BlockSpec(memory_space=pltpu.HBM)
VMEM_SPEC = pl.BlockSpec(memory_space=pltpu.VMEM)


def dot_nn(a, b):
    return lax.dot_general(a, b, (((1,), (0,)), ((), ())), preferred_element_type=F32)


def dot_nt(a, b):
    return lax.dot_general(a, b, (((1,), (1,)), ((), ())), preferred_element_type=F32)


def dot_tn(a, b):
    return lax.dot_general(a, b, (((0,), (0,)), ((), ())), preferred_element_type=F32)


class Links:
    def __init__(self, chips, send_sem, recv_sem):
        self.me = lax.axis_index('tp')
        self.chips = chips
        self.x = lax.div(self.me, CORES)
        self.c = lax.rem(self.me, CORES)
        self.xr = lax.rem(self.x + 1, chips)
        self.xl = lax.rem(self.x + chips - 1, chips)
        self.xo = lax.rem(self.x + 2, chips)
        self.right = self.xr * CORES + self.c
        self.left = self.xl * CORES + self.c
        self.sib = self.x * CORES + 1 - self.c
        self.right_far, self.left_far = self.xr * CORES + 1 - self.c, self.xl * CORES + 1 - self.c
        self.near = (self.right, self.left, self.sib, self.right_far, self.left_far)
        self.send_sem, self.recv_sem, self.pending = send_sem, recv_sem, []

    def enter(self, peers):
        barrier = pltpu.get_barrier_semaphore()
        for peer in peers:
            pl.semaphore_signal(barrier, inc=1, device_id={'tp': peer}, device_id_type=MESH)
        pl.semaphore_wait(barrier, len(peers))

    def others(self):
        size = self.chips * CORES
        return [lax.rem(self.me + step, size) for step in range(1, size)]

    def copy(self, src, dst, peer, bank):
        index = next(bank)
        copy = pltpu.make_async_remote_copy(
            src_ref=src, dst_ref=dst, send_sem=self.send_sem.at[index], recv_sem=self.recv_sem.at[index],
            device_id={'tp': peer}, device_id_type=MESH)
        copy.start()
        self.pending.append(copy)
        return copy

    def drain(self):
        for copy in self.pending:
            copy.wait_send()
        self.pending = []


class Gather:
    def __init__(self, links, full, bank=GATHER):
        self.links, self.full, self.bank = links, full, itertools.count(bank)
        self.half = full.shape[3] // 2
        part_a, part_b = pl.ds(0, self.half), pl.ds(self.half, self.half)
        x, c = links.x, links.c
        self.a, self.b = part_a, part_b
        self.right_a = self.send(x, part_a, links.right)
        self.left_b = self.send(x, part_b, links.left)
        self.right_b = self.send(x, part_b, links.right)
        self.left_a = self.send(x, part_a, links.left)
        self.near = [links.copy(full.at[x, c], full.at[x, c], links.sib, self.bank)]

    def send(self, chip, part, peer):
        ref = self.full.at[chip, self.links.c, :, part]
        return self.links.copy(ref, ref, peer, self.bank)

    @jax.named_scope('gather')
    def relay(self):
        links = self.links
        self.right_a.wait_recv()
        relay_a = self.send(links.xl, self.a, links.right)
        self.near.append(self.send(links.xl, self.a, links.sib))
        self.left_b.wait_recv()
        relay_b = self.send(links.xr, self.b, links.left)
        self.near.append(self.send(links.xr, self.b, links.sib))
        self.far = (relay_a, relay_b)

    @jax.named_scope('finish')
    def finish(self):
        links = self.links
        self.right_b.wait_recv()
        self.near.append(self.send(links.xl, self.b, links.sib))
        self.left_a.wait_recv()
        self.near.append(self.send(links.xr, self.a, links.sib))
        self.far[0].wait_recv()
        self.near.append(self.send(links.xo, self.a, links.sib))
        self.far[1].wait_recv()
        self.near.append(self.send(links.xo, self.b, links.sib))
        for copy in self.near:
            copy.wait_recv()


def reduce_scatter(links, product, part, near, relay, from_left, from_right, fillers=()):
    chips, _, rows, cols = part.shape
    half = cols // 2
    unit = half // sum(SPLIT)
    starts = [unit * sum(SPLIT[:step]) for step in range(STEPS)]
    x, c, xr, xl, xo = links.x, links.c, links.xr, links.xl, links.xo
    swap, first, last = [None] * STEPS, [None] * STEPS, []
    bank = itertools.count(SCATTER)

    def copy_to(src, dst, peer):
        return links.copy(src, dst, peer, bank)

    def spans(step):
        width = unit * SPLIT[step]
        return pl.ds(starts[step], width), pl.ds(half + starts[step], width)

    def make(step):
        swap[step] = []
        span_a, span_b = spans(step)
        for span in (span_a, span_b):
            part[:, :, :, span] = product(span.start, span.size).reshape(chips, CORES, rows, span.size)
            swap[step].append(copy_to(part.at[:, 1 - c, :, span], near.at[:, :, span], links.sib))
        if not step:
            first[step] = (
                (copy_to(part.at[xo, c, :, span_a], relay.at[0, :, span_a], links.right),
                 copy_to(part.at[xo, 1 - c, :, span_a], relay.at[2, :, span_a], links.right_far)),
                (copy_to(part.at[xo, c, :, span_b], relay.at[1, :, span_a], links.left),
                 copy_to(part.at[xo, 1 - c, :, span_b], relay.at[3, :, span_a], links.left_far)))

    def send(step):
        span_a, span_b = spans(step)
        for copy, span in zip(swap[step], (span_a, span_b)):
            copy.wait_recv()
            if step:
                part[:, c, :, span] = part[:, c, :, span] + near[:, :, span]
            else:
                for chip in (x, xr, xl):
                    part[chip, c, :, span] = part[chip, c, :, span] + near[chip, :, span]
        if step:
            first[step] = (
                (copy_to(part.at[xo, c, :, span_a], relay.at[0, :, span_a], links.right),),
                (copy_to(part.at[xo, c, :, span_b], relay.at[1, :, span_a], links.left),))
        last.append(copy_to(part.at[xr, c, :, span_b], from_left.at[:, span_b], links.right))
        last.append(copy_to(part.at[xl, c, :, span_a], from_right.at[:, span_a], links.left))

    def pass_on(step):
        span_a, span_b = spans(step)
        for way, chip, span, target, peer in ((0, xr, span_a, from_left, links.right), (1, xl, span_b, from_right, links.left)):
            for copy in first[step][way]:
                copy.wait_recv()
            total = part[chip, c, :, span] + relay[way, :, span_a]
            if not step:
                total = total + relay[2 + way, :, span_a]
            part[chip, c, :, span] = total
            last.append(copy_to(part.at[chip, c, :, span], target.at[:, span], peer))

    for step in range(STEPS):
        with jax.named_scope(f'make{step}'):
            make(step)
        if step:
            with jax.named_scope(f'send{step - 1}'):
                send(step - 1)
    with jax.named_scope(f'send{STEPS - 1}'):
        send(STEPS - 1)
    with jax.named_scope('fillers'):
        for filler in fillers:
            filler()
    for step in range(STEPS):
        with jax.named_scope(f'pass_on{step}'):
            pass_on(step)
    with jax.named_scope('last'):
        for copy in last:
            copy.wait_recv()
    return part[x, c] + from_left[...] + from_right[...]


def rms_norm(hidden, gain):
    hidden_f = hidden.astype(F32)
    inv_rms = lax.rsqrt(jnp.mean(hidden_f * hidden_f, axis=-1, keepdims=True) + NORM_EPS)
    return (hidden_f * inv_rms * gain).astype(BF16)


def rms_norm_pull(hidden, gain, cotangent):
    hidden_f, cot = hidden.astype(F32), cotangent.astype(F32)
    inv_rms = lax.rsqrt(jnp.mean(hidden_f * hidden_f, axis=-1, keepdims=True) + NORM_EPS)
    scaled = cot * gain
    dot = jnp.mean(scaled * hidden_f, axis=-1, keepdims=True)
    d_hidden = scaled * inv_rms - hidden_f * (inv_rms * inv_rms * inv_rms * dot)
    return d_hidden.astype(BF16), jnp.sum(cot * (hidden_f * inv_rms), axis=0, keepdims=True)


def flat(ref):
    chips, cores, rows, cols = ref.shape
    return ref[...].reshape(chips * cores * rows, cols)


def project(full, weight, out, tile):
    def body(index, carry):
        cols = pl.ds(pl.multiple_of(index * tile, tile), tile)
        out[:, cols] = dot_nn(flat(full), weight[:, cols]).astype(BF16)
        return carry
    lax.fori_loop(0, out.shape[1] // tile, body, 0)


def project_t(full, weight, out, tile):
    def body(index, carry):
        span = pl.ds(pl.multiple_of(index * tile, tile), tile)
        out[:, span] = dot_nt(flat(full), weight[span, :]).astype(BF16)
        return carry
    lax.fori_loop(0, out.shape[1] // tile, body, 0)


def head(ref, index):
    return ref[:, index * HEAD_DIM:(index + 1) * HEAD_DIM]


def attention(qkv, heads_out, probs=None):
    group = heads_out.shape[1] // HEAD_DIM
    seq = qkv.shape[0]
    causal = lax.broadcasted_iota(jnp.int32, (seq, seq), 0) >= lax.broadcasted_iota(jnp.int32, (seq, seq), 1)
    for index in range(group):
        scores = dot_nt(head(qkv, index), head(qkv, group)) * HEAD_DIM ** -0.5
        scores = jnp.where(causal, scores, -1e30)
        weight = jnp.exp(scores - jnp.max(scores, axis=-1, keepdims=True))
        prob = weight / jnp.sum(weight, axis=-1, keepdims=True)
        if probs is not None:
            probs[index] = prob
        heads_out[:, index * HEAD_DIM:(index + 1) * HEAD_DIM] = dot_nn(prob.astype(BF16), head(qkv, group + 1)).astype(BF16)


def attention_pull(qkv, probs, d_heads, d_qkv):
    group = d_heads.shape[1] // HEAD_DIM
    d_keys = d_values = None
    for index in range(group):
        d_out, prob = head(d_heads, index), probs[index]
        d_prob = dot_nt(d_out, head(qkv, group + 1))
        d_value = dot_tn(prob.astype(BF16), d_out)
        d_score = (prob * (d_prob - jnp.sum(d_prob * prob, axis=-1, keepdims=True)) * HEAD_DIM ** -0.5).astype(BF16)
        d_qkv[:, index * HEAD_DIM:(index + 1) * HEAD_DIM] = dot_nn(d_score, head(qkv, group)).astype(BF16)
        d_key = dot_tn(d_score, head(qkv, index))
        d_keys = d_key if d_keys is None else d_keys + d_key
        d_values = d_value if d_values is None else d_values + d_value
    d_qkv[:, group * HEAD_DIM:(group + 1) * HEAD_DIM] = d_keys.astype(BF16)
    d_qkv[:, (group + 1) * HEAD_DIM:(group + 2) * HEAD_DIM] = d_values.astype(BF16)


def load(src, dst, sem):
    copy = pltpu.make_async_copy(src, dst, sem)
    copy.start()
    return copy


def forward_kernel(layers, chips, hidden, gain_attn, gain_mlp, w_qkv, w_out, w_gate, w_up, w_down, *refs):
    outs, refs = refs[:layers], refs[layers:]
    (wq, wo, wg, wu, wd, full_in, full_mid, qkv, heads_out, act, part, near, relay, from_left, from_right,
     state, load_sem, send_sem, recv_sem) = refs
    links = Links(chips, send_sem, recv_sem)
    state[...] = hidden[...]
    links.enter(links.near)
    pairs = ((w_qkv, wq), (w_out, wo), (w_gate, wg), (w_up, wu), (w_down, wd))

    def one_layer(layer, carry):
        row = pl.ds(layer, 1)
        loads = [load(src.at[layer], dst, load_sem.at[index]) for index, (src, dst) in enumerate(pairs)]
        with jax.named_scope('norm_in'):
            full_in[links.x, links.c] = rms_norm(state[...], gain_attn[row, :])
        gather = Gather(links, full_in)
        gather.relay()
        gather.finish()
        loads[0].wait()
        with jax.named_scope('qkv'):
            project(full_in, wq, qkv, qkv.shape[1])
        with jax.named_scope('attention'):
            attention(qkv, heads_out)
        loads[1].wait()
        total = reduce_scatter(links, lambda col, width: dot_nn(heads_out[...], wo[:, pl.ds(col, width)]),
                               part, near.at[0], relay.at[0], from_left.at[0], from_right.at[0])
        with jax.named_scope('norm_mid'):
            hidden_mid = state[...] + total.astype(BF16)
            full_mid[links.x, links.c] = rms_norm(hidden_mid, gain_mlp[row, :])
            state[...] = hidden_mid
        links.drain()
        gather = Gather(links, full_mid)
        gather.relay()
        gather.finish()
        for copy in loads[2:]:
            copy.wait()
        tile = 2 * HEAD_DIM

        def body(index, carry):
            cols = pl.ds(pl.multiple_of(index * tile, tile), tile)
            gate_act = dot_nn(flat(full_mid), wg[:, cols]).astype(BF16).astype(F32)
            up_act = dot_nn(flat(full_mid), wu[:, cols]).astype(BF16).astype(F32)
            act[:, cols] = (gate_act * jax.nn.sigmoid(gate_act) * up_act).astype(BF16)
            return carry
        with jax.named_scope('gate_up'):
            lax.fori_loop(0, act.shape[1] // tile, body, 0, unroll=2)
        total = reduce_scatter(links, lambda col, width: dot_nn(act[...], wd[:, pl.ds(col, width)]),
                               part, near.at[1], relay.at[1], from_left.at[1], from_right.at[1])
        state[...] = state[...] + total.astype(BF16)
        for index, out in enumerate(outs):
            @pl.when(layer == index)
            def _(out=out):
                out[...] = state[...]
        links.drain()
        return carry
    lax.fori_loop(0, layers, one_layer, 0)


def turn(src, dst):
    seq = dst.shape[1]
    tile = HEAD_DIM if dst.shape[0] % (2 * HEAD_DIM) else 2 * HEAD_DIM

    def body(index, carry):
        span = pl.ds(pl.multiple_of(index * tile, tile), tile)
        block = src[:, :, :, span].reshape(seq, tile) if len(src.shape) == 4 else src[:, span]
        dst[span, :] = block.T
        return carry
    lax.fori_loop(0, dst.shape[0] // tile, body, 0)


def backward_kernel(layer, chips, final, hidden, d_out, gain_attn, gain_mlp, w_qkv, w_out, w_gate, w_up, w_down, *refs):
    carried, refs = (refs[0], refs[1:]) if final else (None, refs)
    (d_hidden, gains, o_in, o_mid, o_down, o_attn, o_act, o_gate, o_up, o_heads, o_qkv,
     wq, wo, wgu, wd, full_in, full_mid, full_down, full_attn, qkv, heads_out, act, d_gu, d_heads, d_qkv,
     probs, t_in, t_mid, t_act, t_heads, part, near, relay, from_left, from_right, gain_mid, gain_last,
     load_sem, save_sem, send_sem, recv_sem) = refs
    links = Links(chips, send_sem, recv_sem)
    x, c = links.x, links.c
    units = act.shape[1]
    left, right = pl.ds(0, units), pl.ds(units, units)
    wg, wu, d_gate, d_up = wgu.at[:, left], wgu.at[:, right], d_gu.at[:, left], d_gu.at[:, right]
    pairs = ((w_qkv, wq), (w_out, wo), (w_gate, wg), (w_up, wu), (w_down, wd))
    loads = [load(src.at[layer], dst, load_sem.at[index]) for index, (src, dst) in enumerate(pairs)]
    saves = []

    def save(src, dst):
        saves.append(load(src, dst, save_sem.at[len(saves)]))

    row = pl.ds(layer, 1)
    full_in[x, c] = rms_norm(hidden[...], gain_attn[row, :])
    full_down[x, c] = d_out[...]
    links.enter(links.others() if final else links.near)
    gather = Gather(links, full_in)
    gather.relay()
    gather_down = Gather(links, full_down, GATHER_DOWN)
    gather.finish()
    loads[0].wait()
    with jax.named_scope('qkv'):
        project(full_in, wq, qkv, qkv.shape[1])
    gather_down.relay()
    with jax.named_scope('attention'):
        attention(qkv, heads_out, probs)
    loads[1].wait()

    def gated():
        gather_down.finish()
        save(full_down, o_down)
        loads[4].wait()
        project_t(full_down, wd, act, 2 * HEAD_DIM)

    def turn_in():
        turn(full_in, t_in)
        turn(heads_out, t_heads)
        save(t_in, o_in)
        save(t_heads, o_heads)

    def turn_mid():
        turn(full_mid, t_mid)
        turn(act, t_act)
        save(t_mid, o_mid)
        save(t_act, o_act)

    total = reduce_scatter(links, lambda col, width: dot_nn(heads_out[...], wo[:, pl.ds(col, width)]),
                           part, near.at[0], relay.at[0], from_left.at[0], from_right.at[0], [gated, turn_in])
    hidden_mid = hidden[...] + total.astype(BF16)
    d_hidden[...] = hidden_mid
    full_mid[x, c] = rms_norm(hidden_mid, gain_mlp[row, :])
    links.drain()
    gather = Gather(links, full_mid)
    gather.relay()
    gather.finish()
    loads[2].wait()
    loads[3].wait()
    tile = 2 * HEAD_DIM

    def body(index, carry):
        cols = pl.ds(pl.multiple_of(index * tile, tile), tile)
        gate_act = dot_nn(flat(full_mid), wg[:, cols]).astype(BF16).astype(F32)
        up_act = dot_nn(flat(full_mid), wu[:, cols]).astype(BF16).astype(F32)
        sig = jax.nn.sigmoid(gate_act)
        silu = gate_act * sig
        d_act = act[:, cols].astype(F32)
        d_up[:, cols] = (d_act * silu).astype(BF16)
        d_gate[:, cols] = (d_act * up_act * (sig + silu * (1.0 - sig))).astype(BF16)
        act[:, cols] = (silu * up_act).astype(BF16)
        return carry
    with jax.named_scope('gate_up'):
        lax.fori_loop(0, act.shape[1] // tile, body, 0, unroll=2)
    save(d_gate, o_gate)
    save(d_up, o_up)

    def mid_product(col, width):
        return dot_nt(d_gu[...], wgu[pl.ds(col, width), :])

    total = reduce_scatter(links, mid_product, part, near.at[1], relay.at[1], from_left.at[1], from_right.at[1],
                           [turn_mid])
    with jax.named_scope('pull_mid'):
        d_norm, d_gain = rms_norm_pull(d_hidden[...], gain_mlp[row, :], total.astype(BF16))
    d_mid = d_out[...] + d_norm
    full_attn[x, c] = d_mid
    d_hidden[...] = d_mid
    links.drain()
    gather = Gather(links, full_attn)
    lanes = gain_mid.shape[2]
    done = carried.shape[0] if final else 0

    def put(ref, index, value):
        for line in range(lanes):
            ref[index, line:line + 1, :] = value[:, line * HEAD_DIM:(line + 1) * HEAD_DIM]

    mine = gain_mid.at[links.me]
    if final:
        mine[1:done + 1] = carried[...]
    put(mine, 0, d_gain)
    gather.relay()
    gather.finish()
    save(full_attn, o_attn)
    shares, bank = [], itertools.count(SHARE)
    if final:
        shares = [links.copy(mine, mine, peer, bank) for peer in links.others()]
    with jax.named_scope('d_heads'):
        project_t(full_attn, wo, d_heads, d_heads.shape[1])
    with jax.named_scope('attention_pull'):
        attention_pull(qkv, probs, d_heads, d_qkv)
    save(d_qkv, o_qkv)
    total = reduce_scatter(links, lambda col, width: dot_nt(d_qkv[...], wq[pl.ds(col, width), :]),
                           part, near.at[2], relay.at[2], from_left.at[2], from_right.at[2])
    with jax.named_scope('pull_in'):
        d_norm, d_gain = rms_norm_pull(hidden[...], gain_attn[row, :], total.astype(BF16))
    mine_last = gain_last.at[links.me]
    put(mine_last, 0, d_gain)
    if final:
        shares += [links.copy(mine_last, mine_last, peer, bank) for peer in links.others()]
    d_hidden[...] = d_hidden[...] + d_norm
    if final:
        with jax.named_scope('shares'):
            for copy in shares:
                copy.wait_recv()
        size = chips * CORES
        gains[1:done + 2] = sum([gain_mid[peer] for peer in range(1, size)], gain_mid[0])
        gains[0:1] = sum([gain_last[peer] for peer in range(1, size)], gain_last[0])
    else:
        gains[0:1] = mine_last[...]
        gains[1:2] = mine[...]
    with jax.named_scope('saves'):
        for copy in saves:
            copy.wait()
        links.drain()


def grads_kernel(layer, fresh, final, *refs):
    ins, refs = refs[:9], refs[9:]
    small, refs = (refs[:3], refs[3:]) if final else (None, refs)
    if not fresh:
        refs = refs[5:]
    outs, refs = refs[:5], refs[5:]
    small_outs, refs = (refs[:4], refs[4:]) if final else (None, refs)
    bufs, stages, (load_sem, save_sem) = refs[:9], refs[9:14], refs[14:]
    t_in, t_mid, full_down, full_attn, t_act, d_gate, d_up, t_heads, d_qkv = bufs
    loads = {}

    def fetch(*names):
        for name in names:
            loads[name] = load(ins[name], bufs[name], load_sem.at[name])

    fetch(8, 0)
    jobs = ((t_in, d_qkv, 0, 1024, (8, 0)), (t_heads, full_attn, 1, 192, (7, 3)), (t_mid, d_gate, 2, 512, (1, 5)),
            (t_mid, d_up, 3, 512, (6,)), (t_act, full_down, 4, 256, (4, 2)))
    stores = []
    for left, right, place, size, needs in jobs:
        for index in needs:
            loads[index].wait()
        if not place:
            fetch(7, 3, 1, 5, 6, 4, 2)
        out, stage = outs[place], stages[place]
        rows, cols = out.shape[1], out.shape[2]

        def body(index, carry, left=left, right=right, size=size, cols=cols, out=out, stage=stage, place=place):
            span = pl.ds(pl.multiple_of(index * size, size), size)
            turned = left[span, :]
            for col in range(0, cols, 256):
                width = min(256, cols - col)
                if len(right.shape) == 4:
                    chips, cores, some, _ = right.shape
                    piece = right[:, :, :, col:col + width].reshape(chips * cores * some, width)
                else:
                    piece = right[:, col:col + width]
                stage[span, col:col + width] = dot_nn(turned, piece).astype(BF16)
            load(stage.at[span, :], out.at[layer, span, :], save_sem.at[place])
            return carry
        with jax.named_scope(f'job{place}'):
            lax.fori_loop(0, rows // size, body, 0)
        stores.append(pltpu.make_async_copy(stage, out.at[layer], save_sem.at[place]))
    if final:
        small_outs[0][...] = small[0][...]
        small_outs[1][...] = small[1][...]
        for index in range(small[2].shape[0]):
            target = small_outs[2 + index % 2]
            for line in range(small[2].shape[1]):
                target[index // 2:index // 2 + 1, line * HEAD_DIM:(line + 1) * HEAD_DIM] = small[2][index, line:line + 1, :]
    with jax.named_scope('stores'):
        for copy in stores:
            copy.wait()


def vmem(*shape, dtype=BF16):
    return pltpu.VMEM(shape, dtype)


def solution(mesh):
    chips = mesh.shape['tp'] // CORES
    row_spec = P(('dp', 'tp'), None)
    col_spec = P(None, None, 'tp')
    mid_spec = P(None, 'tp', None)
    in_specs = (row_spec, row_spec, P(None, None), P(None, None), col_spec, mid_spec, col_spec, col_spec, mid_spec)
    out_specs = (row_spec, row_spec, P('dp', None, 'tp'), P('dp', 'tp', None), P('dp', None, 'tp'), P('dp', None, 'tp'), P('dp', 'tp', None), P('dp', None), P('dp', None))

    def device_step(x, grad_y, gain_attn, gain_mlp, w_qkv, w_out, w_gate, w_up, w_down):
        layers, width, qkv_cols = w_qkv.shape
        head_cols, units, rows = w_out.shape[1], w_gate.shape[2], x.shape[0]
        group = head_cols // HEAD_DIM
        seq = chips * CORES * rows
        lanes = width // HEAD_DIM
        full = (chips, CORES, rows, width)
        weights = (w_qkv, w_out, w_gate, w_up, w_down)
        weight_bufs = [vmem(*weight.shape[1:]) for weight in weights]

        def ring_bufs(uses):
            return [vmem(*full, dtype=F32), vmem(uses, chips, rows, width, dtype=F32), vmem(uses, 4, rows, width // 2, dtype=F32),
                    vmem(uses, rows, width, dtype=F32), vmem(uses, rows, width, dtype=F32)]

        def dma(count):
            return pltpu.SemaphoreType.DMA((count,))

        def params(ident):
            return pltpu.CompilerParams(collective_id=ident, has_side_effects=True, vmem_limit_bytes=VMEM_LIMIT)

        def forward(hidden):
            copies = SHARE
            return pl.pallas_call(
                functools.partial(forward_kernel, layers, chips),
                out_shape=[jax.ShapeDtypeStruct(hidden.shape, BF16)] * layers,
                in_specs=[VMEM_SPEC] * 3 + [ANY] * 5,
                out_specs=[VMEM_SPEC] * layers,
                scratch_shapes=weight_bufs + [vmem(*full), vmem(*full), vmem(seq, qkv_cols), vmem(seq, head_cols), vmem(seq, units)]
                + ring_bufs(2) + [vmem(*hidden.shape), dma(5), dma(copies), dma(copies)],
                compiler_params=params(layers), name='forward',
            )(hidden, gain_attn, gain_mlp, *weights)

        def backward(layer, hidden, d_out, carried):
            final = layer == 0
            copies = SHARE + (2 * (chips * CORES - 1) if final else 0)
            done = carried[0].shape[0] if final else 0
            factor = lambda *shape: jax.ShapeDtypeStruct(shape, BF16)
            return pl.pallas_call(
                functools.partial(backward_kernel, layer, chips, final),
                out_shape=[factor(*hidden.shape), jax.ShapeDtypeStruct((done + 2, lanes, HEAD_DIM), F32)]
                + [factor(width, seq)] * 2 + [factor(*full)] * 2
                + [factor(units, seq), factor(seq, units), factor(seq, units), factor(head_cols, seq), factor(seq, qkv_cols)],
                in_specs=[VMEM_SPEC] * 4 + [ANY] * 5 + [VMEM_SPEC] * len(carried),
                out_specs=[VMEM_SPEC] * 2 + [ANY] * 9,
                scratch_shapes=weight_bufs[:2] + [vmem(width, 2 * units), weight_bufs[4]] + [vmem(*full)] * 4
                + [vmem(seq, qkv_cols), vmem(seq, head_cols), vmem(seq, units), vmem(seq, 2 * units),
                   vmem(seq, head_cols), vmem(seq, qkv_cols), vmem(group, seq, seq, dtype=F32),
                   vmem(width, seq), vmem(width, seq), vmem(units, seq), vmem(head_cols, seq)] + ring_bufs(3)
                + [vmem(chips * CORES, done + 1, lanes, HEAD_DIM, dtype=F32), vmem(chips * CORES, 1, lanes, HEAD_DIM, dtype=F32),
                   dma(5), dma(9), dma(copies), dma(copies)],
                compiler_params=params(layer), name=f'backward_{layer}',
            )(hidden, d_out, gain_attn, gain_mlp, *weights, *carried)

        grad_shapes = [jax.ShapeDtypeStruct(weight.shape, BF16) for weight in weights]

        def grads(layer, factors, small, into):
            fresh, final = not into, layer == 0
            shapes = [jax.ShapeDtypeStruct(value.shape, value.dtype) for value in (x, x, gain_attn, gain_mlp)]
            return pl.pallas_call(
                functools.partial(grads_kernel, layer, fresh, final),
                out_shape=grad_shapes + (shapes if final else []),
                in_specs=[ANY] * len(factors) + [VMEM_SPEC] * len(small) + [ANY] * len(into),
                out_specs=[ANY] * 5 + [VMEM_SPEC] * (4 if final else 0),
                scratch_shapes=[vmem(*factor.shape) for factor in factors] + [vmem(*weight.shape[1:]) for weight in weights]
                + [dma(len(factors)), dma(5)],
                input_output_aliases={len(factors) + len(small) + index: index for index in range(len(into))},
                compiler_params=pltpu.CompilerParams(vmem_limit_bytes=VMEM_LIMIT), name=f'grads_{layer}',
            )(*factors, *small, *into)

        kept = [x, *forward(x)]
        d_hidden, out_grads, partial_gains = grad_y, [], []
        for layer in reversed(range(layers)):
            carried = [jnp.concatenate(partial_gains[::-1])] if layer == 0 else []
            d_hidden, gains, *factors = backward(layer, kept[layer], d_hidden, carried)
            partial_gains.append(gains)
            if layer:
                out_grads = grads(layer, factors, [], out_grads)
                d_hidden, *out_grads = lax.optimization_barrier((d_hidden, *out_grads))
        *out_grads, y, grad_x, grad_attn, grad_mlp = grads(0, factors, [kept[-1], d_hidden, gains], out_grads)
        return (y, grad_x, *out_grads, grad_attn, grad_mlp)

    return jax.shard_map(device_step, mesh=mesh, in_specs=in_specs, out_specs=out_specs, check_vma=False)
```

```python
import functools
import itertools

import jax
import jax.numpy as jnp
from jax import lax
from jax.experimental import pallas as pl
from jax.experimental.pallas import tpu as pltpu
from jax.sharding import PartitionSpec as P

HEAD_DIM = 128
NORM_EPS = 1e-5
CORES = 2
MESH = pl.DeviceIdType.MESH
F32 = jnp.float32
BF16 = jnp.bfloat16
VMEM_LIMIT = 66_000_000
SPLIT = (2, 2, 4, 4)
STEPS = len(SPLIT)
GATHER, GATHER_DOWN, SCATTER = 0, 13, 26
SHARE = SCATTER + 8 * STEPS + 2
ANY = pl.BlockSpec(memory_space=pltpu.HBM)
VMEM_SPEC = pl.BlockSpec(memory_space=pltpu.VMEM)


def dot_nn(a, b):
    return lax.dot_general(a, b, (((1,), (0,)), ((), ())), preferred_element_type=F32)


def dot_nt(a, b):
    return lax.dot_general(a, b, (((1,), (1,)), ((), ())), preferred_element_type=F32)


def dot_tn(a, b):
    return lax.dot_general(a, b, (((0,), (0,)), ((), ())), preferred_element_type=F32)


class Links:
    def __init__(self, chips, send_sem, recv_sem):
        self.me = lax.axis_index('tp')
        self.chips = chips
        self.x = lax.div(self.me, CORES)
        self.c = lax.rem(self.me, CORES)
        self.xr = lax.rem(self.x + 1, chips)
        self.xl = lax.rem(self.x + chips - 1, chips)
        self.xo = lax.rem(self.x + 2, chips)
        self.right = self.xr * CORES + self.c
        self.left = self.xl * CORES + self.c
        self.sib = self.x * CORES + 1 - self.c
        self.right_far, self.left_far = self.xr * CORES + 1 - self.c, self.xl * CORES + 1 - self.c
        self.near = (self.right, self.left, self.sib, self.right_far, self.left_far)
        self.send_sem, self.recv_sem, self.pending = send_sem, recv_sem, []

    def enter(self, peers):
        barrier = pltpu.get_barrier_semaphore()
        for peer in peers:
            pl.semaphore_signal(barrier, inc=1, device_id={'tp': peer}, device_id_type=MESH)
        pl.semaphore_wait(barrier, len(peers))

    def others(self):
        size = self.chips * CORES
        return [lax.rem(self.me + step, size) for step in range(1, size)]

    def copy(self, src, dst, peer, bank):
        index = next(bank)
        copy = pltpu.make_async_remote_copy(
            src_ref=src, dst_ref=dst, send_sem=self.send_sem.at[index], recv_sem=self.recv_sem.at[index],
            device_id={'tp': peer}, device_id_type=MESH)
        copy.start()
        self.pending.append(copy)
        return copy

    def drain(self):
        for copy in self.pending:
            copy.wait_send()
        self.pending = []


class Gather:
    def __init__(self, links, full, bank=GATHER):
        self.links, self.full, self.bank = links, full, itertools.count(bank)
        self.half = full.shape[3] // 2
        part_a, part_b = pl.ds(0, self.half), pl.ds(self.half, self.half)
        x, c = links.x, links.c
        self.a, self.b = part_a, part_b
        self.right_a = self.send(x, part_a, links.right)
        self.left_b = self.send(x, part_b, links.left)
        self.right_b = self.send(x, part_b, links.right)
        self.left_a = self.send(x, part_a, links.left)
        self.near = [links.copy(full.at[x, c], full.at[x, c], links.sib, self.bank)]

    def send(self, chip, part, peer):
        ref = self.full.at[chip, self.links.c, :, part]
        return self.links.copy(ref, ref, peer, self.bank)

    @jax.named_scope('gather')
    def relay(self):
        links = self.links
        self.right_a.wait_recv()
        relay_a = self.send(links.xl, self.a, links.right)
        self.near.append(self.send(links.xl, self.a, links.sib))
        self.left_b.wait_recv()
        relay_b = self.send(links.xr, self.b, links.left)
        self.near.append(self.send(links.xr, self.b, links.sib))
        self.far = (relay_a, relay_b)

    @jax.named_scope('finish')
    def finish(self):
        links = self.links
        self.right_b.wait_recv()
        self.near.append(self.send(links.xl, self.b, links.sib))
        self.left_a.wait_recv()
        self.near.append(self.send(links.xr, self.a, links.sib))
        self.far[0].wait_recv()
        self.near.append(self.send(links.xo, self.a, links.sib))
        self.far[1].wait_recv()
        self.near.append(self.send(links.xo, self.b, links.sib))
        for copy in self.near:
            copy.wait_recv()


def reduce_scatter(links, product, part, near, relay, from_left, from_right, fillers=()):
    chips, _, rows, cols = part.shape
    half = cols // 2
    unit = half // sum(SPLIT)
    starts = [unit * sum(SPLIT[:step]) for step in range(STEPS)]
    x, c, xr, xl, xo = links.x, links.c, links.xr, links.xl, links.xo
    swap, first, last = [None] * STEPS, [None] * STEPS, []
    bank = itertools.count(SCATTER)

    def copy_to(src, dst, peer):
        return links.copy(src, dst, peer, bank)

    def spans(step):
        width = unit * SPLIT[step]
        return pl.ds(starts[step], width), pl.ds(half + starts[step], width)

    def make(step):
        swap[step] = []
        span_a, span_b = spans(step)
        both = product(span_a, span_b).reshape(chips, CORES, rows, 2 * span_a.size)
        part[:, :, :, span_a] = both[:, :, :, :span_a.size]
        part[:, :, :, span_b] = both[:, :, :, span_a.size:]
        for span in (span_a, span_b):
            swap[step].append(copy_to(part.at[:, 1 - c, :, span], near.at[:, :, span], links.sib))
        if not step:
            first[step] = (
                (copy_to(part.at[xo, c, :, span_a], relay.at[0, :, span_a], links.right),
                 copy_to(part.at[xo, 1 - c, :, span_a], relay.at[2, :, span_a], links.right_far)),
                (copy_to(part.at[xo, c, :, span_b], relay.at[1, :, span_a], links.left),
                 copy_to(part.at[xo, 1 - c, :, span_b], relay.at[3, :, span_a], links.left_far)))

    def send(step):
        span_a, span_b = spans(step)
        for copy, span in zip(swap[step], (span_a, span_b)):
            copy.wait_recv()
            if step:
                part[:, c, :, span] = part[:, c, :, span] + near[:, :, span]
            else:
                for chip in (x, xr, xl):
                    part[chip, c, :, span] = part[chip, c, :, span] + near[chip, :, span]
        if step:
            first[step] = (
                (copy_to(part.at[xo, c, :, span_a], relay.at[0, :, span_a], links.right),),
                (copy_to(part.at[xo, c, :, span_b], relay.at[1, :, span_a], links.left),))
        last.append(copy_to(part.at[xr, c, :, span_b], from_left.at[:, span_b], links.right))
        last.append(copy_to(part.at[xl, c, :, span_a], from_right.at[:, span_a], links.left))

    def pass_on(step):
        span_a, span_b = spans(step)
        for way, chip, span, target, peer in ((0, xr, span_a, from_left, links.right), (1, xl, span_b, from_right, links.left)):
            for copy in first[step][way]:
                copy.wait_recv()
            total = part[chip, c, :, span] + relay[way, :, span_a]
            if not step:
                total = total + relay[2 + way, :, span_a]
            part[chip, c, :, span] = total
            last.append(copy_to(part.at[chip, c, :, span], target.at[:, span], peer))

    for step in range(STEPS):
        with jax.named_scope(f'make{step}'):
            make(step)
        if step:
            with jax.named_scope(f'send{step - 1}'):
                send(step - 1)
    with jax.named_scope(f'send{STEPS - 1}'):
        send(STEPS - 1)
    with jax.named_scope('fillers'):
        for filler in fillers:
            filler()
    for step in range(STEPS):
        with jax.named_scope(f'pass_on{step}'):
            pass_on(step)
    with jax.named_scope('last'):
        for copy in last:
            copy.wait_recv()
    return part[x, c] + from_left[...] + from_right[...]


def rms_norm(hidden, gain):
    hidden_f = hidden.astype(F32)
    inv_rms = lax.rsqrt(jnp.mean(hidden_f * hidden_f, axis=-1, keepdims=True) + NORM_EPS)
    return (hidden_f * inv_rms * gain).astype(BF16)


def rms_norm_pull(hidden, gain, cotangent):
    hidden_f, cot = hidden.astype(F32), cotangent.astype(F32)
    inv_rms = lax.rsqrt(jnp.mean(hidden_f * hidden_f, axis=-1, keepdims=True) + NORM_EPS)
    scaled = cot * gain
    dot = jnp.mean(scaled * hidden_f, axis=-1, keepdims=True)
    d_hidden = scaled * inv_rms - hidden_f * (inv_rms * inv_rms * inv_rms * dot)
    return d_hidden.astype(BF16), jnp.sum(cot * (hidden_f * inv_rms), axis=0, keepdims=True)


def columns(ref, *spans):
    return jnp.concatenate([ref[:, span] for span in spans], axis=1)


def lines(ref, *spans):
    return jnp.concatenate([ref[span, :] for span in spans], axis=0)


def flat(ref):
    chips, cores, rows, cols = ref.shape
    return ref[...].reshape(chips * cores * rows, cols)


def project(full, weight, out, tile):
    def body(index, carry):
        cols = pl.ds(pl.multiple_of(index * tile, tile), tile)
        out[:, cols] = dot_nn(flat(full), weight[:, cols]).astype(BF16)
        return carry
    lax.fori_loop(0, out.shape[1] // tile, body, 0)


def project_t(full, weight, out, tile):
    def body(index, carry):
        span = pl.ds(pl.multiple_of(index * tile, tile), tile)
        out[:, span] = dot_nt(flat(full), weight[span, :]).astype(BF16)
        return carry
    lax.fori_loop(0, out.shape[1] // tile, body, 0)


def head(ref, index):
    return ref[:, index * HEAD_DIM:(index + 1) * HEAD_DIM]


def attention(qkv, heads_out, probs=None):
    group = heads_out.shape[1] // HEAD_DIM
    seq = qkv.shape[0]
    causal = lax.broadcasted_iota(jnp.int32, (seq, seq), 0) >= lax.broadcasted_iota(jnp.int32, (seq, seq), 1)
    for index in range(group):
        scores = dot_nt(head(qkv, index), head(qkv, group)) * HEAD_DIM ** -0.5
        scores = jnp.where(causal, scores, -1e30)
        weight = jnp.exp(scores - jnp.max(scores, axis=-1, keepdims=True))
        prob = weight / jnp.sum(weight, axis=-1, keepdims=True)
        if probs is not None:
            probs[index] = prob
        heads_out[:, index * HEAD_DIM:(index + 1) * HEAD_DIM] = dot_nn(prob.astype(BF16), head(qkv, group + 1)).astype(BF16)


def attention_pull(qkv, probs, d_heads, d_qkv):
    group = d_heads.shape[1] // HEAD_DIM
    d_keys = d_values = None
    for index in range(group):
        d_out, prob = head(d_heads, index), probs[index]
        d_prob = dot_nt(d_out, head(qkv, group + 1))
        d_value = dot_tn(prob.astype(BF16), d_out)
        d_score = (prob * (d_prob - jnp.sum(d_prob * prob, axis=-1, keepdims=True)) * HEAD_DIM ** -0.5).astype(BF16)
        d_qkv[:, index * HEAD_DIM:(index + 1) * HEAD_DIM] = dot_nn(d_score, head(qkv, group)).astype(BF16)
        d_key = dot_tn(d_score, head(qkv, index))
        d_keys = d_key if d_keys is None else d_keys + d_key
        d_values = d_value if d_values is None else d_values + d_value
    d_qkv[:, group * HEAD_DIM:(group + 1) * HEAD_DIM] = d_keys.astype(BF16)
    d_qkv[:, (group + 1) * HEAD_DIM:(group + 2) * HEAD_DIM] = d_values.astype(BF16)


def load(src, dst, sem):
    copy = pltpu.make_async_copy(src, dst, sem)
    copy.start()
    return copy


def forward_kernel(layers, chips, hidden, gain_attn, gain_mlp, w_qkv, w_out, w_gate, w_up, w_down, *refs):
    outs, refs = refs[:layers], refs[layers:]
    (wq, wo, wg, wu, wd, full_in, full_mid, qkv, heads_out, act, part, near, relay, from_left, from_right,
     state, load_sem, send_sem, recv_sem) = refs
    links = Links(chips, send_sem, recv_sem)
    state[...] = hidden[...]
    links.enter(links.near)
    pairs = ((w_qkv, wq), (w_out, wo), (w_gate, wg), (w_up, wu), (w_down, wd))

    def one_layer(layer, carry):
        row = pl.ds(layer, 1)
        loads = [load(src.at[layer], dst, load_sem.at[index]) for index, (src, dst) in enumerate(pairs)]
        with jax.named_scope('norm_in'):
            full_in[links.x, links.c] = rms_norm(state[...], gain_attn[row, :])
        gather = Gather(links, full_in)
        gather.relay()
        gather.finish()
        loads[0].wait()
        with jax.named_scope('qkv'):
            project(full_in, wq, qkv, qkv.shape[1])
        with jax.named_scope('attention'):
            attention(qkv, heads_out)
        loads[1].wait()
        total = reduce_scatter(links, lambda *spans: dot_nn(heads_out[...], columns(wo, *spans)),
                               part, near.at[0], relay.at[0], from_left.at[0], from_right.at[0])
        with jax.named_scope('norm_mid'):
            hidden_mid = state[...] + total.astype(BF16)
            full_mid[links.x, links.c] = rms_norm(hidden_mid, gain_mlp[row, :])
            state[...] = hidden_mid
        links.drain()
        gather = Gather(links, full_mid)
        gather.relay()
        gather.finish()
        for copy in loads[2:]:
            copy.wait()
        tile = 2 * HEAD_DIM

        def body(index, carry):
            cols = pl.ds(pl.multiple_of(index * tile, tile), tile)
            both = dot_nn(flat(full_mid), jnp.concatenate([wg[:, cols], wu[:, cols]], axis=1)).astype(BF16).astype(F32)
            gate_act, up_act = both[:, :tile], both[:, tile:]
            act[:, cols] = (gate_act * jax.nn.sigmoid(gate_act) * up_act).astype(BF16)
            return carry
        with jax.named_scope('gate_up'):
            lax.fori_loop(0, act.shape[1] // tile, body, 0, unroll=2)
        total = reduce_scatter(links, lambda *spans: dot_nn(act[...], columns(wd, *spans)),
                               part, near.at[1], relay.at[1], from_left.at[1], from_right.at[1])
        state[...] = state[...] + total.astype(BF16)
        for index, out in enumerate(outs):
            @pl.when(layer == index)
            def _(out=out):
                out[...] = state[...]
        links.drain()
        return carry
    lax.fori_loop(0, layers, one_layer, 0)


def turn(src, dst):
    seq = dst.shape[1]
    tile = HEAD_DIM if dst.shape[0] % (2 * HEAD_DIM) else 2 * HEAD_DIM

    def body(index, carry):
        span = pl.ds(pl.multiple_of(index * tile, tile), tile)
        block = src[:, :, :, span].reshape(seq, tile) if len(src.shape) == 4 else src[:, span]
        dst[span, :] = block.T
        return carry
    lax.fori_loop(0, dst.shape[0] // tile, body, 0)


def backward_kernel(layer, chips, final, hidden, d_out, gain_attn, gain_mlp, w_qkv, w_out, w_gate, w_up, w_down, *refs):
    carried, refs = (refs[0], refs[1:]) if final else (None, refs)
    (d_hidden, gains, o_in, o_mid, o_down, o_attn, o_act, o_gate, o_up, o_heads, o_qkv,
     wq, wo, wgu, wd, full_in, full_mid, full_down, full_attn, qkv, heads_out, act, d_gu, d_heads, d_qkv,
     probs, t_in, t_mid, t_act, t_heads, part, near, relay, from_left, from_right, gain_mid, gain_last,
     load_sem, save_sem, send_sem, recv_sem) = refs
    links = Links(chips, send_sem, recv_sem)
    x, c = links.x, links.c
    units = act.shape[1]
    left, right = pl.ds(0, units), pl.ds(units, units)
    wg, wu, d_gate, d_up = wgu.at[:, left], wgu.at[:, right], d_gu.at[:, left], d_gu.at[:, right]
    pairs = ((w_qkv, wq), (w_out, wo), (w_gate, wg), (w_up, wu), (w_down, wd))
    loads = [load(src.at[layer], dst, load_sem.at[index]) for index, (src, dst) in enumerate(pairs)]
    saves = []

    def save(src, dst):
        saves.append(load(src, dst, save_sem.at[len(saves)]))

    row = pl.ds(layer, 1)
    full_in[x, c] = rms_norm(hidden[...], gain_attn[row, :])
    full_down[x, c] = d_out[...]
    links.enter(links.others() if final else links.near)
    gather = Gather(links, full_in)
    gather.relay()
    gather_down = Gather(links, full_down, GATHER_DOWN)
    gather.finish()
    loads[0].wait()
    with jax.named_scope('qkv'):
        project(full_in, wq, qkv, qkv.shape[1])
    gather_down.relay()
    with jax.named_scope('attention'):
        attention(qkv, heads_out, probs)
    loads[1].wait()

    def gated():
        gather_down.finish()
        save(full_down, o_down)
        loads[4].wait()
        project_t(full_down, wd, act, 4 * HEAD_DIM)

    def turn_in():
        turn(full_in, t_in)
        turn(heads_out, t_heads)
        save(t_in, o_in)
        save(t_heads, o_heads)

    def turn_mid():
        turn(full_mid, t_mid)
        turn(act, t_act)
        save(t_mid, o_mid)
        save(t_act, o_act)

    total = reduce_scatter(links, lambda *spans: dot_nn(heads_out[...], columns(wo, *spans)),
                           part, near.at[0], relay.at[0], from_left.at[0], from_right.at[0], [gated, turn_in])
    hidden_mid = hidden[...] + total.astype(BF16)
    d_hidden[...] = hidden_mid
    full_mid[x, c] = rms_norm(hidden_mid, gain_mlp[row, :])
    links.drain()
    gather = Gather(links, full_mid)
    gather.relay()
    gather.finish()
    loads[2].wait()
    loads[3].wait()
    tile = 2 * HEAD_DIM

    def body(index, carry):
        cols = pl.ds(pl.multiple_of(index * tile, tile), tile)
        both = dot_nn(flat(full_mid), jnp.concatenate([wg[:, cols], wu[:, cols]], axis=1)).astype(BF16).astype(F32)
        gate_act, up_act = both[:, :tile], both[:, tile:]
        sig = jax.nn.sigmoid(gate_act)
        silu = gate_act * sig
        d_act = act[:, cols].astype(F32)
        d_up[:, cols] = (d_act * silu).astype(BF16)
        d_gate[:, cols] = (d_act * up_act * (sig + silu * (1.0 - sig))).astype(BF16)
        act[:, cols] = (silu * up_act).astype(BF16)
        return carry
    with jax.named_scope('gate_up'):
        lax.fori_loop(0, act.shape[1] // tile, body, 0, unroll=2)
    save(d_gate, o_gate)
    save(d_up, o_up)

    def mid_product(*spans):
        return dot_nt(d_gu[...], lines(wgu, *spans))

    total = reduce_scatter(links, mid_product, part, near.at[1], relay.at[1], from_left.at[1], from_right.at[1],
                           [turn_mid])
    with jax.named_scope('pull_mid'):
        d_norm, d_gain = rms_norm_pull(d_hidden[...], gain_mlp[row, :], total.astype(BF16))
    d_mid = d_out[...] + d_norm
    full_attn[x, c] = d_mid
    d_hidden[...] = d_mid
    links.drain()
    gather = Gather(links, full_attn)
    lanes = gain_mid.shape[2]
    done = carried.shape[0] if final else 0

    def put(ref, index, value):
        for line in range(lanes):
            ref[index, line:line + 1, :] = value[:, line * HEAD_DIM:(line + 1) * HEAD_DIM]

    mine = gain_mid.at[links.me]
    if final:
        mine[1:done + 1] = carried[...]
    put(mine, 0, d_gain)
    gather.relay()
    gather.finish()
    save(full_attn, o_attn)
    shares, bank = [], itertools.count(SHARE)
    if final:
        shares = [links.copy(mine, mine, peer, bank) for peer in links.others()]
    with jax.named_scope('d_heads'):
        project_t(full_attn, wo, d_heads, d_heads.shape[1])
    with jax.named_scope('attention_pull'):
        attention_pull(qkv, probs, d_heads, d_qkv)
    save(d_qkv, o_qkv)
    total = reduce_scatter(links, lambda *spans: dot_nt(d_qkv[...], lines(wq, *spans)),
                           part, near.at[2], relay.at[2], from_left.at[2], from_right.at[2])
    with jax.named_scope('pull_in'):
        d_norm, d_gain = rms_norm_pull(hidden[...], gain_attn[row, :], total.astype(BF16))
    mine_last = gain_last.at[links.me]
    put(mine_last, 0, d_gain)
    if final:
        shares += [links.copy(mine_last, mine_last, peer, bank) for peer in links.others()]
    d_hidden[...] = d_hidden[...] + d_norm
    if final:
        with jax.named_scope('shares'):
            for copy in shares:
                copy.wait_recv()
        size = chips * CORES
        gains[1:done + 2] = sum([gain_mid[peer] for peer in range(1, size)], gain_mid[0])
        gains[0:1] = sum([gain_last[peer] for peer in range(1, size)], gain_last[0])
    else:
        gains[0:1] = mine_last[...]
        gains[1:2] = mine[...]
    with jax.named_scope('saves'):
        for copy in saves:
            copy.wait()
        links.drain()


def grads_kernel(layer, fresh, final, *refs):
    ins, refs = refs[:9], refs[9:]
    small, refs = (refs[:3], refs[3:]) if final else (None, refs)
    if not fresh:
        refs = refs[5:]
    outs, refs = refs[:5], refs[5:]
    small_outs, refs = (refs[:4], refs[4:]) if final else (None, refs)
    bufs, stages, (load_sem, save_sem) = refs[:9], refs[9:14], refs[14:]
    t_in, t_mid, full_down, full_attn, t_act, d_gate, d_up, t_heads, d_qkv = bufs
    loads = {}

    def fetch(*names):
        for name in names:
            loads[name] = load(ins[name], bufs[name], load_sem.at[name])

    fetch(8, 0)
    jobs = ((t_in, d_qkv, 0, 1024, (8, 0)), (t_heads, full_attn, 1, 192, (7, 3)), (t_mid, d_gate, 2, 512, (1, 5)),
            (t_mid, d_up, 3, 512, (6,)), (t_act, full_down, 4, 256, (4, 2)))
    stores = []
    for left, right, place, size, needs in jobs:
        for index in needs:
            loads[index].wait()
        if not place:
            fetch(7, 3, 1, 5, 6, 4, 2)
        out, stage = outs[place], stages[place]
        rows, cols = out.shape[1], out.shape[2]

        def body(index, carry, left=left, right=right, size=size, cols=cols, out=out, stage=stage, place=place):
            span = pl.ds(pl.multiple_of(index * size, size), size)
            turned = left[span, :]
            for col in range(0, cols, 512):
                width = min(512, cols - col)
                if len(right.shape) == 4:
                    chips, cores, some, _ = right.shape
                    piece = right[:, :, :, col:col + width].reshape(chips * cores * some, width)
                else:
                    piece = right[:, col:col + width]
                stage[span, col:col + width] = dot_nn(turned, piece).astype(BF16)
            load(stage.at[span, :], out.at[layer, span, :], save_sem.at[place])
            return carry
        with jax.named_scope(f'job{place}'):
            lax.fori_loop(0, rows // size, body, 0)
        stores.append(pltpu.make_async_copy(stage, out.at[layer], save_sem.at[place]))
    if final:
        small_outs[0][...] = small[0][...]
        small_outs[1][...] = small[1][...]
        for index in range(small[2].shape[0]):
            target = small_outs[2 + index % 2]
            for line in range(small[2].shape[1]):
                target[index // 2:index // 2 + 1, line * HEAD_DIM:(line + 1) * HEAD_DIM] = small[2][index, line:line + 1, :]
    with jax.named_scope('stores'):
        for copy in stores:
            copy.wait()


def vmem(*shape, dtype=BF16):
    return pltpu.VMEM(shape, dtype)


def solution(mesh):
    chips = mesh.shape['tp'] // CORES
    row_spec = P(('dp', 'tp'), None)
    col_spec = P(None, None, 'tp')
    mid_spec = P(None, 'tp', None)
    in_specs = (row_spec, row_spec, P(None, None), P(None, None), col_spec, mid_spec, col_spec, col_spec, mid_spec)
    out_specs = (row_spec, row_spec, P('dp', None, 'tp'), P('dp', 'tp', None), P('dp', None, 'tp'), P('dp', None, 'tp'), P('dp', 'tp', None), P('dp', None), P('dp', None))

    def device_step(x, grad_y, gain_attn, gain_mlp, w_qkv, w_out, w_gate, w_up, w_down):
        layers, width, qkv_cols = w_qkv.shape
        head_cols, units, rows = w_out.shape[1], w_gate.shape[2], x.shape[0]
        group = head_cols // HEAD_DIM
        seq = chips * CORES * rows
        lanes = width // HEAD_DIM
        full = (chips, CORES, rows, width)
        weights = (w_qkv, w_out, w_gate, w_up, w_down)
        weight_bufs = [vmem(*weight.shape[1:]) for weight in weights]

        def ring_bufs(uses):
            return [vmem(*full, dtype=F32), vmem(uses, chips, rows, width, dtype=F32), vmem(uses, 4, rows, width // 2, dtype=F32),
                    vmem(uses, rows, width, dtype=F32), vmem(uses, rows, width, dtype=F32)]

        def dma(count):
            return pltpu.SemaphoreType.DMA((count,))

        def params(ident):
            return pltpu.CompilerParams(collective_id=ident, has_side_effects=True, vmem_limit_bytes=VMEM_LIMIT)

        def forward(hidden):
            copies = SHARE
            return pl.pallas_call(
                functools.partial(forward_kernel, layers, chips),
                out_shape=[jax.ShapeDtypeStruct(hidden.shape, BF16)] * layers,
                in_specs=[VMEM_SPEC] * 3 + [ANY] * 5,
                out_specs=[VMEM_SPEC] * layers,
                scratch_shapes=weight_bufs + [vmem(*full), vmem(*full), vmem(seq, qkv_cols), vmem(seq, head_cols), vmem(seq, units)]
                + ring_bufs(2) + [vmem(*hidden.shape), dma(5), dma(copies), dma(copies)],
                compiler_params=params(layers), name='forward',
            )(hidden, gain_attn, gain_mlp, *weights)

        def backward(layer, hidden, d_out, carried):
            final = layer == 0
            copies = SHARE + (2 * (chips * CORES - 1) if final else 0)
            done = carried[0].shape[0] if final else 0
            factor = lambda *shape: jax.ShapeDtypeStruct(shape, BF16)
            return pl.pallas_call(
                functools.partial(backward_kernel, layer, chips, final),
                out_shape=[factor(*hidden.shape), jax.ShapeDtypeStruct((done + 2, lanes, HEAD_DIM), F32)]
                + [factor(width, seq)] * 2 + [factor(*full)] * 2
                + [factor(units, seq), factor(seq, units), factor(seq, units), factor(head_cols, seq), factor(seq, qkv_cols)],
                in_specs=[VMEM_SPEC] * 4 + [ANY] * 5 + [VMEM_SPEC] * len(carried),
                out_specs=[VMEM_SPEC] * 2 + [ANY] * 9,
                scratch_shapes=weight_bufs[:2] + [vmem(width, 2 * units), weight_bufs[4]] + [vmem(*full)] * 4
                + [vmem(seq, qkv_cols), vmem(seq, head_cols), vmem(seq, units), vmem(seq, 2 * units),
                   vmem(seq, head_cols), vmem(seq, qkv_cols), vmem(group, seq, seq, dtype=F32),
                   vmem(width, seq), vmem(width, seq), vmem(units, seq), vmem(head_cols, seq)] + ring_bufs(3)
                + [vmem(chips * CORES, done + 1, lanes, HEAD_DIM, dtype=F32), vmem(chips * CORES, 1, lanes, HEAD_DIM, dtype=F32),
                   dma(5), dma(9), dma(copies), dma(copies)],
                compiler_params=params(layer), name=f'backward_{layer}',
            )(hidden, d_out, gain_attn, gain_mlp, *weights, *carried)

        grad_shapes = [jax.ShapeDtypeStruct(weight.shape, BF16) for weight in weights]

        def grads(layer, factors, small, into):
            fresh, final = not into, layer == 0
            shapes = [jax.ShapeDtypeStruct(value.shape, value.dtype) for value in (x, x, gain_attn, gain_mlp)]
            return pl.pallas_call(
                functools.partial(grads_kernel, layer, fresh, final),
                out_shape=grad_shapes + (shapes if final else []),
                in_specs=[ANY] * len(factors) + [VMEM_SPEC] * len(small) + [ANY] * len(into),
                out_specs=[ANY] * 5 + [VMEM_SPEC] * (4 if final else 0),
                scratch_shapes=[vmem(*factor.shape) for factor in factors] + [vmem(*weight.shape[1:]) for weight in weights]
                + [dma(len(factors)), dma(5)],
                input_output_aliases={len(factors) + len(small) + index: index for index in range(len(into))},
                compiler_params=pltpu.CompilerParams(vmem_limit_bytes=VMEM_LIMIT), name=f'grads_{layer}',
            )(*factors, *small, *into)

        kept = [x, *forward(x)]
        d_hidden, out_grads, partial_gains = grad_y, [], []
        for layer in reversed(range(layers)):
            carried = [jnp.concatenate(partial_gains[::-1])] if layer == 0 else []
            d_hidden, gains, *factors = backward(layer, kept[layer], d_hidden, carried)
            partial_gains.append(gains)
            if layer:
                out_grads = grads(layer, factors, [], out_grads)
                d_hidden, *out_grads = lax.optimization_barrier((d_hidden, *out_grads))
        *out_grads, y, grad_x, grad_attn, grad_mlp = grads(0, factors, [kept[-1], d_hidden, gains], out_grads)
        return (y, grad_x, *out_grads, grad_attn, grad_mlp)

    return jax.shard_map(device_step, mesh=mesh, in_specs=in_specs, out_specs=out_specs, check_vma=False)
```

```python
import functools
import itertools

import jax
import jax.numpy as jnp
from jax import lax
from jax.experimental import pallas as pl
from jax.experimental.pallas import tpu as pltpu
from jax.sharding import PartitionSpec as P

HEAD_DIM = 128
NORM_EPS = 1e-5
CORES = 2
MESH = pl.DeviceIdType.MESH
F32 = jnp.float32
BF16 = jnp.bfloat16
VMEM_LIMIT = 66_000_000
SPLIT = (2, 2, 4, 4)
STEPS = len(SPLIT)
GATHER, GATHER_DOWN, SCATTER = 0, 13, 26
SHARE = SCATTER + 8 * STEPS + 2
ANY = pl.BlockSpec(memory_space=pltpu.HBM)
VMEM_SPEC = pl.BlockSpec(memory_space=pltpu.VMEM)


def dot_nn(a, b):
    return lax.dot_general(a, b, (((1,), (0,)), ((), ())), preferred_element_type=F32)


def dot_nt(a, b):
    return lax.dot_general(a, b, (((1,), (1,)), ((), ())), preferred_element_type=F32)


def dot_tn(a, b):
    return lax.dot_general(a, b, (((0,), (0,)), ((), ())), preferred_element_type=F32)


class Links:
    def __init__(self, chips, send_sem, recv_sem):
        self.me = lax.axis_index('tp')
        self.chips = chips
        self.x = lax.div(self.me, CORES)
        self.c = lax.rem(self.me, CORES)
        self.xr = lax.rem(self.x + 1, chips)
        self.xl = lax.rem(self.x + chips - 1, chips)
        self.xo = lax.rem(self.x + 2, chips)
        self.right = self.xr * CORES + self.c
        self.left = self.xl * CORES + self.c
        self.sib = self.x * CORES + 1 - self.c
        self.right_far, self.left_far = self.xr * CORES + 1 - self.c, self.xl * CORES + 1 - self.c
        self.near = (self.right, self.left, self.sib, self.right_far, self.left_far)
        self.send_sem, self.recv_sem, self.pending = send_sem, recv_sem, []

    def enter(self, peers):
        barrier = pltpu.get_barrier_semaphore()
        for peer in peers:
            pl.semaphore_signal(barrier, inc=1, device_id={'tp': peer}, device_id_type=MESH)
        pl.semaphore_wait(barrier, len(peers))

    def others(self):
        size = self.chips * CORES
        return [lax.rem(self.me + step, size) for step in range(1, size)]

    def copy(self, src, dst, peer, bank):
        index = next(bank)
        copy = pltpu.make_async_remote_copy(
            src_ref=src, dst_ref=dst, send_sem=self.send_sem.at[index], recv_sem=self.recv_sem.at[index],
            device_id={'tp': peer}, device_id_type=MESH)
        copy.start()
        self.pending.append(copy)
        return copy

    def drain(self):
        for copy in self.pending:
            copy.wait_send()
        self.pending = []


class Gather:
    def __init__(self, links, full, bank=GATHER):
        self.links, self.full, self.bank = links, full, itertools.count(bank)
        self.half = full.shape[3] // 2
        part_a, part_b = pl.ds(0, self.half), pl.ds(self.half, self.half)
        x, c = links.x, links.c
        self.a, self.b = part_a, part_b
        self.right_a = self.send(x, part_a, links.right)
        self.left_b = self.send(x, part_b, links.left)
        self.right_b = self.send(x, part_b, links.right)
        self.left_a = self.send(x, part_a, links.left)
        self.near = [links.copy(full.at[x, c], full.at[x, c], links.sib, self.bank)]

    def send(self, chip, part, peer):
        ref = self.full.at[chip, self.links.c, :, part]
        return self.links.copy(ref, ref, peer, self.bank)

    @jax.named_scope('gather')
    def relay(self):
        links = self.links
        self.right_a.wait_recv()
        relay_a = self.send(links.xl, self.a, links.right)
        self.near.append(self.send(links.xl, self.a, links.sib))
        self.left_b.wait_recv()
        relay_b = self.send(links.xr, self.b, links.left)
        self.near.append(self.send(links.xr, self.b, links.sib))
        self.far = (relay_a, relay_b)

    @jax.named_scope('finish')
    def finish(self):
        links = self.links
        self.right_b.wait_recv()
        self.near.append(self.send(links.xl, self.b, links.sib))
        self.left_a.wait_recv()
        self.near.append(self.send(links.xr, self.a, links.sib))
        self.far[0].wait_recv()
        self.near.append(self.send(links.xo, self.a, links.sib))
        self.far[1].wait_recv()
        self.near.append(self.send(links.xo, self.b, links.sib))
        for copy in self.near:
            copy.wait_recv()


def reduce_scatter(links, use, product, ring, fillers=()):
    part, near, relay, from_left, from_right = ring
    _, chips, _, rows, _ = part[0].shape
    half = sum(ref.shape[4] for ref in part)
    x, c, xr, xl, xo = links.x, links.c, links.xr, links.xl, links.xo
    swap, first, last = [None] * STEPS, [None] * STEPS, []
    bank = itertools.count(SCATTER)

    def copy_to(src, dst, peer):
        return links.copy(src, dst, peer, bank)

    def spans(step):
        width = unit * SPLIT[step]
        return pl.ds(starts[step], width), pl.ds(half + starts[step], width)

    def make(step):
        mine, width = part[step], part[step].shape[4]
        start = sum(ref.shape[4] for ref in part[:step])
        both = product(pl.ds(start, width), pl.ds(half + start, width)).reshape(chips, CORES, rows, 2 * width)
        mine[0] = both[:, :, :, :width]
        mine[1] = both[:, :, :, width:]
        swap[step] = copy_to(mine.at[:, :, 1 - c], near[step].at[use], links.sib)
        if not step:
            first[step] = tuple(
                (copy_to(mine.at[side, xo, c], relay[step].at[use, side], same),
                 copy_to(mine.at[side, xo, 1 - c], relay[step].at[use, 2 + side], other))
                for side, same, other in ((0, links.right, links.right_far), (1, links.left, links.left_far)))

    def send(step):
        mine = part[step]
        swap[step].wait_recv()
        if step:
            mine[:, :, c] = mine[:, :, c] + near[step][use]
            first[step] = tuple((copy_to(mine.at[side, xo, c], relay[step].at[use, side], peer),)
                                for side, peer in ((0, links.right), (1, links.left)))
        else:
            for chip in (x, xr, xl):
                mine[:, chip, c] = mine[:, chip, c] + near[step][use, :, chip]
        last.append(copy_to(mine.at[1, xr, c], from_left[step].at[use, 1], links.right))
        last.append(copy_to(mine.at[0, xl, c], from_right[step].at[use, 0], links.left))

    def pass_on(step):
        mine = part[step]
        for side, chip, target, peer in ((0, xr, from_left, links.right), (1, xl, from_right, links.left)):
            for copy in first[step][side]:
                copy.wait_recv()
            total = mine[side, chip, c] + relay[step][use, side]
            if not step:
                total = total + relay[step][use, 2 + side]
            mine[side, chip, c] = total
            last.append(copy_to(mine.at[side, chip, c], target[step].at[use, side], peer))

    for step in range(STEPS):
        with jax.named_scope(f'make{step}'):
            make(step)
        if step:
            with jax.named_scope(f'send{step - 1}'):
                send(step - 1)
    with jax.named_scope(f'send{STEPS - 1}'):
        send(STEPS - 1)
    with jax.named_scope('fillers'):
        for filler in fillers:
            filler()
    for step in range(STEPS):
        with jax.named_scope(f'pass_on{step}'):
            pass_on(step)
    with jax.named_scope('last'):
        for copy in last:
            copy.wait_recv()
    return jnp.concatenate([part[step][side, x, c] + from_left[step][use, side] + from_right[step][use, side]
                            for side in range(2) for step in range(STEPS)], axis=1)


def rms_norm(hidden, gain):
    hidden_f = hidden.astype(F32)
    inv_rms = lax.rsqrt(jnp.mean(hidden_f * hidden_f, axis=-1, keepdims=True) + NORM_EPS)
    return (hidden_f * inv_rms * gain).astype(BF16)


def rms_norm_pull(hidden, gain, cotangent):
    hidden_f, cot = hidden.astype(F32), cotangent.astype(F32)
    inv_rms = lax.rsqrt(jnp.mean(hidden_f * hidden_f, axis=-1, keepdims=True) + NORM_EPS)
    scaled = cot * gain
    dot = jnp.mean(scaled * hidden_f, axis=-1, keepdims=True)
    d_hidden = scaled * inv_rms - hidden_f * (inv_rms * inv_rms * inv_rms * dot)
    return d_hidden.astype(BF16), jnp.sum(cot * (hidden_f * inv_rms), axis=0, keepdims=True)


def columns(ref, *spans):
    return jnp.concatenate([ref[:, span] for span in spans], axis=1)


def lines(ref, *spans):
    return jnp.concatenate([ref[span, :] for span in spans], axis=0)


def flat(ref):
    chips, cores, rows, cols = ref.shape
    return ref[...].reshape(chips * cores * rows, cols)


def project(full, weight, out, tile):
    def body(index, carry):
        cols = pl.ds(pl.multiple_of(index * tile, tile), tile)
        out[:, cols] = dot_nn(flat(full), weight[:, cols]).astype(BF16)
        return carry
    lax.fori_loop(0, out.shape[1] // tile, body, 0)


def project_t(full, weight, out, tile):
    def body(index, carry):
        span = pl.ds(pl.multiple_of(index * tile, tile), tile)
        out[:, span] = dot_nt(flat(full), weight[span, :]).astype(BF16)
        return carry
    lax.fori_loop(0, out.shape[1] // tile, body, 0)


def head(ref, index):
    return ref[:, index * HEAD_DIM:(index + 1) * HEAD_DIM]


def attention(qkv, heads_out, probs=None):
    group = heads_out.shape[1] // HEAD_DIM
    seq = qkv.shape[0]
    causal = lax.broadcasted_iota(jnp.int32, (seq, seq), 0) >= lax.broadcasted_iota(jnp.int32, (seq, seq), 1)
    for index in range(group):
        scores = dot_nt(head(qkv, index), head(qkv, group)) * HEAD_DIM ** -0.5
        scores = jnp.where(causal, scores, -1e30)
        weight = jnp.exp(scores - jnp.max(scores, axis=-1, keepdims=True))
        prob = weight / jnp.sum(weight, axis=-1, keepdims=True)
        if probs is not None:
            probs[index] = prob
        heads_out[:, index * HEAD_DIM:(index + 1) * HEAD_DIM] = dot_nn(prob.astype(BF16), head(qkv, group + 1)).astype(BF16)


def attention_pull(qkv, probs, d_heads, d_qkv):
    group = d_heads.shape[1] // HEAD_DIM
    d_keys = d_values = None
    for index in range(group):
        d_out, prob = head(d_heads, index), probs[index]
        d_prob = dot_nt(d_out, head(qkv, group + 1))
        d_value = dot_tn(prob.astype(BF16), d_out)
        d_score = (prob * (d_prob - jnp.sum(d_prob * prob, axis=-1, keepdims=True)) * HEAD_DIM ** -0.5).astype(BF16)
        d_qkv[:, index * HEAD_DIM:(index + 1) * HEAD_DIM] = dot_nn(d_score, head(qkv, group)).astype(BF16)
        d_key = dot_tn(d_score, head(qkv, index))
        d_keys = d_key if d_keys is None else d_keys + d_key
        d_values = d_value if d_values is None else d_values + d_value
    d_qkv[:, group * HEAD_DIM:(group + 1) * HEAD_DIM] = d_keys.astype(BF16)
    d_qkv[:, (group + 1) * HEAD_DIM:(group + 2) * HEAD_DIM] = d_values.astype(BF16)


def load(src, dst, sem):
    copy = pltpu.make_async_copy(src, dst, sem)
    copy.start()
    return copy


def forward_kernel(layers, chips, hidden, gain_attn, gain_mlp, w_qkv, w_out, w_gate, w_up, w_down, *refs):
    outs, refs = refs[:layers], refs[layers:]
    (wq, wo, wg, wu, wd, full_in, full_mid, qkv, heads_out, act, *ring, state, load_sem, send_sem, recv_sem) = refs
    links = Links(chips, send_sem, recv_sem)
    state[...] = hidden[...]
    links.enter(links.near)
    pairs = ((w_qkv, wq), (w_out, wo), (w_gate, wg), (w_up, wu), (w_down, wd))

    def one_layer(layer, carry):
        row = pl.ds(layer, 1)
        loads = [load(src.at[layer], dst, load_sem.at[index]) for index, (src, dst) in enumerate(pairs)]
        with jax.named_scope('norm_in'):
            full_in[links.x, links.c] = rms_norm(state[...], gain_attn[row, :])
        gather = Gather(links, full_in)
        gather.relay()
        gather.finish()
        loads[0].wait()
        with jax.named_scope('qkv'):
            project(full_in, wq, qkv, qkv.shape[1])
        with jax.named_scope('attention'):
            attention(qkv, heads_out)
        loads[1].wait()
        total = reduce_scatter(links, 0, lambda *spans: dot_nn(heads_out[...], columns(wo, *spans)), ring)
        with jax.named_scope('norm_mid'):
            hidden_mid = state[...] + total.astype(BF16)
            full_mid[links.x, links.c] = rms_norm(hidden_mid, gain_mlp[row, :])
            state[...] = hidden_mid
        links.drain()
        gather = Gather(links, full_mid)
        gather.relay()
        gather.finish()
        for copy in loads[2:]:
            copy.wait()
        tile = 2 * HEAD_DIM

        def body(index, carry):
            cols = pl.ds(pl.multiple_of(index * tile, tile), tile)
            both = dot_nn(flat(full_mid), jnp.concatenate([wg[:, cols], wu[:, cols]], axis=1)).astype(BF16).astype(F32)
            gate_act, up_act = both[:, :tile], both[:, tile:]
            act[:, cols] = (gate_act * jax.nn.sigmoid(gate_act) * up_act).astype(BF16)
            return carry
        with jax.named_scope('gate_up'):
            lax.fori_loop(0, act.shape[1] // tile, body, 0, unroll=2)
        total = reduce_scatter(links, 1, lambda *spans: dot_nn(act[...], columns(wd, *spans)), ring)
        state[...] = state[...] + total.astype(BF16)
        for index, out in enumerate(outs):
            @pl.when(layer == index)
            def _(out=out):
                out[...] = state[...]
        links.drain()
        return carry
    lax.fori_loop(0, layers, one_layer, 0)


def turn(src, dst):
    seq = dst.shape[1]
    tile = HEAD_DIM if dst.shape[0] % (2 * HEAD_DIM) else 2 * HEAD_DIM

    def body(index, carry):
        span = pl.ds(pl.multiple_of(index * tile, tile), tile)
        block = src[:, :, :, span].reshape(seq, tile) if len(src.shape) == 4 else src[:, span]
        dst[span, :] = block.T
        return carry
    lax.fori_loop(0, dst.shape[0] // tile, body, 0)


def backward_kernel(layer, chips, final, hidden, d_out, gain_attn, gain_mlp, w_qkv, w_out, w_gate, w_up, w_down, *refs):
    carried, refs = (refs[0], refs[1:]) if final else (None, refs)
    (d_hidden, gains, o_in, o_mid, o_down, o_attn, o_act, o_gate, o_up, o_heads, o_qkv,
     wq, wo, wgu, wd, full_in, full_mid, full_down, full_attn, qkv, heads_out, act, d_gu, d_heads, d_qkv,
     probs, t_in, t_mid, t_act, t_heads, *ring, gain_mid, gain_last,
     load_sem, save_sem, send_sem, recv_sem) = refs
    links = Links(chips, send_sem, recv_sem)
    x, c = links.x, links.c
    units = act.shape[1]
    left, right = pl.ds(0, units), pl.ds(units, units)
    wg, wu, d_gate, d_up = wgu.at[:, left], wgu.at[:, right], d_gu.at[:, left], d_gu.at[:, right]
    pairs = ((w_qkv, wq), (w_out, wo), (w_gate, wg), (w_up, wu), (w_down, wd))
    loads = [load(src.at[layer], dst, load_sem.at[index]) for index, (src, dst) in enumerate(pairs)]
    saves = []

    def save(src, dst):
        saves.append(load(src, dst, save_sem.at[len(saves)]))

    row = pl.ds(layer, 1)
    full_in[x, c] = rms_norm(hidden[...], gain_attn[row, :])
    full_down[x, c] = d_out[...]
    links.enter(links.others() if final else links.near)
    gather = Gather(links, full_in)
    gather.relay()
    gather_down = Gather(links, full_down, GATHER_DOWN)
    gather.finish()
    loads[0].wait()
    with jax.named_scope('qkv'):
        project(full_in, wq, qkv, qkv.shape[1])
    gather_down.relay()
    with jax.named_scope('attention'):
        attention(qkv, heads_out, probs)
    loads[1].wait()

    def gated():
        gather_down.finish()
        save(full_down, o_down)
        loads[4].wait()
        project_t(full_down, wd, act, 4 * HEAD_DIM)

    def turn_in():
        turn(full_in, t_in)
        turn(heads_out, t_heads)
        save(t_in, o_in)
        save(t_heads, o_heads)

    def turn_mid():
        turn(full_mid, t_mid)
        turn(act, t_act)
        save(t_mid, o_mid)
        save(t_act, o_act)

    total = reduce_scatter(links, 0, lambda *spans: dot_nn(heads_out[...], columns(wo, *spans)), ring, [gated, turn_in])
    hidden_mid = hidden[...] + total.astype(BF16)
    d_hidden[...] = hidden_mid
    full_mid[x, c] = rms_norm(hidden_mid, gain_mlp[row, :])
    links.drain()
    gather = Gather(links, full_mid)
    gather.relay()
    gather.finish()
    loads[2].wait()
    loads[3].wait()
    tile = 2 * HEAD_DIM

    def body(index, carry):
        cols = pl.ds(pl.multiple_of(index * tile, tile), tile)
        both = dot_nn(flat(full_mid), jnp.concatenate([wg[:, cols], wu[:, cols]], axis=1)).astype(BF16).astype(F32)
        gate_act, up_act = both[:, :tile], both[:, tile:]
        sig = jax.nn.sigmoid(gate_act)
        silu = gate_act * sig
        d_act = act[:, cols].astype(F32)
        d_up[:, cols] = (d_act * silu).astype(BF16)
        d_gate[:, cols] = (d_act * up_act * (sig + silu * (1.0 - sig))).astype(BF16)
        act[:, cols] = (silu * up_act).astype(BF16)
        return carry
    with jax.named_scope('gate_up'):
        lax.fori_loop(0, act.shape[1] // tile, body, 0, unroll=2)
    save(d_gate, o_gate)
    save(d_up, o_up)

    def mid_product(*spans):
        return dot_nt(d_gu[...], lines(wgu, *spans))

    total = reduce_scatter(links, 1, mid_product, ring,
                           [turn_mid])
    with jax.named_scope('pull_mid'):
        d_norm, d_gain = rms_norm_pull(d_hidden[...], gain_mlp[row, :], total.astype(BF16))
    d_mid = d_out[...] + d_norm
    full_attn[x, c] = d_mid
    d_hidden[...] = d_mid
    links.drain()
    gather = Gather(links, full_attn)
    lanes = gain_mid.shape[2]
    done = carried.shape[0] if final else 0

    def put(ref, index, value):
        for line in range(lanes):
            ref[index, line:line + 1, :] = value[:, line * HEAD_DIM:(line + 1) * HEAD_DIM]

    mine = gain_mid.at[links.me]
    if final:
        mine[1:done + 1] = carried[...]
    put(mine, 0, d_gain)
    gather.relay()
    gather.finish()
    save(full_attn, o_attn)
    shares, bank = [], itertools.count(SHARE)
    if final:
        shares = [links.copy(mine, mine, peer, bank) for peer in links.others()]
    with jax.named_scope('d_heads'):
        project_t(full_attn, wo, d_heads, d_heads.shape[1])
    with jax.named_scope('attention_pull'):
        attention_pull(qkv, probs, d_heads, d_qkv)
    save(d_qkv, o_qkv)
    total = reduce_scatter(links, 2, lambda *spans: dot_nt(d_qkv[...], lines(wq, *spans)), ring)
    with jax.named_scope('pull_in'):
        d_norm, d_gain = rms_norm_pull(hidden[...], gain_attn[row, :], total.astype(BF16))
    mine_last = gain_last.at[links.me]
    put(mine_last, 0, d_gain)
    if final:
        shares += [links.copy(mine_last, mine_last, peer, bank) for peer in links.others()]
    d_hidden[...] = d_hidden[...] + d_norm
    if final:
        with jax.named_scope('shares'):
            for copy in shares:
                copy.wait_recv()
        size = chips * CORES
        gains[1:done + 2] = sum([gain_mid[peer] for peer in range(1, size)], gain_mid[0])
        gains[0:1] = sum([gain_last[peer] for peer in range(1, size)], gain_last[0])
    else:
        gains[0:1] = mine_last[...]
        gains[1:2] = mine[...]
    with jax.named_scope('saves'):
        for copy in saves:
            copy.wait()
        links.drain()


def grads_kernel(layer, fresh, final, *refs):
    ins, refs = refs[:9], refs[9:]
    small, refs = (refs[:3], refs[3:]) if final else (None, refs)
    if not fresh:
        refs = refs[5:]
    outs, refs = refs[:5], refs[5:]
    small_outs, refs = (refs[:4], refs[4:]) if final else (None, refs)
    bufs, stages, (load_sem, save_sem) = refs[:9], refs[9:14], refs[14:]
    t_in, t_mid, full_down, full_attn, t_act, d_gate, d_up, t_heads, d_qkv = bufs
    loads = {}

    def fetch(*names):
        for name in names:
            loads[name] = load(ins[name], bufs[name], load_sem.at[name])

    fetch(8, 0)
    jobs = ((t_in, d_qkv, 0, 1024, (8, 0)), (t_heads, full_attn, 1, 192, (7, 3)), (t_mid, d_gate, 2, 512, (1, 5)),
            (t_mid, d_up, 3, 512, (6,)), (t_act, full_down, 4, 256, (4, 2)))
    stores = []
    for left, right, place, size, needs in jobs:
        for index in needs:
            loads[index].wait()
        if not place:
            fetch(7, 3, 1, 5, 6, 4, 2)
        out, stage = outs[place], stages[place]
        rows, cols = out.shape[1], out.shape[2]

        def body(index, carry, left=left, right=right, size=size, cols=cols, out=out, stage=stage, place=place):
            span = pl.ds(pl.multiple_of(index * size, size), size)
            turned = left[span, :]
            for col in range(0, cols, 512):
                width = min(512, cols - col)
                if len(right.shape) == 4:
                    chips, cores, some, _ = right.shape
                    piece = right[:, :, :, col:col + width].reshape(chips * cores * some, width)
                else:
                    piece = right[:, col:col + width]
                stage[span, col:col + width] = dot_nn(turned, piece).astype(BF16)
            load(stage.at[span, :], out.at[layer, span, :], save_sem.at[place])
            return carry
        with jax.named_scope(f'job{place}'):
            lax.fori_loop(0, rows // size, body, 0)
        stores.append(pltpu.make_async_copy(stage, out.at[layer], save_sem.at[place]))
    if final:
        small_outs[0][...] = small[0][...]
        small_outs[1][...] = small[1][...]
        for index in range(small[2].shape[0]):
            target = small_outs[2 + index % 2]
            for line in range(small[2].shape[1]):
                target[index // 2:index // 2 + 1, line * HEAD_DIM:(line + 1) * HEAD_DIM] = small[2][index, line:line + 1, :]
    with jax.named_scope('stores'):
        for copy in stores:
            copy.wait()


def vmem(*shape, dtype=BF16):
    return pltpu.VMEM(shape, dtype)


def solution(mesh):
    chips = mesh.shape['tp'] // CORES
    row_spec = P(('dp', 'tp'), None)
    col_spec = P(None, None, 'tp')
    mid_spec = P(None, 'tp', None)
    in_specs = (row_spec, row_spec, P(None, None), P(None, None), col_spec, mid_spec, col_spec, col_spec, mid_spec)
    out_specs = (row_spec, row_spec, P('dp', None, 'tp'), P('dp', 'tp', None), P('dp', None, 'tp'), P('dp', None, 'tp'), P('dp', 'tp', None), P('dp', None), P('dp', None))

    def device_step(x, grad_y, gain_attn, gain_mlp, w_qkv, w_out, w_gate, w_up, w_down):
        layers, width, qkv_cols = w_qkv.shape
        head_cols, units, rows = w_out.shape[1], w_gate.shape[2], x.shape[0]
        group = head_cols // HEAD_DIM
        seq = chips * CORES * rows
        lanes = width // HEAD_DIM
        full = (chips, CORES, rows, width)
        weights = (w_qkv, w_out, w_gate, w_up, w_down)
        weight_bufs = [vmem(*weight.shape[1:]) for weight in weights]

        def ring_bufs(uses):
            lead = ((2, chips, CORES), (uses, 2, chips), (uses, 4), (uses, 2), (uses, 2))
            widths = [width // 2 // sum(SPLIT) * share for share in SPLIT]
            return [tuple(vmem(*dims, rows, cols, dtype=F32) for cols in widths) for dims in lead]

        def dma(count):
            return pltpu.SemaphoreType.DMA((count,))

        def params(ident):
            return pltpu.CompilerParams(collective_id=ident, has_side_effects=True, vmem_limit_bytes=VMEM_LIMIT)

        def forward(hidden):
            copies = SHARE
            return pl.pallas_call(
                functools.partial(forward_kernel, layers, chips),
                out_shape=[jax.ShapeDtypeStruct(hidden.shape, BF16)] * layers,
                in_specs=[VMEM_SPEC] * 3 + [ANY] * 5,
                out_specs=[VMEM_SPEC] * layers,
                scratch_shapes=weight_bufs + [vmem(*full), vmem(*full), vmem(seq, qkv_cols), vmem(seq, head_cols), vmem(seq, units)]
                + ring_bufs(2) + [vmem(*hidden.shape), dma(5), dma(copies), dma(copies)],
                compiler_params=params(layers), name='forward',
            )(hidden, gain_attn, gain_mlp, *weights)

        def backward(layer, hidden, d_out, carried):
            final = layer == 0
            copies = SHARE + (2 * (chips * CORES - 1) if final else 0)
            done = carried[0].shape[0] if final else 0
            factor = lambda *shape: jax.ShapeDtypeStruct(shape, BF16)
            return pl.pallas_call(
                functools.partial(backward_kernel, layer, chips, final),
                out_shape=[factor(*hidden.shape), jax.ShapeDtypeStruct((done + 2, lanes, HEAD_DIM), F32)]
                + [factor(width, seq)] * 2 + [factor(*full)] * 2
                + [factor(units, seq), factor(seq, units), factor(seq, units), factor(head_cols, seq), factor(seq, qkv_cols)],
                in_specs=[VMEM_SPEC] * 4 + [ANY] * 5 + [VMEM_SPEC] * len(carried),
                out_specs=[VMEM_SPEC] * 2 + [ANY] * 9,
                scratch_shapes=weight_bufs[:2] + [vmem(width, 2 * units), weight_bufs[4]] + [vmem(*full)] * 4
                + [vmem(seq, qkv_cols), vmem(seq, head_cols), vmem(seq, units), vmem(seq, 2 * units),
                   vmem(seq, head_cols), vmem(seq, qkv_cols), vmem(group, seq, seq, dtype=F32),
                   vmem(width, seq), vmem(width, seq), vmem(units, seq), vmem(head_cols, seq)] + ring_bufs(3)
                + [vmem(chips * CORES, done + 1, lanes, HEAD_DIM, dtype=F32), vmem(chips * CORES, 1, lanes, HEAD_DIM, dtype=F32),
                   dma(5), dma(9), dma(copies), dma(copies)],
                compiler_params=params(layer), name=f'backward_{layer}',
            )(hidden, d_out, gain_attn, gain_mlp, *weights, *carried)

        grad_shapes = [jax.ShapeDtypeStruct(weight.shape, BF16) for weight in weights]

        def grads(layer, factors, small, into):
            fresh, final = not into, layer == 0
            shapes = [jax.ShapeDtypeStruct(value.shape, value.dtype) for value in (x, x, gain_attn, gain_mlp)]
            return pl.pallas_call(
                functools.partial(grads_kernel, layer, fresh, final),
                out_shape=grad_shapes + (shapes if final else []),
                in_specs=[ANY] * len(factors) + [VMEM_SPEC] * len(small) + [ANY] * len(into),
                out_specs=[ANY] * 5 + [VMEM_SPEC] * (4 if final else 0),
                scratch_shapes=[vmem(*factor.shape) for factor in factors] + [vmem(*weight.shape[1:]) for weight in weights]
                + [dma(len(factors)), dma(5)],
                input_output_aliases={len(factors) + len(small) + index: index for index in range(len(into))},
                compiler_params=pltpu.CompilerParams(vmem_limit_bytes=VMEM_LIMIT), name=f'grads_{layer}',
            )(*factors, *small, *into)

        kept = [x, *forward(x)]
        d_hidden, out_grads, partial_gains = grad_y, [], []
        for layer in reversed(range(layers)):
            carried = [jnp.concatenate(partial_gains[::-1])] if layer == 0 else []
            d_hidden, gains, *factors = backward(layer, kept[layer], d_hidden, carried)
            partial_gains.append(gains)
            if layer:
                out_grads = grads(layer, factors, [], out_grads)
                d_hidden, *out_grads = lax.optimization_barrier((d_hidden, *out_grads))
        *out_grads, y, grad_x, grad_attn, grad_mlp = grads(0, factors, [kept[-1], d_hidden, gains], out_grads)
        return (y, grad_x, *out_grads, grad_attn, grad_mlp)

    return jax.shard_map(device_step, mesh=mesh, in_specs=in_specs, out_specs=out_specs, check_vma=False)
```

```python
import functools
import itertools

import jax
import jax.numpy as jnp
from jax import lax
from jax.experimental import pallas as pl
from jax.experimental.pallas import tpu as pltpu
from jax.sharding import PartitionSpec as P

HEAD_DIM = 128
NORM_EPS = 1e-5
CORES = 2
MESH = pl.DeviceIdType.MESH
F32 = jnp.float32
BF16 = jnp.bfloat16
VMEM_LIMIT = 66_000_000
SPLIT = (3, 4, 5)
STEPS = len(SPLIT)
GATHER, GATHER_DOWN, SCATTER = 0, 13, 26
SHARE = SCATTER + 8 * STEPS + 2
ANY = pl.BlockSpec(memory_space=pltpu.HBM)
VMEM_SPEC = pl.BlockSpec(memory_space=pltpu.VMEM)


def dot_nn(a, b):
    return lax.dot_general(a, b, (((1,), (0,)), ((), ())), preferred_element_type=F32)


def dot_nt(a, b):
    return lax.dot_general(a, b, (((1,), (1,)), ((), ())), preferred_element_type=F32)


def dot_tn(a, b):
    return lax.dot_general(a, b, (((0,), (0,)), ((), ())), preferred_element_type=F32)


class Links:
    def __init__(self, chips, send_sem, recv_sem):
        self.me = lax.axis_index('tp')
        self.chips = chips
        self.x = lax.div(self.me, CORES)
        self.c = lax.rem(self.me, CORES)
        self.xr = lax.rem(self.x + 1, chips)
        self.xl = lax.rem(self.x + chips - 1, chips)
        self.xo = lax.rem(self.x + 2, chips)
        self.right = self.xr * CORES + self.c
        self.left = self.xl * CORES + self.c
        self.sib = self.x * CORES + 1 - self.c
        self.right_far, self.left_far = self.xr * CORES + 1 - self.c, self.xl * CORES + 1 - self.c
        self.near = (self.right, self.left, self.sib, self.right_far, self.left_far)
        self.send_sem, self.recv_sem, self.pending = send_sem, recv_sem, []

    def enter(self, peers):
        barrier = pltpu.get_barrier_semaphore()
        for peer in peers:
            pl.semaphore_signal(barrier, inc=1, device_id={'tp': peer}, device_id_type=MESH)
        pl.semaphore_wait(barrier, len(peers))

    def others(self):
        size = self.chips * CORES
        return [lax.rem(self.me + step, size) for step in range(1, size)]

    def copy(self, src, dst, peer, bank):
        index = next(bank)
        copy = pltpu.make_async_remote_copy(
            src_ref=src, dst_ref=dst, send_sem=self.send_sem.at[index], recv_sem=self.recv_sem.at[index],
            device_id={'tp': peer}, device_id_type=MESH)
        copy.start()
        self.pending.append(copy)
        return copy

    def drain(self):
        for copy in self.pending:
            copy.wait_send()
        self.pending = []


class Gather:
    def __init__(self, links, full, bank=GATHER):
        self.links, self.full, self.bank = links, full, itertools.count(bank)
        self.half = full.shape[3] // 2
        part_a, part_b = pl.ds(0, self.half), pl.ds(self.half, self.half)
        x, c = links.x, links.c
        self.a, self.b = part_a, part_b
        self.right_a = self.send(x, part_a, links.right)
        self.left_b = self.send(x, part_b, links.left)
        self.right_b = self.send(x, part_b, links.right)
        self.left_a = self.send(x, part_a, links.left)
        self.near = [links.copy(full.at[x, c], full.at[x, c], links.sib, self.bank)]

    def send(self, chip, part, peer):
        ref = self.full.at[chip, self.links.c, :, part]
        return self.links.copy(ref, ref, peer, self.bank)

    @jax.named_scope('gather')
    def relay(self):
        links = self.links
        self.right_a.wait_recv()
        relay_a = self.send(links.xl, self.a, links.right)
        self.near.append(self.send(links.xl, self.a, links.sib))
        self.left_b.wait_recv()
        relay_b = self.send(links.xr, self.b, links.left)
        self.near.append(self.send(links.xr, self.b, links.sib))
        self.far = (relay_a, relay_b)

    @jax.named_scope('finish')
    def finish(self):
        links = self.links
        self.right_b.wait_recv()
        self.near.append(self.send(links.xl, self.b, links.sib))
        self.left_a.wait_recv()
        self.near.append(self.send(links.xr, self.a, links.sib))
        self.far[0].wait_recv()
        self.near.append(self.send(links.xo, self.a, links.sib))
        self.far[1].wait_recv()
        self.near.append(self.send(links.xo, self.b, links.sib))
        for copy in self.near:
            copy.wait_recv()


def reduce_scatter(links, use, product, ring, fillers=()):
    part, near, relay, from_left, from_right = ring
    _, chips, _, rows, _ = part[0].shape
    half = sum(ref.shape[4] for ref in part)
    x, c, xr, xl, xo = links.x, links.c, links.xr, links.xl, links.xo
    swap, first, last = [None] * STEPS, [None] * STEPS, []
    bank = itertools.count(SCATTER)

    def copy_to(src, dst, peer):
        return links.copy(src, dst, peer, bank)

    def spans(step):
        width = unit * SPLIT[step]
        return pl.ds(starts[step], width), pl.ds(half + starts[step], width)

    def make(step):
        mine, width = part[step], part[step].shape[4]
        start = sum(ref.shape[4] for ref in part[:step])
        both = product(pl.ds(start, width), pl.ds(half + start, width)).reshape(chips, CORES, rows, 2 * width)
        mine[0] = both[:, :, :, :width]
        mine[1] = both[:, :, :, width:]
        swap[step] = copy_to(mine.at[:, :, 1 - c], near[step].at[use], links.sib)
        if not step:
            first[step] = tuple(
                (copy_to(mine.at[side, xo, c], relay[step].at[use, side], same),
                 copy_to(mine.at[side, xo, 1 - c], relay[step].at[use, 2 + side], other))
                for side, same, other in ((0, links.right, links.right_far), (1, links.left, links.left_far)))

    def send(step):
        mine = part[step]
        swap[step].wait_recv()
        if step:
            mine[:, :, c] = mine[:, :, c] + near[step][use]
            first[step] = tuple((copy_to(mine.at[side, xo, c], relay[step].at[use, side], peer),)
                                for side, peer in ((0, links.right), (1, links.left)))
        else:
            for chip in (x, xr, xl):
                mine[:, chip, c] = mine[:, chip, c] + near[step][use, :, chip]
        last.append(copy_to(mine.at[1, xr, c], from_left[step].at[use, 1], links.right))
        last.append(copy_to(mine.at[0, xl, c], from_right[step].at[use, 0], links.left))

    def pass_on(step):
        mine = part[step]
        for side, chip, target, peer in ((0, xr, from_left, links.right), (1, xl, from_right, links.left)):
            for copy in first[step][side]:
                copy.wait_recv()
            total = mine[side, chip, c] + relay[step][use, side]
            if not step:
                total = total + relay[step][use, 2 + side]
            mine[side, chip, c] = total
            last.append(copy_to(mine.at[side, chip, c], target[step].at[use, side], peer))

    for step in range(STEPS):
        with jax.named_scope(f'make{step}'):
            make(step)
        if step:
            with jax.named_scope(f'send{step - 1}'):
                send(step - 1)
    with jax.named_scope(f'send{STEPS - 1}'):
        send(STEPS - 1)
    with jax.named_scope('fillers'):
        for filler in fillers:
            filler()
    for step in range(STEPS):
        with jax.named_scope(f'pass_on{step}'):
            pass_on(step)
    with jax.named_scope('last'):
        for copy in last:
            copy.wait_recv()
    return jnp.concatenate([part[step][side, x, c] + from_left[step][use, side] + from_right[step][use, side]
                            for side in range(2) for step in range(STEPS)], axis=1)


def rms_norm(hidden, gain):
    hidden_f = hidden.astype(F32)
    inv_rms = lax.rsqrt(jnp.mean(hidden_f * hidden_f, axis=-1, keepdims=True) + NORM_EPS)
    return (hidden_f * inv_rms * gain).astype(BF16)


def rms_norm_pull(hidden, gain, cotangent):
    hidden_f, cot = hidden.astype(F32), cotangent.astype(F32)
    inv_rms = lax.rsqrt(jnp.mean(hidden_f * hidden_f, axis=-1, keepdims=True) + NORM_EPS)
    scaled = cot * gain
    dot = jnp.mean(scaled * hidden_f, axis=-1, keepdims=True)
    d_hidden = scaled * inv_rms - hidden_f * (inv_rms * inv_rms * inv_rms * dot)
    return d_hidden.astype(BF16), jnp.sum(cot * (hidden_f * inv_rms), axis=0, keepdims=True)


def columns(ref, *spans):
    return jnp.concatenate([ref[:, span] for span in spans], axis=1)


def lines(ref, *spans):
    return jnp.concatenate([ref[span, :] for span in spans], axis=0)


def flat(ref):
    chips, cores, rows, cols = ref.shape
    return ref[...].reshape(chips * cores * rows, cols)


def project(full, weight, out, tile):
    def body(index, carry):
        cols = pl.ds(pl.multiple_of(index * tile, tile), tile)
        out[:, cols] = dot_nn(flat(full), weight[:, cols]).astype(BF16)
        return carry
    lax.fori_loop(0, out.shape[1] // tile, body, 0)


def project_t(full, weight, out, tile):
    def body(index, carry):
        span = pl.ds(pl.multiple_of(index * tile, tile), tile)
        out[:, span] = dot_nt(flat(full), weight[span, :]).astype(BF16)
        return carry
    lax.fori_loop(0, out.shape[1] // tile, body, 0)


def head(ref, index):
    return ref[:, index * HEAD_DIM:(index + 1) * HEAD_DIM]


def attention(qkv, heads_out, probs=None):
    group = heads_out.shape[1] // HEAD_DIM
    seq = qkv.shape[0]
    causal = lax.broadcasted_iota(jnp.int32, (seq, seq), 0) >= lax.broadcasted_iota(jnp.int32, (seq, seq), 1)
    for index in range(group):
        scores = dot_nt(head(qkv, index), head(qkv, group)) * HEAD_DIM ** -0.5
        scores = jnp.where(causal, scores, -1e30)
        weight = jnp.exp(scores - jnp.max(scores, axis=-1, keepdims=True))
        prob = weight / jnp.sum(weight, axis=-1, keepdims=True)
        if probs is not None:
            probs[index] = prob
        heads_out[:, index * HEAD_DIM:(index + 1) * HEAD_DIM] = dot_nn(prob.astype(BF16), head(qkv, group + 1)).astype(BF16)


def attention_pull(qkv, probs, d_heads, d_qkv):
    group = d_heads.shape[1] // HEAD_DIM
    d_keys = d_values = None
    for index in range(group):
        d_out, prob = head(d_heads, index), probs[index]
        d_prob = dot_nt(d_out, head(qkv, group + 1))
        d_value = dot_tn(prob.astype(BF16), d_out)
        d_score = (prob * (d_prob - jnp.sum(d_prob * prob, axis=-1, keepdims=True)) * HEAD_DIM ** -0.5).astype(BF16)
        d_qkv[:, index * HEAD_DIM:(index + 1) * HEAD_DIM] = dot_nn(d_score, head(qkv, group)).astype(BF16)
        d_key = dot_tn(d_score, head(qkv, index))
        d_keys = d_key if d_keys is None else d_keys + d_key
        d_values = d_value if d_values is None else d_values + d_value
    d_qkv[:, group * HEAD_DIM:(group + 1) * HEAD_DIM] = d_keys.astype(BF16)
    d_qkv[:, (group + 1) * HEAD_DIM:(group + 2) * HEAD_DIM] = d_values.astype(BF16)


def load(src, dst, sem):
    copy = pltpu.make_async_copy(src, dst, sem)
    copy.start()
    return copy


def forward_kernel(layers, chips, hidden, gain_attn, gain_mlp, w_qkv, w_out, w_gate, w_up, w_down, *refs):
    outs, refs = refs[:layers], refs[layers:]
    (wq, wo, wg, wu, wd, full_in, full_mid, qkv, heads_out, act, *ring, state, load_sem, send_sem, recv_sem) = refs
    links = Links(chips, send_sem, recv_sem)
    state[...] = hidden[...]
    links.enter(links.near)
    pairs = ((w_qkv, wq), (w_out, wo), (w_gate, wg), (w_up, wu), (w_down, wd))

    def one_layer(layer, carry):
        row = pl.ds(layer, 1)
        loads = [load(src.at[layer], dst, load_sem.at[index]) for index, (src, dst) in enumerate(pairs)]
        with jax.named_scope('norm_in'):
            full_in[links.x, links.c] = rms_norm(state[...], gain_attn[row, :])
        gather = Gather(links, full_in)
        gather.relay()
        gather.finish()
        loads[0].wait()
        with jax.named_scope('qkv'):
            project(full_in, wq, qkv, qkv.shape[1])
        with jax.named_scope('attention'):
            attention(qkv, heads_out)
        loads[1].wait()
        total = reduce_scatter(links, 0, lambda *spans: dot_nn(heads_out[...], columns(wo, *spans)), ring)
        with jax.named_scope('norm_mid'):
            hidden_mid = state[...] + total.astype(BF16)
            full_mid[links.x, links.c] = rms_norm(hidden_mid, gain_mlp[row, :])
            state[...] = hidden_mid
        links.drain()
        gather = Gather(links, full_mid)
        gather.relay()
        gather.finish()
        for copy in loads[2:]:
            copy.wait()
        tile = 2 * HEAD_DIM

        def body(index, carry):
            cols = pl.ds(pl.multiple_of(index * tile, tile), tile)
            both = dot_nn(flat(full_mid), jnp.concatenate([wg[:, cols], wu[:, cols]], axis=1)).astype(BF16).astype(F32)
            gate_act, up_act = both[:, :tile], both[:, tile:]
            act[:, cols] = (gate_act * jax.nn.sigmoid(gate_act) * up_act).astype(BF16)
            return carry
        with jax.named_scope('gate_up'):
            lax.fori_loop(0, act.shape[1] // tile, body, 0, unroll=2)
        total = reduce_scatter(links, 1, lambda *spans: dot_nn(act[...], columns(wd, *spans)), ring)
        state[...] = state[...] + total.astype(BF16)
        for index, out in enumerate(outs):
            @pl.when(layer == index)
            def _(out=out):
                out[...] = state[...]
        links.drain()
        return carry
    lax.fori_loop(0, layers, one_layer, 0)


def turn(src, dst):
    seq = dst.shape[1]
    tile = HEAD_DIM if dst.shape[0] % (2 * HEAD_DIM) else 2 * HEAD_DIM

    def body(index, carry):
        span = pl.ds(pl.multiple_of(index * tile, tile), tile)
        block = src[:, :, :, span].reshape(seq, tile) if len(src.shape) == 4 else src[:, span]
        dst[span, :] = block.T
        return carry
    lax.fori_loop(0, dst.shape[0] // tile, body, 0)


def backward_kernel(layer, chips, final, hidden, d_out, gain_attn, gain_mlp, w_qkv, w_out, w_gate, w_up, w_down, *refs):
    carried, refs = (refs[0], refs[1:]) if final else (None, refs)
    (d_hidden, gains, o_in, o_mid, o_down, o_attn, o_act, o_gate, o_up, o_heads, o_qkv,
     wq, wo, wgu, wd, full_in, full_mid, full_down, full_attn, qkv, heads_out, act, d_gu, d_heads, d_qkv,
     probs, t_in, t_mid, t_act, t_heads, *ring, gain_mid, gain_last,
     load_sem, save_sem, send_sem, recv_sem) = refs
    links = Links(chips, send_sem, recv_sem)
    x, c = links.x, links.c
    units = act.shape[1]
    left, right = pl.ds(0, units), pl.ds(units, units)
    wg, wu, d_gate, d_up = wgu.at[:, left], wgu.at[:, right], d_gu.at[:, left], d_gu.at[:, right]
    pairs = ((w_qkv, wq), (w_out, wo), (w_gate, wg), (w_up, wu), (w_down, wd))
    loads = [load(src.at[layer], dst, load_sem.at[index]) for index, (src, dst) in enumerate(pairs)]
    saves = []

    def save(src, dst):
        saves.append(load(src, dst, save_sem.at[len(saves)]))

    row = pl.ds(layer, 1)
    full_in[x, c] = rms_norm(hidden[...], gain_attn[row, :])
    full_down[x, c] = d_out[...]
    links.enter(links.others() if final else links.near)
    gather = Gather(links, full_in)
    gather.relay()
    gather_down = Gather(links, full_down, GATHER_DOWN)
    gather.finish()
    loads[0].wait()
    with jax.named_scope('qkv'):
        project(full_in, wq, qkv, qkv.shape[1])
    gather_down.relay()
    with jax.named_scope('attention'):
        attention(qkv, heads_out, probs)
    loads[1].wait()

    def gated():
        gather_down.finish()
        save(full_down, o_down)
        loads[4].wait()
        project_t(full_down, wd, act, 4 * HEAD_DIM)

    def turn_in():
        turn(full_in, t_in)
        turn(heads_out, t_heads)
        save(t_in, o_in)
        save(t_heads, o_heads)

    def turn_mid():
        turn(full_mid, t_mid)
        turn(act, t_act)
        save(t_mid, o_mid)
        save(t_act, o_act)

    total = reduce_scatter(links, 0, lambda *spans: dot_nn(heads_out[...], columns(wo, *spans)), ring, [gated, turn_in])
    hidden_mid = hidden[...] + total.astype(BF16)
    d_hidden[...] = hidden_mid
    full_mid[x, c] = rms_norm(hidden_mid, gain_mlp[row, :])
    links.drain()
    gather = Gather(links, full_mid)
    gather.relay()
    gather.finish()
    loads[2].wait()
    loads[3].wait()
    tile = 2 * HEAD_DIM

    def body(index, carry):
        cols = pl.ds(pl.multiple_of(index * tile, tile), tile)
        both = dot_nn(flat(full_mid), jnp.concatenate([wg[:, cols], wu[:, cols]], axis=1)).astype(BF16).astype(F32)
        gate_act, up_act = both[:, :tile], both[:, tile:]
        sig = jax.nn.sigmoid(gate_act)
        silu = gate_act * sig
        d_act = act[:, cols].astype(F32)
        d_up[:, cols] = (d_act * silu).astype(BF16)
        d_gate[:, cols] = (d_act * up_act * (sig + silu * (1.0 - sig))).astype(BF16)
        act[:, cols] = (silu * up_act).astype(BF16)
        return carry
    with jax.named_scope('gate_up'):
        lax.fori_loop(0, act.shape[1] // tile, body, 0, unroll=2)
    save(d_gate, o_gate)
    save(d_up, o_up)

    def mid_product(*spans):
        return dot_nt(d_gu[...], lines(wgu, *spans))

    total = reduce_scatter(links, 1, mid_product, ring,
                           [turn_mid])
    with jax.named_scope('pull_mid'):
        d_norm, d_gain = rms_norm_pull(d_hidden[...], gain_mlp[row, :], total.astype(BF16))
    d_mid = d_out[...] + d_norm
    full_attn[x, c] = d_mid
    d_hidden[...] = d_mid
    links.drain()
    gather = Gather(links, full_attn)
    lanes = gain_mid.shape[2]
    done = carried.shape[0] if final else 0

    def put(ref, index, value):
        for line in range(lanes):
            ref[index, line:line + 1, :] = value[:, line * HEAD_DIM:(line + 1) * HEAD_DIM]

    mine = gain_mid.at[links.me]
    if final:
        mine[1:done + 1] = carried[...]
    put(mine, 0, d_gain)
    gather.relay()
    gather.finish()
    save(full_attn, o_attn)
    shares, bank = [], itertools.count(SHARE)
    if final:
        shares = [links.copy(mine, mine, peer, bank) for peer in links.others()]
    with jax.named_scope('d_heads'):
        project_t(full_attn, wo, d_heads, d_heads.shape[1])
    with jax.named_scope('attention_pull'):
        attention_pull(qkv, probs, d_heads, d_qkv)
    save(d_qkv, o_qkv)
    total = reduce_scatter(links, 2, lambda *spans: dot_nt(d_qkv[...], lines(wq, *spans)), ring)
    with jax.named_scope('pull_in'):
        d_norm, d_gain = rms_norm_pull(hidden[...], gain_attn[row, :], total.astype(BF16))
    mine_last = gain_last.at[links.me]
    put(mine_last, 0, d_gain)
    if final:
        shares += [links.copy(mine_last, mine_last, peer, bank) for peer in links.others()]
    d_hidden[...] = d_hidden[...] + d_norm
    if final:
        with jax.named_scope('shares'):
            for copy in shares:
                copy.wait_recv()
        size = chips * CORES
        gains[1:done + 2] = sum([gain_mid[peer] for peer in range(1, size)], gain_mid[0])
        gains[0:1] = sum([gain_last[peer] for peer in range(1, size)], gain_last[0])
    else:
        gains[0:1] = mine_last[...]
        gains[1:2] = mine[...]
    with jax.named_scope('saves'):
        for copy in saves:
            copy.wait()
        links.drain()


def grads_kernel(layer, fresh, final, *refs):
    ins, refs = refs[:9], refs[9:]
    small, refs = (refs[:3], refs[3:]) if final else (None, refs)
    if not fresh:
        refs = refs[5:]
    outs, refs = refs[:5], refs[5:]
    small_outs, refs = (refs[:4], refs[4:]) if final else (None, refs)
    bufs, stages, (load_sem, save_sem), refs = refs[:9], refs[9:14], refs[14:16], refs[16:]
    t_in, t_mid, full_down, full_attn, t_act, d_gate, d_up, t_heads, d_qkv = bufs
    loads = {}

    def fetch(*names):
        for name in names:
            loads[name] = load(ins[name], bufs[name], load_sem.at[name])

    fetch(8, 0)
    if final:
        *small_bufs, small_sem = refs
        arrivals = [load(src, dst, small_sem.at[index]) for index, (src, dst) in enumerate(zip(small, small_bufs))]
    jobs = ((t_in, d_qkv, 0, 1024, (8, 0)), (t_heads, full_attn, 1, 192, (7, 3)), (t_mid, d_gate, 2, 512, (1, 5)),
            (t_mid, d_up, 3, 512, (6,)), (t_act, full_down, 4, 256, (4, 2)))
    stores = []
    for left, right, place, size, needs in jobs:
        for index in needs:
            loads[index].wait()
        if not place:
            fetch(7, 3, 1, 5, 6, 4, 2)
        out, stage = outs[place], stages[place]
        rows, cols = out.shape[1], out.shape[2]

        def body(index, carry, left=left, right=right, size=size, cols=cols, out=out, stage=stage, place=place):
            span = pl.ds(pl.multiple_of(index * size, size), size)
            turned = left[span, :]
            for col in range(0, cols, 512):
                width = min(512, cols - col)
                if len(right.shape) == 4:
                    chips, cores, some, _ = right.shape
                    piece = right[:, :, :, col:col + width].reshape(chips * cores * some, width)
                else:
                    piece = right[:, col:col + width]
                stage[span, col:col + width] = dot_nn(turned, piece).astype(BF16)
            load(stage.at[span, :], out.at[layer, span, :], save_sem.at[place])
            return carry
        with jax.named_scope(f'job{place}'):
            lax.fori_loop(0, rows // size, body, 0)
        stores.append(pltpu.make_async_copy(stage, out.at[layer], save_sem.at[place]))
        if final and not place:
            for copy in arrivals:
                copy.wait()
            pairs = small_bufs[2]
            for index in range(pairs.shape[0]):
                target = small_bufs[3 + index % 2]
                for line in range(pairs.shape[1]):
                    target[index // 2:index // 2 + 1, line * HEAD_DIM:(line + 1) * HEAD_DIM] = pairs[index, line:line + 1, :]
            sources = (small_bufs[0], small_bufs[1], small_bufs[3], small_bufs[4])
            stores += [load(src, dst, small_sem.at[3 + index]) for index, (src, dst) in enumerate(zip(sources, small_outs))]
    with jax.named_scope('stores'):
        for copy in stores:
            copy.wait()


def vmem(*shape, dtype=BF16):
    return pltpu.VMEM(shape, dtype)


def solution(mesh):
    chips = mesh.shape['tp'] // CORES
    row_spec = P(('dp', 'tp'), None)
    col_spec = P(None, None, 'tp')
    mid_spec = P(None, 'tp', None)
    in_specs = (row_spec, row_spec, P(None, None), P(None, None), col_spec, mid_spec, col_spec, col_spec, mid_spec)
    out_specs = (row_spec, row_spec, P('dp', None, 'tp'), P('dp', 'tp', None), P('dp', None, 'tp'), P('dp', None, 'tp'), P('dp', 'tp', None), P('dp', None), P('dp', None))

    def device_step(x, grad_y, gain_attn, gain_mlp, w_qkv, w_out, w_gate, w_up, w_down):
        layers, width, qkv_cols = w_qkv.shape
        head_cols, units, rows = w_out.shape[1], w_gate.shape[2], x.shape[0]
        group = head_cols // HEAD_DIM
        seq = chips * CORES * rows
        lanes = width // HEAD_DIM
        full = (chips, CORES, rows, width)
        weights = (w_qkv, w_out, w_gate, w_up, w_down)
        weight_bufs = [vmem(*weight.shape[1:]) for weight in weights]

        def ring_bufs(uses):
            lead = ((2, chips, CORES), (uses, 2, chips), (uses, 4), (uses, 2), (uses, 2))
            widths = [width // 2 // sum(SPLIT) * share for share in SPLIT]
            return [tuple(vmem(*dims, rows, cols, dtype=F32) for cols in widths) for dims in lead]

        def dma(count):
            return pltpu.SemaphoreType.DMA((count,))

        def params(ident):
            return pltpu.CompilerParams(collective_id=ident, has_side_effects=True, vmem_limit_bytes=VMEM_LIMIT)

        def forward(hidden):
            copies = SHARE
            return pl.pallas_call(
                functools.partial(forward_kernel, layers, chips),
                out_shape=[jax.ShapeDtypeStruct(hidden.shape, BF16)] * layers,
                in_specs=[VMEM_SPEC] * 3 + [ANY] * 5,
                out_specs=[VMEM_SPEC] * layers,
                scratch_shapes=weight_bufs + [vmem(*full), vmem(*full), vmem(seq, qkv_cols), vmem(seq, head_cols), vmem(seq, units)]
                + ring_bufs(2) + [vmem(*hidden.shape), dma(5), dma(copies), dma(copies)],
                compiler_params=params(layers), name='forward',
            )(hidden, gain_attn, gain_mlp, *weights)

        def backward(layer, hidden, d_out, carried):
            final = layer == 0
            copies = SHARE + (2 * (chips * CORES - 1) if final else 0)
            done = carried[0].shape[0] if final else 0
            factor = lambda *shape: jax.ShapeDtypeStruct(shape, BF16)
            return pl.pallas_call(
                functools.partial(backward_kernel, layer, chips, final),
                out_shape=[factor(*hidden.shape), jax.ShapeDtypeStruct((done + 2, lanes, HEAD_DIM), F32)]
                + [factor(width, seq)] * 2 + [factor(*full)] * 2
                + [factor(units, seq), factor(seq, units), factor(seq, units), factor(head_cols, seq), factor(seq, qkv_cols)],
                in_specs=[VMEM_SPEC] * 4 + [ANY] * 5 + [VMEM_SPEC] * len(carried),
                out_specs=[VMEM_SPEC] * 2 + [ANY] * 9,
                scratch_shapes=weight_bufs[:2] + [vmem(width, 2 * units), weight_bufs[4]] + [vmem(*full)] * 4
                + [vmem(seq, qkv_cols), vmem(seq, head_cols), vmem(seq, units), vmem(seq, 2 * units),
                   vmem(seq, head_cols), vmem(seq, qkv_cols), vmem(group, seq, seq, dtype=F32),
                   vmem(width, seq), vmem(width, seq), vmem(units, seq), vmem(head_cols, seq)] + ring_bufs(3)
                + [vmem(chips * CORES, done + 1, lanes, HEAD_DIM, dtype=F32), vmem(chips * CORES, 1, lanes, HEAD_DIM, dtype=F32),
                   dma(5), dma(9), dma(copies), dma(copies)],
                compiler_params=params(layer), name=f'backward_{layer}',
            )(hidden, d_out, gain_attn, gain_mlp, *weights, *carried)

        grad_shapes = [jax.ShapeDtypeStruct(weight.shape, BF16) for weight in weights]

        def grads(layer, factors, small, into):
            fresh, final = not into, layer == 0
            shapes = [jax.ShapeDtypeStruct(value.shape, value.dtype) for value in (x, x, gain_attn, gain_mlp)]
            small_bufs = [vmem(*value.shape, dtype=value.dtype) for value in (*small, gain_attn, gain_mlp)] + [dma(7)]
            return pl.pallas_call(
                functools.partial(grads_kernel, layer, fresh, final),
                out_shape=grad_shapes + (shapes if final else []),
                in_specs=[ANY] * (len(factors) + len(small) + len(into)),
                out_specs=[ANY] * (9 if final else 5),
                scratch_shapes=[vmem(*factor.shape) for factor in factors] + [vmem(*weight.shape[1:]) for weight in weights]
                + [dma(len(factors)), dma(5)] + (small_bufs if final else []),
                input_output_aliases={len(factors) + len(small) + index: index for index in range(len(into))},
                compiler_params=pltpu.CompilerParams(vmem_limit_bytes=VMEM_LIMIT), name=f'grads_{layer}',
            )(*factors, *small, *into)

        kept = [x, *forward(x)]
        d_hidden, out_grads, partial_gains = grad_y, [], []
        for layer in reversed(range(layers)):
            carried = [jnp.concatenate(partial_gains[::-1])] if layer == 0 else []
            d_hidden, gains, *factors = backward(layer, kept[layer], d_hidden, carried)
            partial_gains.append(gains)
            if layer:
                out_grads = grads(layer, factors, [], out_grads)
                d_hidden, *out_grads = lax.optimization_barrier((d_hidden, *out_grads))
        *out_grads, y, grad_x, grad_attn, grad_mlp = grads(0, factors, [kept[-1], d_hidden, gains], out_grads)
        return (y, grad_x, *out_grads, grad_attn, grad_mlp)

    return jax.shard_map(device_step, mesh=mesh, in_specs=in_specs, out_specs=out_specs, check_vma=False)
```
